512 devices in a mesh: gx: 8 (over z), gy: 8 (over y), gz: 8 (over x, core).
Axes of the slice: x: 4, y: 8, z: 8, core: 2. Of those that a mesh axis runs over, the one named last changes fastest.
Arguments:
- right_side: float32 [512, 512, 512], P('gx', 'gy', 'gz'), may hold values from -6 to 6
- guess: float32 [512, 512, 512], P('gx', 'gy', 'gz'), may hold values from -6 to 6
Outputs:
- solution: float32 [512, 512, 512], P('gx', 'gy', 'gz')
- residual: float32 [512, 512, 512], P('gx', 'gy', 'gz')
The draws below stay inside these ranges and needn't reach their ends.
All inputs are finite; a program needn't handle non-finite values.
Results may differ from the reference program's by a relative error of at most 0.0003.
Values sent between devices are 32-bit elements.
A program may use at most 256 MiB of HBM per device.

```python
import jax
import jax.numpy as jnp
from jax import lax

LEVELS = 7
COARSE_SWEEPS = 4
NX = 512
NY = 512
NZ = 512


def level_of(stream_key, dims, split, low, largest):
    def one(axis_at, blocks):
        heights = jax.random.uniform(jax.random.fold_in(jax.random.fold_in(stream_key, 6), axis_at), (blocks,), jnp.float32, low / len(split), largest / len(split))
        return jnp.repeat(jnp.exp(heights), dims[axis_at] // blocks).reshape((-1,) + (1,) * (len(dims) - axis_at - 1))

    loudness = one(*split[0])
    for cut in split[1:]:
        loudness = loudness * one(*cut)
    return loudness


def bell_draw(key, shape, deviation, most, cuts=(), held_as=jnp.bfloat16):
    array = deviation * jax.random.normal(key, shape, jnp.float32)
    if cuts:
        array = array * level_of(key, shape, cuts, -0.22, 0.18)
    return jnp.clip(array, -most, most).astype(held_as)


def setup_inputs(seed: int = 0) -> dict:
    streams_of = jax.random.split(jax.random.key(seed), 3)
    right_side = bell_draw(streams_of[0], (NX, NY, NZ), 1.0, 6.0, ((0, 8), (1, 8), (2, 8)), jnp.float32)
    guess = bell_draw(streams_of[1], (NX, NY, NZ), 1.0, 6.0, ((0, 8), (1, 8), (2, 8)), jnp.float32)
    return dict(right_side=right_side, guess=guess)


def face_total(padded):
    total = padded[2:, 1:-1, 1:-1] + padded[:-2, 1:-1, 1:-1]
    total = total + padded[1:-1, 2:, 1:-1] + padded[1:-1, :-2, 1:-1]
    total = total + padded[1:-1, 1:-1, 2:] + padded[1:-1, 1:-1, :-2]
    return total


def neighbours(field):
    return face_total(jnp.pad(field, 1))


def walls(index, total):
    return (index == 0).astype(jnp.float32) + (index == total - 1).astype(jnp.float32)


def geometry(shape):
    first = lax.iota(jnp.int32, shape[0])[:, None, None]
    second = lax.iota(jnp.int32, shape[1])[None, :, None]
    third = lax.iota(jnp.int32, shape[2])[None, None, :]
    parity = (first + second + third) % 2
    diagonal = 6.0 + walls(first, shape[0]) + walls(second, shape[1]) + walls(third, shape[2])
    return parity == 0, parity == 1, diagonal


def half_sweep(field, source, colour, diagonal, scale):
    updated = (scale * source + neighbours(field)) / diagonal
    return jnp.where(colour, updated, field)


def residual_of(field, source, diagonal, inverse):
    return source - (diagonal * field - neighbours(field)) * inverse


def restrict(remainder):
    shape = remainder.shape
    grouped = remainder.reshape(shape[0] // 2, 2, shape[1] // 2, 2, shape[2] // 2, 2)
    return jnp.sum(grouped, axis=(1, 3, 5)) * 0.125


def odd_pad(field):
    for axis in range(3):
        count = field.shape[axis]
        lowest = -lax.slice_in_dim(field, 0, 1, axis=axis)
        highest = -lax.slice_in_dim(field, count - 1, count, axis=axis)
        field = jnp.concatenate([lowest, field, highest], axis=axis)
    return field


def prolong(padded):
    centre = padded[1:-1, 1:-1, 1:-1]
    below_first = 0.25 * (padded[:-2, 1:-1, 1:-1] - centre)
    above_first = 0.25 * (padded[2:, 1:-1, 1:-1] - centre)
    below_second = 0.25 * (padded[1:-1, :-2, 1:-1] - centre)
    above_second = 0.25 * (padded[1:-1, 2:, 1:-1] - centre)
    below_third = 0.25 * (padded[1:-1, 1:-1, :-2] - centre)
    above_third = 0.25 * (padded[1:-1, 1:-1, 2:] - centre)
    along_first = jnp.stack([below_first, above_first], axis=1)[:, :, :, None, :, None]
    along_second = jnp.stack([below_second, above_second], axis=2)[:, None, :, :, :, None]
    along_third = jnp.stack([below_third, above_third], axis=3)[:, None, :, None, :, :]
    fine = centre[:, None, :, None, :, None] + along_first + along_second + along_third
    shape = centre.shape
    return fine.reshape(2 * shape[0], 2 * shape[1], 2 * shape[2])


def cycle(field, source, level):
    red, black, diagonal = geometry(source.shape)
    scale = 4.0 ** level
    if level == LEVELS - 1:
        for sweep_index in range(COARSE_SWEEPS):
            field = half_sweep(field, source, red, diagonal, scale)
            field = half_sweep(field, source, black, diagonal, scale)
        return field
    field = half_sweep(field, source, red, diagonal, scale)
    field = half_sweep(field, source, black, diagonal, scale)
    coarse = restrict(residual_of(field, source, diagonal, 0.25 ** level))
    correction = cycle(jnp.zeros_like(coarse), coarse, level + 1)
    field = field + prolong(odd_pad(correction))
    field = half_sweep(field, source, red, diagonal, scale)
    return half_sweep(field, source, black, diagonal, scale)


def reference(right_side, guess):
    solution = cycle(guess, right_side, 0)
    red, black, diagonal = geometry(right_side.shape)
    return solution, residual_of(solution, right_side, diagonal, 1.0)
```

```python
import jax
import jax.numpy as jnp
from jax import lax
from jax.experimental import pallas as pl
from jax.experimental.pallas import tpu as pltpu
from jax.sharding import PartitionSpec as P

LEVELS = 7
COARSE_SWEEPS = 4
GATHER = 4
LANES = 128
AXES = ("gx", "gy", "gz")


def rows_of(count):
    return max(8, count)


def lane_iota(rows):
    return lax.broadcasted_iota(jnp.int32, (rows, LANES), 1)


def row_iota(rows):
    return lax.broadcasted_iota(jnp.int32, (rows, LANES), 0)


def loop(count, body):
    if count == 1:
        body(0)
    else:
        def step(i, carry):
            body(i)
            return carry
        lax.fori_loop(0, count, step, 0)


def exact_dot(value, matrix):
    first = value.astype(jnp.bfloat16)
    rest = value - first.astype(jnp.float32)
    second = rest.astype(jnp.bfloat16)
    third = (rest - second.astype(jnp.float32)).astype(jnp.bfloat16)
    dot = lambda part: jnp.dot(part, matrix, preferred_element_type=jnp.float32)
    return (dot(third) + dot(second)) + dot(first)


def widest(count, most):
    return max(size for size in range(1, count + 1) if count % size == 0 and (size <= most or size == 1))


class Level:
    def __init__(self, number, dims, places, counts, v, s, w, d):
        self.number, self.dims, self.places, self.counts = number, dims, places, counts
        self.v, self.s, self.w, self.d = v, s, w, d
        self.rows = rows_of(dims[1])
        self.scale = 4.0 ** number
        self.inverse = 0.25 ** number
        self.chunk = min(dims[0], max(2, 32 * 8 // self.rows))

    def prepare(self):
        x, y, z = self.dims
        row, lane = row_iota(self.rows), lane_iota(self.rows)
        valid = (row < y) & (lane < z)
        at_y, at_z = self.places[1] * y + row, self.places[2] * z + lane
        one = lambda at, total: (at == 0).astype(jnp.float32) + (at == total - 1).astype(jnp.float32)
        base = 6.0 + one(at_y, self.counts[1] * y) + one(at_z, self.counts[2] * z)
        for wall in range(2):
            self.d[wall] = jnp.where(valid, base + wall, 0.0)
            for parity in range(2):
                self.w[2 * wall + parity] = jnp.where(valid & ((row + lane) % 2 == parity), 1.0 / (base + wall), 0.0)
        self.v[...] = jnp.zeros_like(self.v)

    def wall(self, plane):
        at = self.places[0] * self.dims[0] + plane
        last = self.counts[0] * self.dims[0] - 1
        if isinstance(at, int):
            return int(at in (0, last))
        return jnp.where((at == 0) | (at == last), 1, 0)

    def total(self, start, face):
        count, rows, z = self.chunk, self.rows, self.dims[2]
        slab = self.v[pl.ds(start, count + 2), pl.ds(8, rows), :]
        centre = slab[1:-1]
        total = slab[2:] + slab[:-2]
        total = total + self.v[pl.ds(start + 1, count), pl.ds(9, rows), :] + self.v[pl.ds(start + 1, count), pl.ds(7, rows), :]
        lane = lane_iota(rows)
        out = []
        for i in range(count):
            c = centre[i]
            if face is None:
                z_sum = pltpu.roll(c, 1, 1) + pltpu.roll(c, LANES - 1, 1)
            else:
                g = pltpu.roll(face[...], LANES - (start + i), 1)
                if z != 64:
                    g_high = pltpu.roll(g, LANES + z - 64, 1) if z < 64 else g
                    high = jnp.where(lane == z, g_high, c)
                else:
                    high = jnp.where(lane == 64, g, c)
                z_sum = jnp.where(lane == 0, g, pltpu.roll(c, 1, 1)) + pltpu.roll(high, LANES - 1, 1)
            out.append(total[i] + z_sum)
        return out, [centre[i] for i in range(count)]

    def sweep(self, colour, face=None, zero=False):
        def body(step):
            start = step * self.chunk
            if not zero:
                totals, centres = self.total(start, face)
            results = []
            for i in range(self.chunk):
                weight = self.w[2 * self.wall(start + i) + (i + colour) % 2]
                given = self.scale * self.s[start + i]
                if zero:
                    results.append(given * weight)
                else:
                    results.append(jnp.where(weight > 0, (given + totals[i]) * weight, centres[i]))
            for i in range(self.chunk):
                self.v[start + i + 1, pl.ds(8, self.rows), :] = results[i]
        loop(self.dims[0] // self.chunk, body)

    def remainder(self, start, face):
        totals, centres = self.total(start, face)
        out = []
        for i in range(self.chunk):
            d = self.d[self.wall(start + i)]
            out.append(jnp.where(d > 0, self.s[start + i] - (d * centres[i] - totals[i]) * self.inverse, 0.0))
        return out

    def restrict_to(self, target, pairs, face=None):
        rows, z = self.rows, self.dims[2]
        coarse_rows = rows_of(self.dims[1] // 2)
        half = self.chunk // 2
        source_lane = lax.broadcasted_iota(jnp.int32, (LANES, LANES), 0)
        target_lane = lax.broadcasted_iota(jnp.int32, (LANES, LANES), 1)
        halve = jnp.where((source_lane // 2 == target_lane) & (source_lane < z), 0.125, 0.0).astype(jnp.bfloat16)
        if rows < 16:
            pairs[...] = jnp.zeros_like(pairs)

        def first(step):
            r = self.remainder(step * self.chunk, face)
            for i in range(half):
                pairs[step * half + i, pl.ds(0, rows), :] = r[2 * i] + r[2 * i + 1]
        loop(self.dims[0] // self.chunk, first)

        planes = self.dims[0] // 2
        many = min(planes, max(1, 256 // coarse_rows))

        def second(step):
            at = pl.ds(step * many, many)
            q = pairs[at, pl.ds(0, coarse_rows, stride=2), :] + pairs[at, pl.ds(1, coarse_rows, stride=2), :]
            q = exact_dot(q.reshape(many * coarse_rows, LANES), halve)
            target[at] = q.reshape(many, coarse_rows, LANES)
        loop(planes // many, second)

    def reflect(self):
        x, y, z = self.dims
        v = self.v

        def low_x():
            v[0] = -v[1]

        def high_x():
            v[x + 1] = -v[x]

        def low_y():
            for_all = pl.ds(1, x)
            v[for_all, pl.ds(7, 1), :] = -v[for_all, pl.ds(8, 1), :]

        def high_y():
            for_all = pl.ds(1, x)
            v[for_all, pl.ds(8 + y, 1), :] = -v[for_all, pl.ds(7 + y, 1), :]

        for axis, low, high in ((0, low_x, high_x), (1, low_y, high_y)):
            if isinstance(self.counts[axis], int) and isinstance(self.places[axis], int):
                low()
                high()
            else:
                pl.when(self.places[axis] == 0)(low)
                pl.when(self.places[axis] == self.counts[axis] - 1)(high)


def lift(v, dims, places, counts, fine, spread, high_lane, face=None):
    x, y, z = dims
    rows = rows_of(y)
    k = lax.broadcasted_iota(jnp.int32, (LANES, LANES), 0)
    f = lax.broadcasted_iota(jnp.int32, (LANES, LANES), 1)
    inside = f < 2 * z
    own = ((f // 2 == k) & inside).astype(jnp.float32)
    beside = ((f // 2 + 2 * (f % 2) - 1 == k) & inside & (k < z)).astype(jnp.float32)
    low_wall = jnp.where(places[2] == 0, 1.0, 0.0)
    high_wall = jnp.where(places[2] == counts[2] - 1, 1.0, 0.0)
    at_low, at_high = f == 0, f == 2 * z - 1
    beside = beside + jnp.where(at_low & (k == 0), -low_wall, 0.0) + jnp.where(at_low & (k == LANES - 1), 1.0 - low_wall, 0.0)
    beside = beside + jnp.where(at_high & (k == z - 1), -high_wall, 0.0) + jnp.where(at_high & (k == high_lane), 1.0 - high_wall, 0.0)
    both = (0.25 * (own + beside)).astype(jnp.bfloat16)
    own = (0.25 * own).astype(jnp.bfloat16)
    tall = rows + 16
    lane = lane_iota(rows)
    valid = row_iota(rows) < y

    many = widest(x + 2, 832 // tall)

    def first(step):
        at = pl.ds(step * many, many)
        spread[at] = exact_dot(v[at].reshape(many * tall, LANES), own).reshape(many, tall, LANES)
    loop((x + 2) // many, first)

    group = widest(x, 256 // rows)

    def second(step):
        es = []
        for i in range(group):
            plane = step * group + i
            e = v[plane + 1, pl.ds(8, rows), :]
            if face is not None:
                e = jnp.where(lane < z, e, pltpu.roll(face[...], (LANES - 1) - plane, 1))
            es.append(e)
        centres = exact_dot(jnp.concatenate(es, axis=0), both)
        for i in range(group):
            plane = step * group + i
            centre = centres[i * rows:(i + 1) * rows]
            ys = (spread[plane + 1, pl.ds(7, rows), :], spread[plane + 1, pl.ds(9, rows), :])
            for up_x in range(2):
                xs = centre + spread[plane + 2 * up_x, pl.ds(8, rows), :]
                for up_y in range(2):
                    q = xs + ys[up_y]
                    if y < rows:
                        q = jnp.where(valid, q, 0.0)
                    at = (2 * plane + up_x + 1, pl.ds(8 + up_y, rows, stride=2), slice(None))
                    fine.v[at] = fine.v[at] + q
    loop(x // group, second)


def solve_kernel(counts, blocks, coarse, uses, refs):
    right_side, guess, out_v, out_r = refs[:4]
    refs = list(refs[4:])
    take = lambda: refs.pop(0)
    places = tuple(lax.axis_index(axis) for axis in AXES)
    levels = []
    for number, dims in enumerate(blocks[:GATHER]):
        levels.append(Level(number, dims, places, counts, take(), take(), take(), take()))
    for number, dims in enumerate(coarse):
        levels.append(Level(GATHER + number, dims, (0, 0, 0), (1, 1, 1), take(), take(), take(), take()))
    exchange = [(take(), take(), take(), take(), take()) for _ in range(GATHER)]
    pairs = [take() for _ in range(LEVELS - 1)]
    spreads = [take() for _ in range(LEVELS - 1)]
    block_s, block_v, packet, line, joined, packets, line_send, line_recv, gather_send, gather_recv = refs

    barrier = pltpu.get_barrier_semaphore()

    def greet(device):
        pl.semaphore_signal(barrier, inc=1, device_id=device, device_id_type=pl.DeviceIdType.MESH)

    def greet_plane(offset, carry):
        other = lax.rem(places[0] * counts[1] + places[1] + offset, counts[0] * counts[1])
        greet({AXES[0]: other // counts[1], AXES[1]: other % counts[1]})
        return carry
    lax.fori_loop(1, counts[0] * counts[1], greet_plane, 0)
    for offset in range(1, counts[2]):
        greet({AXES[2]: lax.rem(places[2] + offset, counts[2])})
    for level in levels:
        level.prepare()
    block_v[...] = jnp.zeros_like(block_v)
    for number in range(GATHER):
        exchange[number][4][...] = jnp.zeros_like(exchange[number][4])
    z0 = blocks[0][2]
    top = levels[0]

    def load(x):
        top.v[x + 1, pl.ds(8, top.rows), pl.ds(0, z0)] = guess[x]
        top.s[x] = jnp.concatenate([right_side[x], jnp.zeros((top.rows, LANES - z0), jnp.float32)], axis=1)
    loop(blocks[0][0] // 4, lambda step: [load(4 * step + i) for i in range(4)])

    pl.semaphore_wait(barrier, counts[0] * counts[1] + counts[2] - 2)
    turn = [0] * GATHER
    sent = []

    def swap(number):
        level = levels[number]
        out, into, send, recv, face = exchange[number]
        n, v, (x, y, z) = turn[number], level.v, level.dims
        turn[number] += 1
        def folded(value):
            half = value.shape[0] // 2
            return jnp.where(lane_iota(half) < 64, value[:half], pltpu.roll(value[half:], 64, 1))

        def unfolded(value):
            low = lane_iota(value.shape[0]) < 64
            return jnp.concatenate([jnp.where(low, value, 0.0), jnp.where(low, pltpu.roll(value, 64, 1), 0.0)], axis=0)
        if x // 2 < 8:
            folded = unfolded = lambda value: value
        half_y, half_x = max(8, y // 2), max(8, x // 2)
        halves = (half_y, half_y, half_x, half_x, y, y)
        out[n, 0, pl.ds(0, half_y)] = folded(v[x, pl.ds(8, y), :])
        out[n, 1, pl.ds(0, half_y)] = folded(v[1, pl.ds(8, y), :])
        out[n, 2, pl.ds(0, half_x)] = folded(v[pl.ds(1, x), 7 + y, :])
        out[n, 3, pl.ds(0, half_x)] = folded(v[pl.ds(1, x), 8, :])
        lane = lane_iota(y)
        many = min(x, 16)

        def columns(step, carry):
            last, leading = carry
            for i in range(many):
                plane = step * many + i
                c = v[plane + 1, pl.ds(8, y), :]
                turned = pltpu.roll(c, plane + 64, 1)
                last = jnp.where(lane == (plane + 63 + z) % LANES, turned, last)
                leading = jnp.where(lane == plane + 64, turned, leading)
            return last, leading
        zero = jnp.zeros((y, LANES), jnp.float32)
        last, leading = lax.fori_loop(0, x // many, columns, (zero, zero))
        out[n, 4, pl.ds(0, y)] = last
        out[n, 5, pl.ds(0, y)] = leading

        copies = []
        for axis in range(3):
            for way in range(2):
                side = 2 * axis + way
                other = places[axis] + (1 - 2 * way)
                copy = pltpu.make_async_remote_copy(
                    src_ref=out.at[n, side, pl.ds(0, halves[side])], dst_ref=into.at[n, side, pl.ds(0, halves[side])],
                    send_sem=send.at[n, side], recv_sem=recv.at[n, side],
                    device_id={AXES[axis]: other}, device_id_type=pl.DeviceIdType.MESH)
                has_target = other < counts[axis] if way == 0 else other >= 0
                has_origin = places[axis] > 0 if way == 0 else places[axis] < counts[axis] - 1
                pl.when(has_target)(copy.start)
                sent.append((has_target, copy))
                copies.append((has_origin, copy))

        def land(side):
            got = into.at[n, side]
            if side == 0:
                v[0, pl.ds(8, y), :] = unfolded(got[pl.ds(0, half_y)])
            elif side == 1:
                v[x + 1, pl.ds(8, y), :] = unfolded(got[pl.ds(0, half_y)])
            elif side == 2:
                v[pl.ds(1, x), 7, :] = unfolded(got[pl.ds(0, half_x)])
            elif side == 3:
                v[pl.ds(1, x), 8 + y, :] = unfolded(got[pl.ds(0, half_x)])
            elif side == 4:
                face[...] = jnp.where(lane < 64, pltpu.roll(got[pl.ds(0, y)], (65 - z) % LANES, 1), face[...])
            else:
                face[...] = jnp.where(lane >= 64, got[pl.ds(0, y)], face[...])
        for side, (has_origin, copy) in enumerate(copies):
            @pl.when(has_origin)
            def _(side=side, copy=copy):
                copy.wait_recv()
                land(side)
        return face

    for number in range(GATHER):
        level = levels[number]
        if number == 0:
            level.sweep(0, swap(0))
        else:
            level.sweep(0, zero=True)
        level.sweep(1, swap(number))
        target = levels[number + 1].s if number + 1 < GATHER else block_s
        level.restrict_to(target, pairs[number], swap(number))

    bx, by, bz = blocks[GATHER]
    nx, ny, nz = counts
    wide = LANES // bx
    packed = jnp.zeros((rows_of(by), LANES), jnp.float32)
    for x in range(bx):
        packed = packed + pltpu.roll(block_s[x], x * wide + places[2] * bz, 1)
    packet[...] = packed[:by]

    def line_copy(source, target):
        return pltpu.make_async_remote_copy(
            src_ref=packet, dst_ref=line.at[source], send_sem=line_send.at[target], recv_sem=line_recv.at[source],
            device_id={AXES[2]: target}, device_id_type=pl.DeviceIdType.MESH)

    for offset in range(1, nz):
        line_copy(places[2], lax.rem(places[2] + offset, nz)).start()
    merged = packed[:by]
    for offset in range(1, nz):
        source = lax.rem(places[2] + nz - offset, nz)
        line_copy(source, lax.rem(places[2] + offset, nz)).wait_recv()
        merged = merged + line[source]
    joined[...] = merged
    total = nx * ny
    me = places[0] * ny + places[1]

    def plane_copy(source, target):
        return pltpu.make_async_remote_copy(
            src_ref=joined, dst_ref=packets.at[source], send_sem=gather_send.at[target], recv_sem=gather_recv.at[source],
            device_id={AXES[0]: target // ny, AXES[1]: target % ny}, device_id_type=pl.DeviceIdType.MESH)

    def post(offset, carry):
        plane_copy(me, lax.rem(me + offset, total)).start()
        return carry
    lax.fori_loop(1, total, post, 0)
    packets[me] = merged

    def arrive(offset, carry):
        plane_copy(lax.rem(me + total - offset, total), lax.rem(me + offset, total)).wait_recv()
        return carry
    lax.fori_loop(1, total, arrive, 0)
    whole = levels[GATHER]

    def unpack(px):
        for py in range(0, ny, 2):
            pair = jnp.concatenate([packets[px * ny + py], packets[px * ny + py + 1]], axis=0)
            for x in range(bx):
                whole.s[px * bx + x, pl.ds(py * by, 2 * by), :] = pltpu.roll(pair, LANES - x * wide, 1) if x else pair
    loop(nx, unpack)

    for number in range(GATHER, LEVELS - 1):
        level = levels[number]
        level.sweep(0, zero=True)
        level.sweep(1)
        level.restrict_to(levels[number + 1].s, pairs[number])
    level = levels[LEVELS - 1]
    level.sweep(0, zero=True)
    level.sweep(1)
    for _ in range(COARSE_SWEEPS - 1):
        level.sweep(0)
        level.sweep(1)
    for number in reversed(range(GATHER, LEVELS - 1)):
        level, below = levels[number], levels[number + 1]
        below.reflect()
        lift(below.v, below.dims, (0, 0, 0), (1, 1, 1), level, spreads[number], below.dims[2])
        level.sweep(0)
        level.sweep(1)

    whole.reflect()
    shift = lax.rem(LANES - places[2] * bz, LANES)
    odd = lax.rem(places[1], 2) == 1
    for x in range(bx + 2):
        part = whole.v[places[0] * bx + x, pl.ds(pl.multiple_of(places[1] // 2 * 8, 8), 24), :]
        block_v[x, pl.ds(0, 20)] = pltpu.roll(jnp.where(odd, part[4:], part[:20]), shift, 1)
    lift(block_v, blocks[GATHER], places, counts, levels[GATHER - 1], spreads[GATHER - 1], bz)
    for number in reversed(range(GATHER)):
        level = levels[number]
        level.sweep(0, swap(number))
        level.sweep(1, swap(number))
        face = swap(number)
        if number > 0:
            level.reflect()
            lift(level.v, level.dims, places, counts, levels[number - 1], spreads[number - 1], 63, face)

    def finish(step):
        r = top.remainder(step * top.chunk, face)
        for i in range(top.chunk):
            at = step * top.chunk + i
            out_r[at] = r[i][:, :z0]
            out_v[at] = top.v[at + 1, pl.ds(8, top.rows), pl.ds(0, z0)]
    loop(blocks[0][0] // top.chunk, finish)

    for has_target, copy in sent:
        pl.when(has_target)(copy.wait_send)

    for offset in range(1, nz):
        line_copy(places[2], lax.rem(places[2] + offset, nz)).wait_send()

    def leave(offset, carry):
        plane_copy(me, lax.rem(me + offset, total)).wait_send()
        return carry
    lax.fori_loop(1, total, leave, 0)


def solution(mesh):
    counts = tuple(mesh.shape[axis] for axis in AXES)

    def per_device(right_side, guess):
        shape = right_side.shape
        blocks = [tuple(side >> level for side in shape) for level in range(GATHER + 1)]
        whole = tuple(side * count for side, count in zip(blocks[GATHER], counts))
        coarse = [tuple(side >> level for side in whole) for level in range(LEVELS - GATHER)]
        grids = blocks[:GATHER] + coarse
        scratch = []
        vmem = lambda *dims: scratch.append(pltpu.VMEM(dims, jnp.float32))
        for x, y, z in grids:
            vmem(x + 2, rows_of(y) + 16, LANES)
            vmem(x, rows_of(y), LANES)
            vmem(4, rows_of(y), LANES)
            vmem(2, rows_of(y), LANES)
        for number, (x, y, z) in enumerate(blocks[:GATHER]):
            turns = 6 if number == 0 else 5
            side = max(x, y)
            vmem(turns, 6, side, LANES)
            vmem(turns, 6, side, LANES)
            scratch.append(pltpu.SemaphoreType.DMA((turns, 6)))
            scratch.append(pltpu.SemaphoreType.DMA((turns, 6)))
            vmem(y, LANES)
        for x, y, z in grids[:-1]:
            vmem(x // 2, max(16, y), LANES)
        for number in range(LEVELS - 1):
            x, y, z = blocks[number + 1] if number < GATHER else grids[number + 1]
            vmem(x + 2, rows_of(y) + 16, LANES)
        bx, by, bz = blocks[GATHER]
        vmem(bx, rows_of(by), LANES)
        vmem(bx + 2, rows_of(by) + 16, LANES)
        vmem(by, LANES)
        vmem(counts[2], by, LANES)
        vmem(by, LANES)
        total = counts[0] * counts[1]
        vmem(total, by, LANES)
        for many in (counts[2], counts[2], total, total):
            scratch.append(pltpu.SemaphoreType.DMA((many,)))

        def kernel(*refs):
            solve_kernel(counts, blocks, coarse, None, refs)

        whole_block = pl.BlockSpec(memory_space=pltpu.VMEM)
        return pl.pallas_call(
            kernel,
            out_shape=(jax.ShapeDtypeStruct(shape, jnp.float32),) * 2,
            in_specs=[whole_block] * 2,
            out_specs=(whole_block,) * 2,
            scratch_shapes=scratch,
            compiler_params=pltpu.CompilerParams(collective_id=0, has_side_effects=True, vmem_limit_bytes=60 * 2**20),
            name="vcycle",
        )(right_side, guess)

    spec = P(*AXES)
    return jax.shard_map(per_device, mesh=mesh, in_specs=(spec, spec), out_specs=(spec, spec), check_vma=False)
```

```python
import itertools

import jax
import jax.numpy as jnp
from jax import lax
from jax.experimental import pallas as pl
from jax.experimental.pallas import tpu as pltpu
from jax.sharding import PartitionSpec as P

LEVELS = 7
COARSE_SWEEPS = 4
SHARED = 4
LANES = 128
EDGE = 8
AXES = ("gx", "gy", "gz")
MESH = pl.DeviceIdType.MESH
WAYS = [way for way in itertools.product((-1, 0, 1), repeat=3) if any(way)]
FINAL = {1: 1, 2: 2, 3: 3}
REACH = {level: radius + 3 for level, radius in FINAL.items()}


def rows_of(count):
    return max(8, -(-count // 8) * 8)


def lane_iota(rows):
    return lax.broadcasted_iota(jnp.int32, (rows, LANES), 1)


def row_iota(rows):
    return lax.broadcasted_iota(jnp.int32, (rows, LANES), 0)


def loop(count, body):
    if count == 1:
        body(0)
    else:
        def step(i, carry):
            body(i)
            return carry
        lax.fori_loop(0, count, step, 0)


def turn(value, amount):
    amount = amount % LANES
    return pltpu.roll(value, amount, 1) if amount else value


def exact_dot(value, matrix):
    first = value.astype(jnp.bfloat16)
    rest = value - first.astype(jnp.float32)
    second = rest.astype(jnp.bfloat16)
    third = (rest - second.astype(jnp.float32)).astype(jnp.bfloat16)
    dot = lambda part: jnp.dot(part, matrix, preferred_element_type=jnp.float32)
    return (dot(third) + dot(second)) + dot(first)


def widest(count, most, step=1):
    return max(size for size in range(step, count + 1, step) if count % size == 0 and (size <= most or size == step))


def signed(lane):
    return jnp.where(lane < 64, lane, lane - LANES)


class Grid:
    def __init__(self, number, dims, places, counts, v, s, w, d):
        self.number, self.dims, self.places, self.counts = number, dims, places, counts
        self.v, self.s, self.w, self.d = v, s, w, d
        self.reach = REACH.get(number, 0)
        self.ox, self.start, self.height, _, _ = layout(number, dims)
        self.sx, self.sy = (EDGE, 8) if self.reach else (0, 0)
        self.rows = rows_of(dims[1])

    def prepare(self):
        x, y, z = self.dims
        beyond = EDGE if self.reach else 0

        def base(height, start):
            row, lane = row_iota(height) + (start - 8), signed(lane_iota(height))
            at_y, at_z = self.places[1] * y + row, self.places[2] * z + lane
            last_y, last_z = self.counts[1] * y - 1, self.counts[2] * z - 1
            valid = (lane >= -beyond) & (lane < z + beyond) & (row >= -beyond) & (row < y + beyond)
            valid = valid & (at_y >= 0) & (at_y <= last_y) & (at_z >= 0) & (at_z <= last_z)
            one = lambda at, last: (at == 0).astype(jnp.float32) + (at == last).astype(jnp.float32)
            return valid, 6.0 + one(at_y, last_y) + one(at_z, last_z)
        valid, diagonal = base(self.height, self.start)
        for wall in range(2):
            self.w[wall] = jnp.where(valid, 1.0 / (diagonal + wall), 0.0)
        self.w[2] = jnp.zeros_like(diagonal)
        valid, diagonal = base(self.rows, 8)
        for wall in range(2):
            self.d[wall] = jnp.where(valid, diagonal + wall, 0.0)
        self.v[...] = jnp.zeros_like(self.v)
        if self.reach:
            self.s[...] = jnp.zeros_like(self.s)

    def wall(self, plane, beyond=False):
        at = self.places[0] * self.dims[0] + plane
        last = self.counts[0] * self.dims[0] - 1
        if isinstance(at, int):
            return int(at in (0, last))
        kind = jnp.where((at == 0) | (at == last), 1, 0)
        return jnp.where((at < 0) | (at > last), 2, kind) if beyond else kind

    def total(self, plane, count, start, height, face):
        z = self.dims[2]
        at = plane + self.ox
        slab = self.v[pl.ds(at - 1, count + 2), pl.ds(start, height), :]
        centre = slab[1:-1]
        total = slab[2:] + slab[:-2]
        total = total + self.v[pl.ds(at, count), pl.ds(start + 1, height), :] + self.v[pl.ds(at, count), pl.ds(start - 1, height), :]
        lane = lane_iota(height)
        out = []
        for i in range(count):
            c = centre[i]
            if face is None:
                z_sum = pltpu.roll(c, 1, 1) + pltpu.roll(c, LANES - 1, 1)
            else:
                g = pltpu.roll(face[...], LANES - (plane + i), 1)
                high = jnp.where(lane == 64, g, c)
                z_sum = jnp.where(lane == 0, g, pltpu.roll(c, 1, 1)) + pltpu.roll(high, LANES - 1, 1)
            out.append(total[i] + z_sum)
        return out, [centre[i] for i in range(count)]

    def sweep(self, colour, face=None, zero=False, beyond=0):
        start, height = self.start, self.height
        planes = self.dims[0] + 2 * beyond
        chunk = widest(planes, 112 * 8 // height, 2)
        parity = (row_iota(height) + lane_iota(height) + start) % 2

        def body(step):
            first = step * chunk - beyond
            if not zero:
                totals, centres = self.total(first, chunk, start, height, face)
            results = []
            for i in range(chunk):
                weight = self.w[self.wall(first + i, beyond > 0)]
                given = self.s[first + i + self.sx, pl.ds(start - 8 + self.sy, height), :]
                mine = parity == (i + colour + beyond) % 2
                if zero:
                    results.append(jnp.where(mine, given * weight, 0.0))
                else:
                    results.append(jnp.where(mine, (given + totals[i]) * weight, centres[i]))
            for i in range(chunk):
                self.v[first + i + self.ox, pl.ds(start, height), :] = results[i]
        loop(planes // chunk, body)

    def remainder(self, first, chunk, face):
        totals, centres = self.total(first, chunk, 8, self.rows, face)
        out = []
        for i in range(chunk):
            d = self.d[self.wall(first + i)]
            r = self.s[first + i + self.sx, pl.ds(self.sy, self.rows), :] - (d * centres[i] - totals[i])
            out.append(r if self.dims[1] == self.rows else jnp.where(d > 0, r, 0.0))
        return out

    def restrict_to(self, target, corner, pairs, face=None):
        rows, z = self.rows, self.dims[2]
        coarse_rows = rows_of(self.dims[1] // 2)
        chunk = widest(self.dims[0], 32 * 8 // rows, 2)
        half = chunk // 2
        source_lane = lax.broadcasted_iota(jnp.int32, (LANES, LANES), 0)
        target_lane = lax.broadcasted_iota(jnp.int32, (LANES, LANES), 1)
        halve = jnp.where((source_lane // 2 == target_lane) & (source_lane < z), 0.5, 0.0).astype(jnp.bfloat16)
        if rows < 16:
            pairs[...] = jnp.zeros_like(pairs)

        def first(step):
            r = self.remainder(step * chunk, chunk, face)
            for i in range(half):
                pairs[step * half + i, pl.ds(0, rows), :] = r[2 * i] + r[2 * i + 1]
        loop(self.dims[0] // chunk, first)

        planes = self.dims[0] // 2
        many = min(planes, max(1, 256 // coarse_rows))

        def second(step):
            at = pl.ds(step * many, many)
            q = pairs[at, pl.ds(0, coarse_rows, stride=2), :] + pairs[at, pl.ds(1, coarse_rows, stride=2), :]
            q = exact_dot(q.reshape(many * coarse_rows, LANES), halve)
            target[pl.ds(step * many + corner[0], many), pl.ds(corner[1], coarse_rows), :] = q.reshape(many, coarse_rows, LANES)
        loop(planes // many, second)

    def reflect(self):
        (x, y, z), v, ox = self.dims, self.v, self.ox
        margin = 3 if self.reach else 0
        for_all = pl.ds(ox - margin, x + 2 * margin)

        def low_x():
            v[ox - 1] = -v[ox]

        def high_x():
            v[ox + x] = -v[ox + x - 1]

        def low_y():
            v[for_all, pl.ds(7, 1), :] = -v[for_all, pl.ds(8, 1), :]

        def high_y():
            v[for_all, pl.ds(8 + y, 1), :] = -v[for_all, pl.ds(7 + y, 1), :]

        for axis, low, high in ((0, low_x, high_x), (1, low_y, high_y)):
            if isinstance(self.counts[axis], int) and isinstance(self.places[axis], int):
                low()
                high()
            else:
                pl.when(self.places[axis] == 0)(low)
                pl.when(self.places[axis] == self.counts[axis] - 1)(high)


def layout(number, dims):
    x, y, z = dims
    if number in REACH:
        reach = REACH[number]
        height = rows_of(y + 2 * reach)
        return EDGE, 8 - reach, height, x + 2 * EDGE, max(40, y + 24)
    if number == SHARED:
        return EDGE, 8, rows_of(y), x + 2 * EDGE, rows_of(y) + 24
    return 1, 8, rows_of(y), x + 2, rows_of(y) + 16


def below_zero(number):
    return -((FINAL[number] + 3) // 2) if number in REACH else 0


def lift_shape(number, coarse):
    low = below_zero(number)
    count = coarse[0] - 2 * low
    height = rows_of(coarse[1] - 2 * low)
    return low, count, height, count + 2, rows_of(8 + low + height + 1)


def lift(v, ox, dims, places, counts, fine, spread, centre):
    x, y, z = dims
    low, count, height, planes, tall = lift_shape(fine.number, dims)
    beyond = EDGE if fine.reach else 0
    k = signed(lax.broadcasted_iota(jnp.int32, (LANES, LANES), 0))
    f = signed(lax.broadcasted_iota(jnp.int32, (LANES, LANES), 1))
    at = places[2] * (2 * z) + f
    inside = (f >= -beyond) & (f < 2 * z + beyond) & (at >= 0) & (at < counts[2] * 2 * z)
    parent = (f + LANES) // 2 - LANES // 2
    near = parent + jnp.where((f + LANES) % 2 == 1, 1, -1)
    outside = (places[2] * z + near < 0) | (places[2] * z + near >= counts[2] * z)
    own = jnp.where((k == parent) & inside, 0.25, 0.0)
    beside = jnp.where((k == near) & inside, 0.25, 0.0)
    both = own + jnp.where(outside, -own, beside)
    matrix = jnp.concatenate([own, both], axis=1).astype(jnp.bfloat16)

    many = widest(planes, max(1, 832 // tall))

    def first(step):
        e = v[pl.ds(step * many + (ox + low - 1), many), pl.ds(0, tall), :]
        product = exact_dot(e.reshape(many * tall, LANES), matrix)
        at = pl.ds(step * many, many)
        spread[at] = product[:, :LANES].reshape(many, tall, LANES)
        centre[at] = product[:, LANES:].reshape(many, tall, LANES)
    loop(planes // many, first)

    group = widest(count, max(1, 256 // height))
    row = places[1] * y + row_iota(height) + low
    valid = (row >= 0) & (row < counts[1] * y) & (row_iota(height) + low < y + beyond)
    masked = beyond > 0 or y < height

    def second(step):
        for i in range(group):
            plane = step * group + i
            middle = centre[plane + 1, pl.ds(8 + low, height), :]
            ys = (spread[plane + 1, pl.ds(7 + low, height), :], spread[plane + 1, pl.ds(9 + low, height), :])
            if beyond:
                at = places[0] * x + plane + low
                here = valid & ((at >= 0) & (at < counts[0] * x))
            else:
                here = valid
            for up_x in range(2):
                xs = middle + spread[plane + 2 * up_x, pl.ds(8 + low, height), :]
                for up_y in range(2):
                    q = xs + ys[up_y]
                    if masked:
                        q = jnp.where(here, q, 0.0)
                    at = (2 * (plane + low) + up_x + fine.ox, pl.ds(8 + 2 * low + up_y, height, stride=2), slice(None))
                    fine.v[at] = fine.v[at] + q
    loop(count // group, second)


class Ring:
    def __init__(self, level, refs, sems):
        self.level, self.sems = level, sems
        self.body, self.parts = refs[0], refs[1:-len(WAYS)]
        self.got = dict(zip(WAYS, refs[-len(WAYS):]))
        self.places, self.counts = level.places, level.counts

    @staticmethod
    def sizes(n):
        each = LANES // n
        cut = n if n <= 16 else 8
        return each, max(1, n // each), cut, LANES // cut, max(1, n * cut // LANES)

    @staticmethod
    def shape(n, way):
        _, groups, _, _, cuts = Ring.sizes(n)
        return (1 if way[0] else cuts if way[2] else groups, 8 if way[1] else n, LANES)

    def exists(self, way, sign):
        found = None
        for axis in range(3):
            if way[axis]:
                other = self.places[axis] + sign * way[axis]
                one = (other >= 0) if sign * way[axis] < 0 else (other < self.counts[axis])
                found = one if found is None else found & one
        return found

    def clear(self):
        for way in WAYS:
            @pl.when(jnp.logical_not(self.exists(way, -1)))
            def _(way=way):
                self.got[way][...] = jnp.zeros_like(self.got[way])

    def copy(self, way):
        n = self.level.dims[0]
        shape = Ring.shape(n, way)
        source = self.body
        if way[2] and self.parts:
            source = self.parts[0] if way[2] < 0 else self.parts[1]
        groups = source.shape[0]
        group = 0 if way[0] <= 0 else groups - 1
        row = 0 if way[1] <= 0 else n - 8
        k = WAYS.index(way)
        return pltpu.make_async_remote_copy(
            src_ref=source.at[pl.ds(group, shape[0]), pl.ds(row, shape[1])], dst_ref=self.got[way],
            send_sem=self.sems[0].at[k], recv_sem=self.sems[1].at[k],
            device_id={name: self.places[axis] + way[axis] for axis, name in enumerate(AXES) if way[axis]}, device_id_type=MESH)

    def post(self):
        n, s = self.level.dims[0], self.level.s
        each, groups, cut, cuts_each, cuts = Ring.sizes(n)
        plane = lambda x: s[EDGE + x, pl.ds(8, n), :]
        for g in range(groups):
            value = plane(g * each)
            for i in range(1, min(each, n)):
                value = value + turn(plane(g * each + i), i * n)
            self.body[g] = value
        if self.parts:
            lane = lane_iota(n)
            for g in range(cuts):
                low = high = jnp.zeros((n, LANES), jnp.float32)
                for i in range(cuts_each):
                    moved = turn(plane(g * cuts_each + i), cut * i)
                    low = jnp.where(lane // cut == i, moved, low)
                    high = jnp.where((lane + (LANES - n + cut)) % LANES // cut == i, moved, high)
                self.parts[0][g] = low
                self.parts[1][g] = high
        for way in WAYS:
            pl.when(self.exists(way, 1))(self.copy(way).start)

    def land(self):
        n, s, reach = self.level.dims[0], self.level.s, self.level.reach
        each, groups, cut, cuts_each, cuts = Ring.sizes(n)
        for way in WAYS:
            pl.when(self.exists(way, -1))(self.copy(way).wait_recv)
        for to_x, to_y in itertools.product((-1, 0, 1), repeat=2):
            height = 8 if to_y else n
            row = {-1: 0, 0: 8, 1: 8 + n}[to_y]
            lane = lane_iota(height)
            body = self.got[(-to_x, -to_y, 0)] if to_x or to_y else None
            high = self.got[(-to_x, -to_y, -1)]
            low = self.got[(-to_x, -to_y, 1)]
            for x in {-1: range(n - reach, n), 0: range(n), 1: range(reach)}[to_x]:
                at = (EDGE + to_x * n + x, pl.ds(row, height), slice(None))
                g, h = x // each, x // cuts_each
                if to_x < 0:
                    g, h = g - (groups - 1), h - (cuts - 1)
                near = turn(body[g], -(x % each) * n) if body is not None else s[at]
                above = turn(high[h], n - cut * (x % cuts_each))
                under = turn(low[h], -n - cut * (x % cuts_each))
                s[at] = jnp.where(lane < n, near, jnp.where(lane < 64, above, under))

    def finish(self):
        for way in WAYS:
            pl.when(self.exists(way, 1))(self.copy(way).wait_send)


def solve_kernel(counts, blocks, coarse, refs):
    right_side, guess, out_v, out_r = refs[:4]
    refs = list(refs[4:])
    take = lambda count=1: [refs.pop(0) for _ in range(count)] if count > 1 else refs.pop(0)
    places = tuple(lax.axis_index(axis) for axis in AXES)
    levels = []
    for number in range(LEVELS):
        if number < SHARED:
            levels.append(Grid(number, blocks[number], places, counts, *take(4)))
        else:
            levels.append(Grid(number, coarse[number - SHARED], (0, 0, 0), (1, 1, 1), *take(4)))
    exchange = take(5)
    rings = {}
    for number in REACH:
        n = blocks[number][0]
        members = take(1 + (2 if Ring.sizes(n)[2] != n else 0) + len(WAYS))
        rings[number] = Ring(levels[number], members, take(2))
    pairs = take(LEVELS - 1)
    spreads = take(LEVELS - 1)
    centres = take(LEVELS - 1)
    block_s, block_v, packet, line, joined, packets, line_send, line_recv, gather_send, gather_recv = refs

    barrier = pltpu.get_barrier_semaphore()
    nx, ny, nz = counts

    def greet(device):
        pl.semaphore_signal(barrier, inc=1, device_id=device, device_id_type=MESH)

    def greet_plane(offset, carry):
        other = lax.rem(places[0] * ny + places[1] + offset, nx * ny)
        greet({AXES[0]: other // ny, AXES[1]: other % ny})
        return carry
    lax.fori_loop(1, nx * ny, greet_plane, 0)
    for offset in range(1, nz):
        greet({AXES[2]: lax.rem(places[2] + offset, nz)})
    skew = [way for way in WAYS if way[2] and (way[0] or way[1])]
    for way in skew:
        @pl.when(rings[1].exists(way, 1))
        def _(way=way):
            greet({name: places[axis] + way[axis] for axis, name in enumerate(AXES) if way[axis]})

    for level in levels:
        level.prepare()
    for ring in rings.values():
        ring.clear()
    block_v[...] = jnp.zeros_like(block_v)
    face = exchange[4]
    face[...] = jnp.zeros_like(face)
    z0 = blocks[0][2]
    top = levels[0]

    def load(x):
        top.v[x + 1, pl.ds(8, top.rows), pl.ds(0, z0)] = guess[x]
        top.s[x] = jnp.concatenate([right_side[x], jnp.zeros((top.rows, LANES - z0), jnp.float32)], axis=1)
    loop(blocks[0][0] // 4, lambda step: [load(4 * step + i) for i in range(4)])

    near = [jnp.where(place > 0, 1, 0) + jnp.where(place < count - 1, 1, 0) for place, count in zip(places, counts)]
    pl.semaphore_wait(barrier, nx * ny + nz - 2 + near[2] * ((near[0] + 1) * (near[1] + 1) - 1))
    turns = [0]
    sent = []

    def swap():
        level = top
        out, into, send, recv, face = exchange
        n, v, (x, y, z) = turns[0], level.v, level.dims
        turns[0] += 1

        def folded(value):
            half = value.shape[0] // 2
            return jnp.where(lane_iota(half) < 64, value[:half], pltpu.roll(value[half:], 64, 1))

        def unfolded(value):
            low = lane_iota(value.shape[0]) < 64
            return jnp.concatenate([jnp.where(low, value, 0.0), jnp.where(low, pltpu.roll(value, 64, 1), 0.0)], axis=0)
        halves = (y // 2, y // 2, x // 2, x // 2, y, y)
        out[n, 0, pl.ds(0, y // 2)] = folded(v[x, pl.ds(8, y), :])
        out[n, 1, pl.ds(0, y // 2)] = folded(v[1, pl.ds(8, y), :])
        out[n, 2, pl.ds(0, x // 2)] = folded(v[pl.ds(1, x), 7 + y, :])
        out[n, 3, pl.ds(0, x // 2)] = folded(v[pl.ds(1, x), 8, :])
        lane = lane_iota(y)
        many = min(x, 16)

        def columns(step, carry):
            last, leading = carry
            for i in range(many):
                plane = step * many + i
                c = v[plane + 1, pl.ds(8, y), :]
                turned = pltpu.roll(c, plane + 64, 1)
                last = jnp.where(lane == (plane + 63 + z) % LANES, turned, last)
                leading = jnp.where(lane == plane + 64, turned, leading)
            return last, leading
        zero = jnp.zeros((y, LANES), jnp.float32)
        last, leading = lax.fori_loop(0, x // many, columns, (zero, zero))
        out[n, 4, pl.ds(0, y)] = last
        out[n, 5, pl.ds(0, y)] = leading

        copies = []
        for axis in range(3):
            for way in range(2):
                side = 2 * axis + way
                other = places[axis] + (1 - 2 * way)
                copy = pltpu.make_async_remote_copy(
                    src_ref=out.at[n, side, pl.ds(0, halves[side])], dst_ref=into.at[n, side, pl.ds(0, halves[side])],
                    send_sem=send.at[n, side], recv_sem=recv.at[n, side],
                    device_id={AXES[axis]: other}, device_id_type=MESH)
                has_target = other < counts[axis] if way == 0 else other >= 0
                has_origin = places[axis] > 0 if way == 0 else places[axis] < counts[axis] - 1
                pl.when(has_target)(copy.start)
                sent.append((has_target, copy))
                copies.append((has_origin, copy))

        def land(side):
            got = into.at[n, side]
            if side == 0:
                v[0, pl.ds(8, y), :] = unfolded(got[pl.ds(0, y // 2)])
            elif side == 1:
                v[x + 1, pl.ds(8, y), :] = unfolded(got[pl.ds(0, y // 2)])
            elif side == 2:
                v[pl.ds(1, x), 7, :] = unfolded(got[pl.ds(0, x // 2)])
            elif side == 3:
                v[pl.ds(1, x), 8 + y, :] = unfolded(got[pl.ds(0, x // 2)])
            elif side == 4:
                face[...] = jnp.where(lane < 64, pltpu.roll(got[pl.ds(0, y)], (65 - z) % LANES, 1), face[...])
            else:
                face[...] = jnp.where(lane >= 64, got[pl.ds(0, y)], face[...])
        for side, (has_origin, copy) in enumerate(copies):
            @pl.when(has_origin)
            def _(side=side, copy=copy):
                copy.wait_recv()
                land(side)
        return face

    top.sweep(0, swap())
    top.sweep(1, swap())
    top.restrict_to(levels[1].s, (EDGE, 8), pairs[0], swap())
    for number in range(1, SHARED):
        level = levels[number]
        rings[number].post()
        rings[number].land()
        level.sweep(0, zero=True, beyond=level.reach)
        level.sweep(1, beyond=level.reach)
        if number + 1 < SHARED:
            level.restrict_to(levels[number + 1].s, (EDGE, 8), pairs[number])
        else:
            level.restrict_to(block_s, (0, 0), pairs[number])

    bx, by, bz = blocks[SHARED]
    wide = LANES // bx
    packed = jnp.zeros((rows_of(by), LANES), jnp.float32)
    for x in range(bx):
        packed = packed + pltpu.roll(block_s[x], x * wide + places[2] * bz, 1)
    packet[...] = packed[:by]

    def line_copy(source, target):
        return pltpu.make_async_remote_copy(
            src_ref=packet, dst_ref=line.at[source], send_sem=line_send.at[target], recv_sem=line_recv.at[source],
            device_id={AXES[2]: target}, device_id_type=MESH)

    for offset in range(1, nz):
        line_copy(places[2], lax.rem(places[2] + offset, nz)).start()
    merged = packed[:by]
    for offset in range(1, nz):
        source = lax.rem(places[2] + nz - offset, nz)
        line_copy(source, lax.rem(places[2] + offset, nz)).wait_recv()
        merged = merged + line[source]
    joined[...] = merged
    total = nx * ny
    me = places[0] * ny + places[1]

    def plane_copy(source, target):
        return pltpu.make_async_remote_copy(
            src_ref=joined, dst_ref=packets.at[source], send_sem=gather_send.at[target], recv_sem=gather_recv.at[source],
            device_id={AXES[0]: target // ny, AXES[1]: target % ny}, device_id_type=MESH)

    def post(offset, carry):
        plane_copy(me, lax.rem(me + offset, total)).start()
        return carry
    lax.fori_loop(1, total, post, 0)
    packets[me] = merged

    def arrive(offset, carry):
        plane_copy(lax.rem(me + total - offset, total), lax.rem(me + offset, total)).wait_recv()
        return carry
    lax.fori_loop(1, total, arrive, 0)
    whole = levels[SHARED]

    def unpack(px):
        for py in range(0, ny, 2):
            pair = jnp.concatenate([packets[px * ny + py], packets[px * ny + py + 1]], axis=0)
            for x in range(bx):
                whole.s[px * bx + x, pl.ds(py * by, 2 * by), :] = turn(pair, -x * wide)
    loop(nx, unpack)

    for number in range(SHARED, LEVELS - 1):
        level = levels[number]
        level.sweep(0, zero=True)
        level.sweep(1)
        level.restrict_to(levels[number + 1].s, (0, 0), pairs[number])
    level = levels[LEVELS - 1]
    level.sweep(0, zero=True)
    level.sweep(1)
    for _ in range(COARSE_SWEEPS - 1):
        level.sweep(0)
        level.sweep(1)
    for number in reversed(range(SHARED, LEVELS - 1)):
        level, below = levels[number], levels[number + 1]
        below.reflect()
        lift(below.v, below.ox, below.dims, (0, 0, 0), (1, 1, 1), level, spreads[number], centres[number])
        level.sweep(0)
        level.sweep(1)

    whole.reflect()
    shift = lax.rem(LANES - places[2] * bz, LANES)
    odd = lax.rem(places[1] + 1, 2) == 1
    for x in range(bx + 8):
        part = whole.v[places[0] * bx + (x - 4 + whole.ox), pl.ds(pl.multiple_of((places[1] + 1) // 2 * 8, 8), 24), :]
        block_v[x, pl.ds(4, 16)] = pltpu.roll(jnp.where(odd, part[4:20], part[:16]), shift, 1)
    lift(block_v, 4, blocks[SHARED], places, counts, levels[SHARED - 1], spreads[SHARED - 1], centres[SHARED - 1])
    for number in reversed(range(1, SHARED)):
        level = levels[number]
        level.sweep(0, beyond=level.reach - 2)
        level.sweep(1, beyond=level.reach - 2)
        level.reflect()
        lift(level.v, level.ox, level.dims, places, counts, levels[number - 1], spreads[number - 1], centres[number - 1])
    top.sweep(0, swap())
    top.sweep(1, swap())
    face = swap()
    chunk = widest(blocks[0][0], 32 * 8 // top.rows, 2)

    def finish(step):
        r = top.remainder(step * chunk, chunk, face)
        for i in range(chunk):
            at = step * chunk + i
            out_r[at] = r[i][:, :z0]
            out_v[at] = top.v[at + 1, pl.ds(8, top.rows), pl.ds(0, z0)]
    loop(blocks[0][0] // chunk, finish)

    for has_target, copy in sent:
        pl.when(has_target)(copy.wait_send)
    for ring in rings.values():
        ring.finish()
    for offset in range(1, nz):
        line_copy(places[2], lax.rem(places[2] + offset, nz)).wait_send()

    def leave(offset, carry):
        plane_copy(me, lax.rem(me + offset, total)).wait_send()
        return carry
    lax.fori_loop(1, total, leave, 0)


def solution(mesh):
    counts = tuple(mesh.shape[axis] for axis in AXES)

    def per_device(right_side, guess):
        shape = right_side.shape
        blocks = [tuple(side >> level for side in shape) for level in range(SHARED + 1)]
        whole = tuple(side * count for side, count in zip(blocks[SHARED], counts))
        coarse = [tuple(side >> level for side in whole) for level in range(LEVELS - SHARED)]
        grids = blocks[:SHARED] + coarse
        scratch = []
        vmem = lambda *dims: scratch.append(pltpu.VMEM(dims, jnp.float32))
        sems = lambda *dims: scratch.append(pltpu.SemaphoreType.DMA(dims))
        for number, (x, y, z) in enumerate(grids):
            _, _, height, planes, tall = layout(number, (x, y, z))
            vmem(planes, tall, LANES)
            if number in REACH:
                vmem(planes, tall, LANES)
            else:
                vmem(x, rows_of(y), LANES)
            vmem(3, height, LANES)
            vmem(2, rows_of(y), LANES)
        x, y, z = blocks[0]
        side = max(x, y)
        vmem(6, 6, side, LANES)
        vmem(6, 6, side, LANES)
        sems(6, 6)
        sems(6, 6)
        vmem(y, LANES)
        for number in REACH:
            n = blocks[number][0]
            _, groups, cut, _, cuts = Ring.sizes(n)
            vmem(groups, n, LANES)
            if cut != n:
                vmem(cuts, n, LANES)
                vmem(cuts, n, LANES)
            for way in WAYS:
                vmem(*Ring.shape(n, way))
            sems(len(WAYS))
            sems(len(WAYS))
        for x, y, z in grids[:-1]:
            vmem(x // 2, max(16, y), LANES)
        for _ in range(2):
            for number in range(LEVELS - 1):
                _, _, _, planes, tall = lift_shape(number, blocks[number + 1] if number < SHARED else grids[number + 1])
                vmem(planes, tall, LANES)
        bx, by, bz = blocks[SHARED]
        vmem(bx, rows_of(by), LANES)
        vmem(bx + 8, 24, LANES)
        vmem(by, LANES)
        vmem(counts[2], by, LANES)
        vmem(by, LANES)
        total = counts[0] * counts[1]
        vmem(total, by, LANES)
        for many in (counts[2], counts[2], total, total):
            sems(many)

        def kernel(*refs):
            solve_kernel(counts, blocks, coarse, refs)

        whole_block = pl.BlockSpec(memory_space=pltpu.VMEM)
        return pl.pallas_call(
            kernel,
            out_shape=(jax.ShapeDtypeStruct(shape, jnp.float32),) * 2,
            in_specs=[whole_block] * 2,
            out_specs=(whole_block,) * 2,
            scratch_shapes=scratch,
            compiler_params=pltpu.CompilerParams(collective_id=0, has_side_effects=True, vmem_limit_bytes=60 * 2**20),
            name="vcycle",
        )(right_side, guess)

    spec = P(*AXES)
    return jax.shard_map(per_device, mesh=mesh, in_specs=(spec, spec), out_specs=(spec, spec), check_vma=False)
```

```python
import itertools

import jax
import jax.numpy as jnp
from jax import lax
from jax.experimental import pallas as pl
from jax.experimental.pallas import tpu as pltpu
from jax.sharding import PartitionSpec as P

LEVELS = 7
COARSE_SWEEPS = 4
SHARED = 4
VMEM_LIMIT = 32
LANES = 128
EDGE = 8
AXES = ("gx", "gy", "gz")
MESH = pl.DeviceIdType.MESH
WAYS = [way for way in itertools.product((-1, 0, 1), repeat=3) if any(way)]
FINAL = {0: 1, 1: 2, 2: 3, 3: 3}
REACH = {level: FINAL[level] + 3 for level in range(1, SHARED)}


def rows_of(count):
    return max(8, -(-count // 8) * 8)


def lane_iota(rows):
    return lax.broadcasted_iota(jnp.int32, (rows, LANES), 1)


def row_iota(rows):
    return lax.broadcasted_iota(jnp.int32, (rows, LANES), 0)


def loop(count, body):
    if count == 1:
        body(0)
    else:
        def step(i, carry):
            body(i)
            return carry
        lax.fori_loop(0, count, step, 0)


def turn(value, amount):
    amount = amount % LANES
    return pltpu.roll(value, amount, 1) if amount else value


def exact_dot(value, matrix):
    first = value.astype(jnp.bfloat16)
    rest = value - first.astype(jnp.float32)
    second = rest.astype(jnp.bfloat16)
    third = (rest - second.astype(jnp.float32)).astype(jnp.bfloat16)
    dot = lambda part: jnp.dot(part, matrix, preferred_element_type=jnp.float32)
    return (dot(third) + dot(second)) + dot(first)


def widest(count, most, step=1):
    return max(size for size in range(step, count + 1, step) if count % size == 0 and (size <= most or size == step))


def signed(lane):
    return jnp.where(lane < 96, lane, lane - LANES)


class Grid:
    def __init__(self, number, dims, places, counts, v, s, w, d):
        self.number, self.dims, self.places, self.counts = number, dims, places, counts
        self.v, self.s, self.w, self.d = v, s, w, d
        self.reach = REACH.get(number, 0)
        self.ox, self.start, self.height, _, _ = layout(number, dims)
        self.sx, self.sy = (EDGE, 8) if self.reach else (0, 0)
        self.rows = rows_of(dims[1])

    def prepare(self):
        x, y, z = self.dims
        beyond = EDGE if self.reach else 0

        def base(height, start):
            row, lane = row_iota(height) + (start - 8), signed(lane_iota(height))
            at_y, at_z = self.places[1] * y + row, self.places[2] * z + lane
            last_y, last_z = self.counts[1] * y - 1, self.counts[2] * z - 1
            valid = (lane >= -beyond) & (lane < z + beyond) & (row >= -beyond) & (row < y + beyond)
            valid = valid & (at_y >= 0) & (at_y <= last_y) & (at_z >= 0) & (at_z <= last_z)
            one = lambda at, last: (at == 0).astype(jnp.float32) + (at == last).astype(jnp.float32)
            return valid, 6.0 + one(at_y, last_y) + one(at_z, last_z)
        valid, diagonal = base(self.w.shape[1], self.start)
        for wall in range(2):
            self.w[wall] = jnp.where(valid, 1.0 / (diagonal + wall), 0.0)
        self.w[2] = jnp.zeros_like(diagonal)
        valid, diagonal = base(self.rows, 8)
        for wall in range(2):
            self.d[wall] = jnp.where(valid, diagonal + wall, 0.0)
        self.v[...] = jnp.zeros_like(self.v)
        if self.reach:
            self.s[...] = jnp.zeros_like(self.s)

    def wall(self, plane, beyond=False):
        at = self.places[0] * self.dims[0] + plane
        last = self.counts[0] * self.dims[0] - 1
        if isinstance(at, int):
            return int(at in (0, last))
        kind = jnp.where((at == 0) | (at == last), 1, 0)
        return jnp.where((at < 0) | (at > last), 2, kind) if beyond else kind

    def total(self, plane, count, start, height):
        at = plane + self.ox
        slab = self.v[pl.ds(at - 1, count + 2), pl.ds(start, height), :]
        centre = slab[1:-1]
        total = slab[2:] + slab[:-2]
        total = total + self.v[pl.ds(at, count), pl.ds(start + 1, height), :] + self.v[pl.ds(at, count), pl.ds(start - 1, height), :]
        out = []
        for i in range(count):
            c = centre[i]
            out.append(total[i] + (pltpu.roll(c, 1, 1) + pltpu.roll(c, LANES - 1, 1)))
        return out, [centre[i] for i in range(count)]

    def sweep(self, colour, zero=False, beyond=0):
        start, height = self.start, self.height
        if self.reach and not zero:
            start, height = start + 1, inner_height(self.number, self.dims)
        planes = self.dims[0] + 2 * beyond
        chunk = widest(planes, 112 * 8 // height, 2)
        parity = (row_iota(height) + lane_iota(height) + start) % 2

        def body(step):
            first = step * chunk - beyond
            if not zero:
                totals, centres = self.total(first, chunk, start, height)
            results = []
            for i in range(chunk):
                weight = self.w[self.wall(first + i, beyond > 0), pl.ds(start - self.start, height), :]
                given = self.s[first + i + self.sx, pl.ds(start - 8 + self.sy, height), :]
                mine = parity == (i + colour + beyond) % 2
                if zero:
                    results.append(jnp.where(mine, given * weight, 0.0))
                else:
                    results.append(jnp.where(mine, (given + totals[i]) * weight, centres[i]))
            for i in range(chunk):
                self.v[first + i + self.ox, pl.ds(start, height), :] = results[i]
        loop(planes // chunk, body)

    def remainder(self, first, chunk):
        totals, centres = self.total(first, chunk, 8, self.rows)
        out = []
        for i in range(chunk):
            d = self.d[self.wall(first + i)]
            r = self.s[first + i + self.sx, pl.ds(self.sy, self.rows), :] - (d * centres[i] - totals[i])
            out.append(r if self.dims[1] == self.rows else jnp.where(d > 0, r, 0.0))
        return out

    def restrict_to(self, target, corner, pairs):
        rows = self.rows
        chunk = widest(self.dims[0], 32 * 8 // rows, 2)
        half = chunk // 2
        if rows < 16:
            pairs[...] = jnp.zeros_like(pairs)

        def first(step):
            r = self.remainder(step * chunk, chunk)
            for i in range(half):
                pairs[step * half + i, pl.ds(0, rows), :] = r[2 * i] + r[2 * i + 1]
        loop(self.dims[0] // chunk, first)
        narrow(self.dims, target, corner, pairs)

    def reflect(self):
        (x, y, z), v, ox = self.dims, self.v, self.ox
        margin = 3 if self.reach else 0
        for_all = pl.ds(ox - margin, x + 2 * margin)

        def low_x():
            v[ox - 1] = -v[ox]

        def high_x():
            v[ox + x] = -v[ox + x - 1]

        def low_y():
            v[for_all, pl.ds(7, 1), :] = -v[for_all, pl.ds(8, 1), :]

        def high_y():
            v[for_all, pl.ds(8 + y, 1), :] = -v[for_all, pl.ds(7 + y, 1), :]

        for axis, low, high in ((0, low_x, high_x), (1, low_y, high_y)):
            if isinstance(self.counts[axis], int) and isinstance(self.places[axis], int):
                low()
                high()
            else:
                pl.when(self.places[axis] == 0)(low)
                pl.when(self.places[axis] == self.counts[axis] - 1)(high)


def narrow(dims, target, corner, pairs):
    x, y, z = dims
    coarse_rows = rows_of(y // 2)
    source_lane = lax.broadcasted_iota(jnp.int32, (LANES, LANES), 0)
    target_lane = lax.broadcasted_iota(jnp.int32, (LANES, LANES), 1)
    halve = jnp.where((source_lane // 2 == target_lane) & (source_lane < z), 0.5, 0.0).astype(jnp.bfloat16)
    planes = x // 2
    many = min(planes, max(1, 256 // coarse_rows))

    def second(step):
        at = pl.ds(step * many, many)
        q = pairs[at, pl.ds(0, coarse_rows, stride=2), :] + pairs[at, pl.ds(1, coarse_rows, stride=2), :]
        q = exact_dot(q.reshape(many * coarse_rows, LANES), halve)
        target[pl.ds(step * many + corner[0], many), pl.ds(corner[1], coarse_rows), :] = q.reshape(many, coarse_rows, LANES)
    loop(planes // many, second)


def layout(number, dims):
    x, y, z = dims
    if number in REACH:
        reach = REACH[number]
        height = rows_of(y + 2 * reach)
        return EDGE, 8 - reach, height, x + 2 * EDGE, max(40, y + 24)
    if number == SHARED:
        return EDGE, 8, rows_of(y), x + 2 * EDGE, rows_of(y) + 24
    return 1, 8, rows_of(y), x + 2, rows_of(y) + 16


def inner_height(number, dims):
    return rows_of(dims[1] + 2 * REACH[number] - 2)


def below_zero(number):
    return -((FINAL[number] + 3) // 2) if number in FINAL else 0


def lift_shape(number, coarse):
    low = below_zero(number)
    count = coarse[0] - 2 * low
    height = rows_of(coarse[1] - 2 * low)
    return low, count, height, count + 2, rows_of(8 + low + height + 1)


def widen(v, ox, dims, places, counts, number, spread, centre):
    z = dims[2]
    low, count, height, planes, tall = lift_shape(number, dims)
    beyond = EDGE if number in FINAL else 0
    k = signed(lax.broadcasted_iota(jnp.int32, (LANES, LANES), 0))
    f = signed(lax.broadcasted_iota(jnp.int32, (LANES, LANES), 1))
    at = places[2] * (2 * z) + f
    inside = (f >= -beyond) & (f < 2 * z + beyond) & (at >= 0) & (at < counts[2] * 2 * z)
    parent = (f + LANES) // 2 - LANES // 2
    near = parent + jnp.where((f + LANES) % 2 == 1, 1, -1)
    outside = (places[2] * z + near < 0) | (places[2] * z + near >= counts[2] * z)
    own = jnp.where((k == parent) & inside, 0.25, 0.0)
    beside = jnp.where((k == near) & inside, 0.25, 0.0)
    both = own + jnp.where(outside, -own, beside)
    matrix = jnp.concatenate([own, both], axis=1).astype(jnp.bfloat16)
    many = widest(planes, max(1, 1024 // tall))

    def first(step):
        e = v[pl.ds(step * many + (ox + low - 1), many), pl.ds(0, tall), :]
        product = exact_dot(e.reshape(many * tall, LANES), matrix)
        at = pl.ds(step * many, many)
        spread[at] = product[:, :LANES].reshape(many, tall, LANES)
        centre[at] = product[:, LANES:].reshape(many, tall, LANES)
    loop(planes // many, first)


def lift(v, ox, dims, places, counts, fine, spread, centre):
    x, y, z = dims
    number = fine.number
    low, count, height, planes, tall = lift_shape(number, dims)
    beyond = EDGE if number in FINAL else 0
    widen(v, ox, dims, places, counts, number, spread, centre)
    group = widest(count, max(1, 256 // height))
    row = places[1] * y + row_iota(height) + low
    valid = (row >= 0) & (row < counts[1] * y)
    if not beyond:
        valid = row_iota(height) < y
    masked = beyond > 0 or y < height
    even = lane_iota(height) % 2 == 0

    def second(step):
        for i in range(group):
            plane = step * group + i
            middle = centre[plane + 1, pl.ds(8 + low, height), :]
            ys = (spread[plane + 1, pl.ds(7 + low, height), :], spread[plane + 1, pl.ds(9 + low, height), :])
            xs = [spread[plane + 2 * up_x, pl.ds(8 + low, height), :] for up_x in range(2)]
            here = valid
            if beyond:
                at = places[0] * x + plane + low
                here = valid & ((at >= 0) & (at < counts[0] * x))
            for up_y in range(2):
                rows = pl.ds(8 + 2 * low + up_y, height, stride=2)
                middle_y = middle + ys[up_y]
                if number == 0:
                    q = middle_y + jnp.where(even, xs[1 - up_y], xs[up_y])
                    q = jnp.where(here, q, 0.0)
                    at = (plane + low + fine.ox, rows, slice(None))
                    fine.b[at] = fine.b[at] + q
                    continue
                for up_x in range(2):
                    q = middle_y + xs[up_x]
                    if masked:
                        q = jnp.where(here, q, 0.0)
                    at = (2 * (plane + low) + up_x + fine.ox, rows, slice(None))
                    fine.v[at] = fine.v[at] + q
    loop(count // group, second)


def exists(places, counts, way, sign):
    found = None
    for axis in range(3):
        if way[axis]:
            other = places[axis] + sign * way[axis]
            one = (other >= 0) if sign * way[axis] < 0 else (other < counts[axis])
            found = one if found is None else found & one
    return found


def along(places, way):
    return {name: places[axis] + way[axis] for axis, name in enumerate(AXES) if way[axis]}


class Top:
    number, ox, sets = 0, 2, 4

    def __init__(self, dims, places, counts, r, b, gr, gb, w, d, out, got, sems):
        self.dims, self.places, self.counts = dims, places, counts
        self.r, self.b, self.gr, self.gb, self.w, self.d = r, b, gr, gb, w, d
        self.out, self.got, self.sems = out, got, sems
        self.pairs, self.n = dims[0] // 2, dims[1]

    @staticmethod
    def weights(dims, places, counts, height, start, beyond):
        x, y, z = dims
        row, lane = row_iota(height) + (start - 8), signed(lane_iota(height))
        at_y, at_z = places[1] * y + row, places[2] * z + lane
        last_y, last_z = counts[1] * y - 1, counts[2] * z - 1
        valid = (lane >= -beyond) & (lane < z + beyond) & (at_y >= 0) & (at_y <= last_y) & (at_z >= 0) & (at_z <= last_z)
        one = lambda at, last: (at == 0).astype(jnp.float32) + (at == last).astype(jnp.float32)
        return valid, 6.0 + one(at_y, last_y) + one(at_z, last_z), (row + lane + LANES) % 2 == 0

    def clear(self):
        for ref in (self.r, self.b, self.gr, self.gb):
            ref[...] = jnp.zeros_like(ref)

    def prepare(self):
        valid, diagonal, even = self.weights(self.dims, self.places, self.counts, self.n + 8, 6, 4)
        plain, more = (jnp.where(valid, 1.0 / (diagonal + wall), 0.0) for wall in range(2))
        self.w[0] = plain
        self.w[1] = jnp.where(even, more, plain)
        self.w[2] = jnp.where(even, plain, more)
        self.w[3] = jnp.zeros_like(plain)
        write_diagonals(self.d, self.dims, self.places, self.counts)

    def missing(self):
        for way in WAYS:
            @pl.when(jnp.logical_not(exists(self.places, self.counts, way, -1)))
            def _(way=way):
                self.got[way][...] = jnp.zeros_like(self.got[way])

    def kind(self, pair):
        at = self.places[0] * self.pairs + pair
        last = self.counts[0] * self.pairs - 1
        return jnp.where((at < 0) | (at > last), 3, jnp.where(at == 0, 1, jnp.where(at == last, 2, 0)))

    def sweep(self, colour):
        start, height = 6, self.n + 8
        source, target, given = (self.r, self.b, self.gb) if colour else (self.b, self.r, self.gr)
        count = self.pairs + 2
        chunk = widest(count, 17)
        even = (row_iota(height) + lane_iota(height)) % 2 == 0

        def body(step):
            for i in range(chunk):
                k = step * chunk + i - 1
                at = k + 2
                total = around(source, at, start, height, even, colour)
                kind = self.kind(k)
                if colour:
                    kind = jnp.where(kind == 1, 2, jnp.where(kind == 2, 1, kind))
                target[at, pl.ds(start, height), :] = (given[at, pl.ds(start, height), :] + total) * self.w[kind]
        loop(count // chunk, body)

    def restrict_to(self, target, corner, pairs):
        n = self.n
        even = (row_iota(n) + lane_iota(n)) % 2 == 0
        chunk = 4

        def body(step):
            for i in range(chunk):
                k = step * chunk + i
                red, black = remainders(self.r, self.b, self.gr, self.gb, self.d, k + 2, self.kind(k), even, n)
                pairs[k] = red + black
        loop(self.pairs // chunk, body)
        narrow(self.dims, target, corner, pairs)

    @staticmethod
    def shapes(n):
        face = {0: (2, n, LANES), 1: (n // 4, 8, LANES), 2: (3, n, LANES)}
        sent = [face[0], face[0], face[1], face[1], face[2], face[2], (4, 8, LANES)]
        got = {}
        for way in WAYS:
            if sum(map(abs, way)) == 1:
                got[way] = face[[abs(part) for part in way].index(1)]
            elif not way[2]:
                got[way] = (2, 8, LANES)
            elif not way[0]:
                got[way] = (2, 8, LANES)
            else:
                got[way] = (8, LANES)
        return sent, got

    def copies(self, way, again):
        n, out, got = self.n, self.out, self.got[way]
        high = [part > 0 for part in way]
        if sum(map(abs, way)) == 1:
            axis = [abs(part) for part in way].index(1)
            source = out[2 * axis + high[axis]]
            if again and axis != 1:
                source, got = source.at[pl.ds(0, 1)], got.at[pl.ds(0, 1)]
        elif not way[2]:
            source = out[2 + high[1]].at[pl.ds(n // 4 - 2 if high[0] else 0, 2)]
        elif not way[0]:
            row = pl.ds(n - 8 if high[1] else 0, 8)
            source = out[4 + high[2]].at[pl.ds(0, 2), row]
        else:
            source = out[6].at[2 * high[0] + high[2]]
        k = WAYS.index(way)
        return pltpu.make_async_remote_copy(
            src_ref=source, dst_ref=got, send_sem=self.sems[0].at[k], recv_sem=self.sems[1].at[k],
            device_id=along(self.places, way), device_id_type=MESH)

    def pack(self, again):
        n, pairs = self.n, self.pairs
        arrays = [self.b] if again else [self.b, self.gr, self.gb]
        low, tile = lane_iota(n) < 64, lane_iota(8)
        row = row_iota(8)
        half = pairs // 2
        own = lambda ref, k: ref[k + 2, pl.ds(8, n), :]
        for high in range(2):
            near, far = (pairs - 1, pairs - 2) if high else (0, 1)
            self.out[high][0] = jnp.where(low, own(self.b, near), pltpu.roll(own(self.b, far), 64, 1))
            if not again:
                self.out[high][1] = jnp.where(low, own(self.gr, near), pltpu.roll(own(self.gb, near), 64, 1))

            def edge(k, high=high):
                first = 8 + n - 8 if high else 8
                b = self.b[k + 2, pl.ds(first, 8), :]
                if again:
                    return b
                red, black = (pltpu.roll(ref[k + 2, pl.ds(first, 8), :], by, 0) for ref, by in ((self.gr, 4), (self.gb, 2 if high else 6)))
                if high:
                    return jnp.where(row >= 4, b, jnp.where(row >= 2, red, black))
                return jnp.where(row < 4, b, jnp.where(row < 6, red, black))
            for k in range(half):
                self.out[2 + high][k] = jnp.where(tile < 64, edge(k), pltpu.roll(edge(k + half), 64, 1))
        for index, ref in enumerate(arrays):
            def body(t, ref=ref, index=index):
                at = pl.ds(pl.multiple_of(t * 16, 16), 16)
                lane = lane_iota(16)
                ahead = (lane + (LANES - 60)) % LANES
                first = last = jnp.zeros((16, LANES), jnp.float32)
                for k in range(pairs):
                    moved = turn(ref[k + 2, pl.ds(pl.multiple_of(t * 16 + 8, 8), 16), :], 4 * k)
                    first = jnp.where(lane // 4 == k, moved, first)
                    last = jnp.where(ahead // 4 == k, moved, last)
                self.out[4][index, at] = first
                self.out[5][index, at] = last
            loop(n // 16, body)
        for high_x in range(2):
            for high_z in range(2):
                offset = 60 if high_z else 0
                pair, near = (pairs - 2, pairs - 1) if high_x else (0, 0)
                value = jnp.zeros((8, LANES), jnp.float32)
                for t in range(n // 8):
                    rows = pl.ds(8 * t, 8)
                    moved = turn(self.out[4 + high_z][0, rows], 16 * t - 4 * pair - offset)
                    value = jnp.where((tile >= 16 * t) & (tile < 16 * t + 8), moved, value)
                    if not again:
                        moved = turn(self.out[4 + high_z][1, rows], 16 * t + 8 - 4 * near - offset)
                        value = jnp.where((tile >= 16 * t + 8) & (tile < 16 * t + 16), moved, value)
                self.out[6][2 * high_x + high_z] = value

    def post(self, again=False):
        self.pack(again)
        self.send(again)

    def send(self, again=False):
        for way in WAYS:
            pl.when(exists(self.places, self.counts, way, 1))(self.copies(way, again).start)

    def sent(self, again=False):
        for way in WAYS:
            pl.when(exists(self.places, self.counts, way, 1))(self.copies(way, again).wait_send)

    def land(self, again=False):
        n, pairs, got = self.n, self.pairs, self.got
        half = pairs // 2
        for way in WAYS:
            pl.when(exists(self.places, self.counts, way, -1))(self.copies(way, again).wait_recv)
        arrays = [self.b] if again else [self.b, self.gr, self.gb]
        lane, tile = lane_iota(n), lane_iota(8)

        def ends(high, low, to, k):
            pick = to % 8 < 4
            return turn(jnp.where(pick, high, low) if k % 2 == 0 else jnp.where(pick, low, high), 64 - 4 * k)
        for index, ref in enumerate(arrays):
            high, low = got[(0, 0, -1)], got[(0, 0, 1)]

            def body(t, ref=ref, index=index, high=high, low=low):
                at = pl.ds(pl.multiple_of(t * 16, 16), 16)
                to = lane_iota(16)
                h, l = high[index, at], low[index, at]
                for k in range(pairs):
                    own = (k + 2, pl.ds(pl.multiple_of(t * 16 + 8, 8), 16), slice(None))
                    ref[own] = jnp.where(to < 64, ref[own], ends(h, l, to, k))
            loop(n // 16, body)
        for side in (-1, 1):
            face = got[(0, -side, 0)]
            base = 8 + n if side > 0 else 0
            shifts = (0, 4, 2 if side > 0 else 6)
            for index, ref in enumerate(arrays):
                if index < 2:
                    h, l = got[(0, -side, -1)][index], got[(0, -side, 1)][index]
                for k in range(pairs):
                    value = face[k % half]
                    if k >= half:
                        value = pltpu.roll(value, 64, 1)
                    if shifts[index]:
                        value = pltpu.roll(value, shifts[index], 0)
                    if index < 2:
                        value = jnp.where(tile < 64, value, ends(h, l, tile, k))
                    ref[k + 2, pl.ds(base, 8), :] = value
        for side in (-1, 1):
            face = got[(-side, 0, 0)]
            near, far = (pairs + 2, pairs + 3) if side > 0 else (1, 0)
            high, low = got[(-side, 0, -1)], got[(-side, 0, 1)]
            near_lane, far_lane = (0, 4) if side > 0 else (4, 0)

            def beside(first, at, high=high, low=low):
                out = []
                for t in at:
                    up = turn(high[...], 64 - 16 * t - first)
                    out.append(jnp.where(tile < 96, up, turn(low[...], 124 - 16 * t - first)))
                return jnp.concatenate(out, axis=0) if len(out) > 1 else out[0]
            every = range(n // 8)
            both = face[0]
            self.b[near, pl.ds(8, n), :] = jnp.where(lane < 64, both, beside(near_lane, every))
            self.b[far, pl.ds(8, n), :] = jnp.where(lane < 64, pltpu.roll(both, 64, 1), beside(far_lane, every))
            if not again:
                both = face[1]
                self.gr[near, pl.ds(8, n), :] = jnp.where(lane < 64, both, beside(8, every))
                self.gb[near, pl.ds(8, n), :] = pltpu.roll(both, 64, 1)
            for up in (-1, 1):
                edge = got[(-side, -up, 0)]
                base = 8 + n if up > 0 else 0
                corner = (got[(-side, -up, -1)], got[(-side, -up, 1)])
                t = [0 if up > 0 else n // 8 - 1]
                if side > 0:
                    pieces = {near: (0, False), far: (1, False)}
                else:
                    pieces = {near: (1, True), far: (0, True)}
                for place, (group, upper) in pieces.items():
                    value = edge[group]
                    if upper:
                        value = pltpu.roll(value, 64, 1)
                    first = near_lane if place == near else far_lane
                    self.b[place, pl.ds(base, 8), :] = jnp.where(tile < 64, value, beside(first, t, *corner))
                    if place == near and not again:
                        self.gr[place, pl.ds(base, 8), :] = pltpu.roll(value, 4, 0)


def around(source, at, start, height, even, colour):
    s = source[at, pl.ds(start, height), :]
    left, right = source[at - 1, pl.ds(start, height), :], source[at + 1, pl.ds(start, height), :]
    across = jnp.where(even, right, left) if colour else jnp.where(even, left, right)
    total = (s + across) + (source[at, pl.ds(start + 1, height), :] + source[at, pl.ds(start - 1, height), :])
    return total + (pltpu.roll(s, 1, 1) + pltpu.roll(s, LANES - 1, 1))


def remainders(r, b, gr, gb, d, at, kind, even, n):
    rows = pl.ds(8, n)
    other = jnp.where(kind == 1, 2, jnp.where(kind == 2, 1, kind))
    red = gr[at, rows, :] - (d[kind] * r[at, rows, :] - around(b, at, 8, n, even, 0))
    black = gb[at, rows, :] - (d[other] * b[at, rows, :] - around(r, at, 8, n, even, 1))
    return red, black


def write_diagonals(d, dims, places, counts):
    _, diagonal, even = Top.weights(dims, places, counts, dims[1], 8, 0)
    d[0] = diagonal
    d[1] = jnp.where(even, diagonal + 1.0, diagonal)
    d[2] = jnp.where(even, diagonal, diagonal + 1.0)


class Ring:
    def __init__(self, level, refs, sems):
        self.level, self.sems = level, sems
        self.body, self.parts = refs[0], refs[1:-len(WAYS)]
        self.got = dict(zip(WAYS, refs[-len(WAYS):]))
        self.places, self.counts = level.places, level.counts

    @staticmethod
    def sizes(n):
        each = LANES // n
        cut = n if n <= 16 else 8
        return each, max(1, n // each), cut, LANES // cut, max(1, n * cut // LANES)

    @staticmethod
    def thick(n, reach, way):
        each, groups, _, _, cuts = Ring.sizes(n)
        if not way[0]:
            return cuts if way[2] else groups
        return 1 if way[2] else -(-reach // each)

    @staticmethod
    def shape(n, reach, way):
        return (Ring.thick(n, reach, way), 8 if way[1] else n, LANES)

    def clear(self):
        for way in WAYS:
            @pl.when(jnp.logical_not(exists(self.places, self.counts, way, -1)))
            def _(way=way):
                self.got[way][...] = jnp.zeros_like(self.got[way])

    def copy(self, way):
        n = self.level.dims[0]
        shape = Ring.shape(n, self.level.reach, way)
        source = self.body
        if way[2] and self.parts:
            source = self.parts[0] if way[2] < 0 else self.parts[1]
        groups = source.shape[0]
        group = 0 if way[0] <= 0 else groups - shape[0]
        row = 0 if way[1] <= 0 else n - 8
        k = WAYS.index(way)
        return pltpu.make_async_remote_copy(
            src_ref=source.at[pl.ds(group, shape[0]), pl.ds(row, shape[1])], dst_ref=self.got[way],
            send_sem=self.sems[0].at[k], recv_sem=self.sems[1].at[k],
            device_id={name: self.places[axis] + way[axis] for axis, name in enumerate(AXES) if way[axis]}, device_id_type=MESH)

    def post(self):
        n, s = self.level.dims[0], self.level.s
        each, groups, cut, cuts_each, cuts = Ring.sizes(n)
        plane = lambda x: s[EDGE + x, pl.ds(8, n), :]
        for g in range(groups):
            value = plane(g * each)
            for i in range(1, min(each, n)):
                value = value + turn(plane(g * each + i), i * n)
            self.body[g] = value
        if self.parts:
            lane = lane_iota(n)
            for g in range(cuts):
                low = high = jnp.zeros((n, LANES), jnp.float32)
                for i in range(cuts_each):
                    moved = turn(plane(g * cuts_each + i), cut * i)
                    low = jnp.where(lane // cut == i, moved, low)
                    high = jnp.where((lane + (LANES - n + cut)) % LANES // cut == i, moved, high)
                self.parts[0][g] = low
                self.parts[1][g] = high
        for way in WAYS:
            pl.when(exists(self.places, self.counts, way, 1))(self.copy(way).start)

    def land(self):
        n, s, reach = self.level.dims[0], self.level.s, self.level.reach
        each, groups, cut, cuts_each, cuts = Ring.sizes(n)
        for way in WAYS:
            pl.when(exists(self.places, self.counts, way, -1))(self.copy(way).wait_recv)
        for to_x, to_y in itertools.product((-1, 0, 1), repeat=2):
            height = 8 if to_y else n
            row = {-1: 0, 0: 8, 1: 8 + n}[to_y]
            lane = lane_iota(height)
            body = self.got[(-to_x, -to_y, 0)] if to_x or to_y else None
            high = self.got[(-to_x, -to_y, -1)]
            low = self.got[(-to_x, -to_y, 1)]
            for x in {-1: range(n - reach, n), 0: range(n), 1: range(reach)}[to_x]:
                at = (EDGE + to_x * n + x, pl.ds(row, height), slice(None))
                g, h = x // each, x // cuts_each
                if to_x < 0:
                    g, h = g - (groups - body.shape[0]), h - (cuts - high.shape[0])
                near = turn(body[g], -(x % each) * n) if body is not None else s[at]
                above = turn(high[h], n - cut * (x % cuts_each))
                under = turn(low[h], -n - cut * (x % cuts_each))
                s[at] = jnp.where(lane < n, near, jnp.where(lane < 64, above, under))

    def finish(self):
        for way in WAYS:
            pl.when(exists(self.places, self.counts, way, 1))(self.copy(way).wait_send)


def solve_kernel(counts, blocks, coarse, refs):
    right_side, guess, r, b, gr, gb = refs[:6]
    refs = list(refs[6:])
    take = lambda count=1: [refs.pop(0) for _ in range(count)] if count > 1 else refs.pop(0)
    places = tuple(lax.axis_index(axis) for axis in AXES)
    n0 = blocks[0][0]
    raw_g, raw_v, raw_sems = take(3)
    sent_shapes, got_shapes = Top.shapes(n0)
    w0, d0 = take(2)
    top = Top(blocks[0], places, counts, r, b, gr, gb, w0, d0, take(len(sent_shapes)), dict(zip(WAYS, take(len(WAYS)))), take(2))
    levels = [top]
    for number in range(1, LEVELS):
        if number < SHARED:
            levels.append(Grid(number, blocks[number], places, counts, *take(4)))
        else:
            levels.append(Grid(number, coarse[number - SHARED], (0, 0, 0), (1, 1, 1), *take(4)))
    rings = {}
    for number in REACH:
        n = blocks[number][0]
        members = take(1 + (2 if Ring.sizes(n)[2] != n else 0) + len(WAYS))
        rings[number] = Ring(levels[number], members, take(2))
    pairs = take(LEVELS - 1)
    spreads = take(LEVELS - 1)
    centres = take(LEVELS - 1)
    block_s, block_v, packet, line, joined, packets, line_send, line_recv, gather_send, gather_recv = refs

    loads = [pltpu.make_async_copy(source, target, raw_sems.at[i]) for i, (source, target) in enumerate(((right_side, raw_g), (guess, raw_v)))]
    for load in loads:
        load.start()
    barrier = pltpu.get_barrier_semaphore()
    nx, ny, nz = counts

    def greet(device):
        pl.semaphore_signal(barrier, inc=1, device_id=device, device_id_type=MESH)

    def greet_plane(offset, carry):
        other = lax.rem(places[0] * ny + places[1] + offset, nx * ny)
        greet({AXES[0]: other // ny, AXES[1]: other % ny})
        return carry
    lax.fori_loop(1, nx * ny, greet_plane, 0)
    for offset in range(1, nz):
        greet({AXES[2]: lax.rem(places[2] + offset, nz)})
    for way in WAYS:
        if way[2] and (way[0] or way[1]):
            pl.when(exists(places, counts, way, 1))(lambda way=way: greet(along(places, way)))

    top.clear()
    top.prepare()
    top.missing()
    for load in loads:
        load.wait()
    even = (lax.broadcasted_iota(jnp.int32, (n0, n0), 0) + lax.broadcasted_iota(jnp.int32, (n0, n0), 1)) % 2 == 0

    def convert(step):
        for i in range(4):
            k = step * 4 + i
            at = (k + 2, pl.ds(8, n0), pl.ds(0, n0))
            first, second = raw_g[2 * k], raw_g[2 * k + 1]
            gr[at] = jnp.where(even, first, second)
            gb[at] = jnp.where(even, second, first)
            b[at] = jnp.where(even, raw_v[2 * k + 1], raw_v[2 * k])
    loop(n0 // 8, convert)
    top.pack(False)
    near = [jnp.where(place > 0, 1, 0) + jnp.where(place < count - 1, 1, 0) for place, count in zip(places, counts)]
    pl.semaphore_wait(barrier, nx * ny + nz - 2 + near[2] * ((near[0] + 1) * (near[1] + 1) - 1))
    top.send()
    for level in levels[1:]:
        level.prepare()
    for ring in rings.values():
        ring.clear()
    block_v[...] = jnp.zeros_like(block_v)
    top.land()
    top.sweep(0)
    top.sweep(1)
    top.restrict_to(levels[1].s, (EDGE, 8), pairs[0])
    for number in range(1, SHARED):
        level = levels[number]
        rings[number].post()
        if number == 2:
            top.sent()
            top.post(True)
        rings[number].land()
        level.sweep(0, zero=True, beyond=level.reach)
        level.sweep(1, beyond=level.reach - 1)
        if number + 1 < SHARED:
            level.restrict_to(levels[number + 1].s, (EDGE, 8), pairs[number])
        else:
            level.restrict_to(block_s, (0, 0), pairs[number])

    bx, by, bz = blocks[SHARED]
    wide = LANES // bx
    packed = jnp.zeros((rows_of(by), LANES), jnp.float32)
    for x in range(bx):
        packed = packed + pltpu.roll(block_s[x], x * wide + places[2] * bz, 1)
    packet[...] = packed[:by]

    def line_copy(source, target):
        return pltpu.make_async_remote_copy(
            src_ref=packet, dst_ref=line.at[source], send_sem=line_send.at[target], recv_sem=line_recv.at[source],
            device_id={AXES[2]: target}, device_id_type=MESH)

    for offset in range(1, nz):
        line_copy(places[2], lax.rem(places[2] + offset, nz)).start()
    merged = packed[:by]
    for offset in range(1, nz):
        source = lax.rem(places[2] + nz - offset, nz)
        line_copy(source, lax.rem(places[2] + offset, nz)).wait_recv()
        merged = merged + line[source]
    joined[...] = merged
    total = nx * ny
    me = places[0] * ny + places[1]

    def plane_copy(target):
        return pltpu.make_async_remote_copy(
            src_ref=joined, dst_ref=packets.at[me], send_sem=gather_send, recv_sem=gather_recv,
            device_id={AXES[0]: target // ny, AXES[1]: target % ny}, device_id_type=MESH)

    def post(offset, carry):
        plane_copy(lax.rem(me + offset, total)).start()
        return carry
    lax.fori_loop(1, total, post, 0)
    packets[me] = merged
    top.land(True)
    everyone = pltpu.make_async_remote_copy(
        src_ref=packets.at[pl.ds(0, total - 1)], dst_ref=packets.at[pl.ds(0, total - 1)], send_sem=gather_send, recv_sem=gather_recv,
        device_id={AXES[0]: places[0]}, device_id_type=MESH)
    everyone.wait_recv()
    whole = levels[SHARED]

    def unpack(px):
        for py in range(0, ny, 2):
            pair = jnp.concatenate([packets[px * ny + py], packets[px * ny + py + 1]], axis=0)
            for x in range(bx):
                whole.s[px * bx + x, pl.ds(py * by, 2 * by), :] = turn(pair, -x * wide)
    loop(nx, unpack)

    for number in range(SHARED, LEVELS - 1):
        level = levels[number]
        level.sweep(0, zero=True)
        level.sweep(1)
        level.restrict_to(levels[number + 1].s, (0, 0), pairs[number])
    level = levels[LEVELS - 1]
    level.sweep(0, zero=True)
    level.sweep(1)
    for _ in range(COARSE_SWEEPS - 1):
        level.sweep(0)
        level.sweep(1)
    for number in reversed(range(SHARED, LEVELS - 1)):
        level, below = levels[number], levels[number + 1]
        below.reflect()
        lift(below.v, below.ox, below.dims, (0, 0, 0), (1, 1, 1), level, spreads[number], centres[number])
        level.sweep(0)
        level.sweep(1)

    whole.reflect()
    shift = lax.rem(LANES - places[2] * bz, LANES)
    odd = lax.rem(places[1] + 1, 2) == 1
    for x in range(bx + 8):
        part = whole.v[places[0] * bx + (x - 4 + whole.ox), pl.ds(pl.multiple_of((places[1] + 1) // 2 * 8, 8), 24), :]
        block_v[x, pl.ds(4, 16)] = pltpu.roll(jnp.where(odd, part[4:20], part[:16]), shift, 1)
    lift(block_v, 4, blocks[SHARED], places, counts, levels[SHARED - 1], spreads[SHARED - 1], centres[SHARED - 1])
    for number in reversed(range(1, SHARED)):
        level = levels[number]
        level.sweep(0, beyond=level.reach - (1 if number == 1 else 2))
        level.sweep(1, beyond=level.reach - 3)
        level.reflect()
        lift(level.v, level.ox, level.dims, places, counts, levels[number - 1], spreads[number - 1], centres[number - 1])
    top.sweep(0)
    top.sweep(1)

    top.sent(True)
    for ring in rings.values():
        ring.finish()
    for offset in range(1, nz):
        line_copy(places[2], lax.rem(places[2] + offset, nz)).wait_send()
    everyone.wait_send()


def finish_kernel(counts, dims, r, b, gr, gb, solution, residual, d):
    places = tuple(lax.axis_index(axis) for axis in AXES)
    step = pl.program_id(0)
    n, many = dims[1], dims[0] // 2 // pl.num_programs(0)

    @pl.when(step == 0)
    def _():
        write_diagonals(d, dims, places, counts)
    even = (row_iota(n) + lane_iota(n)) % 2 == 0
    last = counts[0] * (dims[0] // 2) - 1
    group = solution.shape[0] // 2
    for i in range(group):
        k = step * group + i
        at = places[0] * (dims[0] // 2) + k
        kind = jnp.where(at == 0, 1, jnp.where(at == last, 2, 0))
        red, black = remainders(r, b, gr, gb, d, k + 2, kind, even, n)
        own = (k + 2, pl.ds(8, n), slice(None))
        for out, x, y in ((solution, r[own], b[own]), (residual, red, black)):
            out[2 * i] = jnp.where(even, x, y)[:, :n]
            out[2 * i + 1] = jnp.where(even, y, x)[:, :n]


def solution(mesh):
    counts = tuple(mesh.shape[axis] for axis in AXES)

    def per_device(right_side, guess):
        shape = right_side.shape
        blocks = [tuple(side >> level for side in shape) for level in range(SHARED + 1)]
        whole = tuple(side * count for side, count in zip(blocks[SHARED], counts))
        coarse = [tuple(side >> level for side in whole) for level in range(LEVELS - SHARED)]
        grids = blocks[:SHARED] + coarse
        n0 = blocks[0][0]
        scratch = []
        vmem = lambda *dims: scratch.append(pltpu.VMEM(dims, jnp.float32))
        sems = lambda *dims: scratch.append(pltpu.SemaphoreType.DMA(dims))
        vmem(*shape)
        vmem(*shape)
        sems(2)
        vmem(4, n0 + 8, LANES)
        vmem(3, n0, LANES)
        sent, got = Top.shapes(n0)
        for dims in sent:
            vmem(*dims)
        for way in WAYS:
            vmem(*got[way])
        sems(len(WAYS))
        sems(len(WAYS))
        for number, (x, y, z) in enumerate(grids):
            if number == 0:
                continue
            _, _, height, planes, tall = layout(number, (x, y, z))
            vmem(planes, tall, LANES)
            if number in REACH:
                vmem(planes, tall, LANES)
            else:
                vmem(x, rows_of(y), LANES)
            vmem(3, max(height, rows_of(inner_height(number, (x, y, z)) + 1)) if number in REACH else height, LANES)
            vmem(2, rows_of(y), LANES)
        for number in REACH:
            n = blocks[number][0]
            _, groups, cut, _, cuts = Ring.sizes(n)
            vmem(groups, n, LANES)
            if cut != n:
                vmem(cuts, n, LANES)
                vmem(cuts, n, LANES)
            for way in WAYS:
                vmem(*Ring.shape(n, REACH[number], way))
            sems(len(WAYS))
            sems(len(WAYS))
        for x, y, z in grids[:-1]:
            vmem(x // 2, max(16, y), LANES)
        for _ in range(2):
            for number in range(LEVELS - 1):
                _, _, _, planes, tall = lift_shape(number, blocks[number + 1] if number < SHARED else grids[number + 1])
                vmem(planes, tall, LANES)
        bx, by, bz = blocks[SHARED]
        vmem(bx, rows_of(by), LANES)
        vmem(bx + 8, 24, LANES)
        vmem(by, LANES)
        vmem(counts[2], by, LANES)
        vmem(by, LANES)
        total = counts[0] * counts[1]
        vmem(total, by, LANES)
        sems(counts[2])
        sems(counts[2])
        scratch.append(pltpu.SemaphoreType.DMA)
        scratch.append(pltpu.SemaphoreType.DMA)

        def kernel(*refs):
            solve_kernel(counts, blocks, coarse, refs)

        whole_block = pl.BlockSpec(memory_space=pltpu.VMEM)
        field = jax.ShapeDtypeStruct((n0 // 2 + 4, n0 + 24, LANES), jnp.float32)
        fields = pl.pallas_call(
            kernel,
            out_shape=(field,) * 4,
            in_specs=[pl.BlockSpec(memory_space=pltpu.HBM)] * 2,
            out_specs=(whole_block,) * 4,
            scratch_shapes=scratch,
            compiler_params=pltpu.CompilerParams(collective_id=0, has_side_effects=True, vmem_limit_bytes=VMEM_LIMIT * 2**20),
            name="vcycle",
        )(right_side, guess)

        def last(*refs):
            finish_kernel(counts, shape, *refs)
        block = pl.BlockSpec((8,) + shape[1:], lambda i: (i, 0, 0))
        return pl.pallas_call(
            last,
            grid=(n0 // 8,),
            out_shape=(jax.ShapeDtypeStruct(shape, jnp.float32),) * 2,
            in_specs=[whole_block] * 4,
            out_specs=(block,) * 2,
            scratch_shapes=[pltpu.VMEM((3, n0, LANES), jnp.float32)],
            compiler_params=pltpu.CompilerParams(vmem_limit_bytes=8 * 2**20),
            name="finish",
        )(*fields)

    spec = P(*AXES)
    return jax.shard_map(per_device, mesh=mesh, in_specs=(spec, spec), out_specs=(spec, spec), check_vma=False)
```

```python
import itertools

import jax
import jax.numpy as jnp
from jax import lax
from jax.experimental import pallas as pl
from jax.experimental.pallas import tpu as pltpu
from jax.sharding import PartitionSpec as P

LEVELS = 7
COARSE_SWEEPS = 4
SHARED = 4
VMEM_LIMIT = 46
LANES = 128
EDGE = 8
AXES = ("gx", "gy", "gz")
MESH = pl.DeviceIdType.MESH
WAYS = [way for way in itertools.product((-1, 0, 1), repeat=3) if any(way)]
FINAL = {0: 1, 1: 2, 2: 3, 3: 3}
REACH = {level: FINAL[level] + 3 for level in range(1, SHARED)}
SPARE = {SHARED - 2: 4}


def rows_of(count):
    return max(8, -(-count // 8) * 8)


def lane_iota(rows):
    return lax.broadcasted_iota(jnp.int32, (rows, LANES), 1)


def row_iota(rows):
    return lax.broadcasted_iota(jnp.int32, (rows, LANES), 0)


def loop(count, body):
    if count == 1:
        body(0)
    else:
        def step(i, carry):
            body(i)
            return carry
        lax.fori_loop(0, count, step, 0)


def turn(value, amount):
    amount = amount % LANES
    return pltpu.roll(value, amount, 1) if amount else value


def near_dot(value, matrix):
    first = value.astype(jnp.bfloat16)
    second = (value - first.astype(jnp.float32)).astype(jnp.bfloat16)
    dot = lambda part: jnp.dot(part, matrix, preferred_element_type=jnp.float32)
    return dot(second) + dot(first)


def widest(count, most, step=1):
    return max(size for size in range(step, count + 1, step) if count % size == 0 and (size <= most or size == step))


def signed(lane):
    return jnp.where(lane < 96, lane, lane - LANES)


class Grid:
    def __init__(self, number, dims, places, counts, v, s, w, d):
        self.number, self.dims, self.places, self.counts = number, dims, places, counts
        self.v, self.s, self.w, self.d = v, s, w, d
        self.reach = REACH.get(number, 0)
        self.ox, self.start, self.height, _, _ = layout(number, dims)
        self.sx, self.sy = (EDGE, 8) if self.reach else (0, 0)
        self.rows = rows_of(dims[1])
        self.spare, self.tall = spare_of(number, dims)

    def prepare(self):
        x, y, z = self.dims
        beyond = EDGE if self.reach else 0

        def base(height, start):
            row, lane = row_iota(height) + (start - 8), signed(lane_iota(height))
            at_y, at_z = self.places[1] * y + row, self.places[2] * z + lane
            last_y, last_z = self.counts[1] * y - 1, self.counts[2] * z - 1
            valid = (lane >= -beyond) & (lane < z + beyond) & (row >= -beyond) & (row < y + beyond)
            valid = valid & (at_y >= 0) & (at_y <= last_y) & (at_z >= 0) & (at_z <= last_z)
            one = lambda at, last: (at == 0).astype(jnp.float32) + (at == last).astype(jnp.float32)
            return valid, 6.0 + one(at_y, last_y) + one(at_z, last_z)
        valid, diagonal = base(self.w.shape[1], self.start)
        for wall in range(2):
            self.w[wall] = jnp.where(valid, 1.0 / (diagonal + wall), 0.0)
        self.w[2] = jnp.zeros_like(diagonal)
        valid, diagonal = base(self.tall, 8 - self.spare)
        for wall in range(2):
            self.d[wall] = jnp.where(valid, diagonal + wall, 0.0)
        self.v[...] = jnp.zeros_like(self.v)
        if self.reach:
            self.s[...] = jnp.zeros_like(self.s)

    def wall(self, plane, beyond=False):
        at = self.places[0] * self.dims[0] + plane
        last = self.counts[0] * self.dims[0] - 1
        if isinstance(at, int):
            return int(at in (0, last))
        kind = jnp.where((at == 0) | (at == last), 1, 0)
        return jnp.where((at < 0) | (at > last), 2, kind) if beyond else kind

    def total(self, plane, count, start, height):
        at = plane + self.ox
        slab = self.v[pl.ds(at - 1, count + 2), pl.ds(start, height), :]
        centre = slab[1:-1]
        total = slab[2:] + slab[:-2]
        total = total + self.v[pl.ds(at, count), pl.ds(start + 1, height), :] + self.v[pl.ds(at, count), pl.ds(start - 1, height), :]
        out = []
        for i in range(count):
            c = centre[i]
            out.append(total[i] + (pltpu.roll(c, 1, 1) + pltpu.roll(c, LANES - 1, 1)))
        return out, [centre[i] for i in range(count)]

    def sweep(self, colour, zero=False, beyond=0):
        start, height = self.start, self.height
        if self.reach and not zero:
            start, height = start + 1, inner_height(self.number, self.dims)
        planes = self.dims[0] + 2 * beyond
        chunk = widest(planes, 112 * 8 // height, 2)
        parity = (row_iota(height) + lane_iota(height) + start) % 2

        def body(step):
            first = step * chunk - beyond
            if not zero:
                totals, centres = self.total(first, chunk, start, height)
            results = []
            for i in range(chunk):
                weight = self.w[self.wall(first + i, beyond > 0), pl.ds(start - self.start, height), :]
                given = self.s[first + i + self.sx, pl.ds(start - 8 + self.sy, height), :]
                mine = parity == (i + colour + beyond) % 2
                if zero:
                    results.append(jnp.where(mine, given * weight, 0.0))
                else:
                    results.append(jnp.where(mine, (given + totals[i]) * weight, centres[i]))
            for i in range(chunk):
                self.v[first + i + self.ox, pl.ds(start, height), :] = results[i]
        loop(planes // chunk, body)

    def remainder(self, first, chunk):
        totals, centres = self.total(first, chunk, 8 - self.spare, self.tall)
        out = []
        for i in range(chunk):
            d = self.d[self.wall(first + i)]
            r = self.s[first + i + self.sx, pl.ds(self.sy - self.spare, self.tall), :] - (d * centres[i] - totals[i])
            out.append(r if self.dims[1] >= 8 else jnp.where(d > 0, r, 0.0))
        return out

    def restrict_to(self, target, corner, pairs):
        rows, planes = self.tall, self.dims[0] + 2 * self.spare
        chunk = widest(planes, 96 * 8 // rows, 2)
        half = chunk // 2
        if rows < 16:
            pairs[...] = jnp.zeros_like(pairs)

        def first(step):
            r = self.remainder(step * chunk - self.spare, chunk)
            for i in range(half):
                pairs[step * half + i, pl.ds(0, rows), :] = r[2 * i] + r[2 * i + 1]
        loop(planes // chunk, first)
        narrow(planes, rows, self.dims[2], self.spare, target, [at - self.spare // 2 for at in corner], pairs)

    def reflect(self):
        (x, y, z), v, ox = self.dims, self.v, self.ox
        margin = 3 if self.reach else 0
        for_all = pl.ds(ox - margin, x + 2 * margin)

        def low_x():
            v[ox - 1] = -v[ox]

        def high_x():
            v[ox + x] = -v[ox + x - 1]

        def low_y():
            v[for_all, pl.ds(7, 1), :] = -v[for_all, pl.ds(8, 1), :]

        def high_y():
            v[for_all, pl.ds(8 + y, 1), :] = -v[for_all, pl.ds(7 + y, 1), :]

        for axis, low, high in ((0, low_x, high_x), (1, low_y, high_y)):
            if isinstance(self.counts[axis], int) and isinstance(self.places[axis], int):
                low()
                high()
            else:
                pl.when(self.places[axis] == 0)(low)
                pl.when(self.places[axis] == self.counts[axis] - 1)(high)


def narrow(planes, rows, z, spare, target, corner, pairs):
    coarse_rows = rows_of(rows // 2)
    source_lane = signed(lax.broadcasted_iota(jnp.int32, (LANES, LANES), 0))
    target_lane = signed(lax.broadcasted_iota(jnp.int32, (LANES, LANES), 1))
    inside = (source_lane >= -spare) & (source_lane < z + spare)
    halve = jnp.where(((source_lane + LANES) // 2 - LANES // 2 == target_lane) & inside, 0.5, 0.0).astype(jnp.bfloat16)
    planes = planes // 2
    many = widest(planes, max(1, 512 // coarse_rows))

    def second(step):
        at = pl.ds(step * many, many)
        q = pairs[at, pl.ds(0, coarse_rows, stride=2), :] + pairs[at, pl.ds(1, coarse_rows, stride=2), :]
        q = near_dot(q.reshape(many * coarse_rows, LANES), halve)
        target[pl.ds(step * many + corner[0], many), pl.ds(corner[1], coarse_rows), :] = q.reshape(many, coarse_rows, LANES)
    loop(planes // many, second)


def spare_of(number, dims):
    spare = SPARE.get(number, 0)
    return spare, -(-(dims[1] + 2 * spare) // 16) * 16 if spare else rows_of(dims[1])


def layout(number, dims):
    x, y, z = dims
    if number in REACH:
        reach = REACH[number]
        height = rows_of(y + 2 * reach)
        return EDGE, 8 - reach, height, x + 2 * EDGE, max(40, y + 24)
    if number == SHARED:
        return EDGE, 8, rows_of(y), x + 2 * EDGE, rows_of(y) + 24
    return 1, 8, rows_of(y), x + 2, rows_of(y) + 16


def inner_height(number, dims):
    return rows_of(dims[1] + 2 * REACH[number] - 2)


def below_zero(number):
    return -((FINAL[number] + 3) // 2) if number in FINAL else 0


def lift_shape(number, coarse):
    low = below_zero(number)
    count = coarse[0] - 2 * low
    height = rows_of(coarse[1] - 2 * low)
    return low, count, height, count + 2, rows_of(8 + low + height + 1)


def widen(v, ox, dims, places, counts, number, spread, centre):
    z = dims[2]
    low, count, height, planes, tall = lift_shape(number, dims)
    beyond = EDGE if number in FINAL else 0
    k = signed(lax.broadcasted_iota(jnp.int32, (LANES, LANES), 0))
    f = signed(lax.broadcasted_iota(jnp.int32, (LANES, LANES), 1))
    at = places[2] * (2 * z) + f
    inside = (f >= -beyond) & (f < 2 * z + beyond) & (at >= 0) & (at < counts[2] * 2 * z)
    parent = (f + LANES) // 2 - LANES // 2
    near = parent + jnp.where((f + LANES) % 2 == 1, 1, -1)
    outside = (places[2] * z + near < 0) | (places[2] * z + near >= counts[2] * z)
    own = jnp.where((k == parent) & inside, 0.25, 0.0)
    beside = jnp.where((k == near) & inside, 0.25, 0.0)
    both = own + jnp.where(outside, -own, beside)
    matrix = jnp.concatenate([own, both], axis=1).astype(jnp.bfloat16)
    many = widest(planes, max(1, 1024 // tall))

    def first(step):
        e = v[pl.ds(step * many + (ox + low - 1), many), pl.ds(0, tall), :]
        product = near_dot(e.reshape(many * tall, LANES), matrix)
        at = pl.ds(step * many, many)
        spread[at] = product[:, :LANES].reshape(many, tall, LANES)
        centre[at] = product[:, LANES:].reshape(many, tall, LANES)
    loop(planes // many, first)


def lift(v, ox, dims, places, counts, fine, spread, centre):
    x, y, z = dims
    number = fine.number
    low, count, height, planes, tall = lift_shape(number, dims)
    beyond = EDGE if number in FINAL else 0
    widen(v, ox, dims, places, counts, number, spread, centre)
    group = widest(count, max(1, 256 // height))
    row = places[1] * y + row_iota(height) + low
    valid = (row >= 0) & (row < counts[1] * y)
    if not beyond:
        valid = row_iota(height) < y
    masked = beyond > 0 or y < height
    even = lane_iota(height) % 2 == 0

    def second(step):
        for i in range(group):
            plane = step * group + i
            middle = centre[plane + 1, pl.ds(8 + low, height), :]
            ys = (spread[plane + 1, pl.ds(7 + low, height), :], spread[plane + 1, pl.ds(9 + low, height), :])
            xs = [spread[plane + 2 * up_x, pl.ds(8 + low, height), :] for up_x in range(2)]
            here = valid
            if beyond:
                at = places[0] * x + plane + low
                here = valid & ((at >= 0) & (at < counts[0] * x))
            for up_y in range(2):
                rows = pl.ds(8 + 2 * low + up_y, height, stride=2)
                middle_y = middle + ys[up_y]
                if number == 0:
                    q = middle_y + jnp.where(even, xs[1 - up_y], xs[up_y])
                    q = jnp.where(here, q, 0.0)
                    at = (plane + low + fine.ox, rows, slice(None))
                    fine.b[at] = fine.b[at] + q
                    continue
                for up_x in range(2):
                    q = middle_y + xs[up_x]
                    if masked:
                        q = jnp.where(here, q, 0.0)
                    at = (2 * (plane + low) + up_x + fine.ox, rows, slice(None))
                    fine.v[at] = fine.v[at] + q
    loop(count // group, second)


def exists(places, counts, way, sign):
    found = None
    for axis in range(3):
        if way[axis]:
            other = places[axis] + sign * way[axis]
            one = (other >= 0) if sign * way[axis] < 0 else (other < counts[axis])
            found = one if found is None else found & one
    return found


def along(places, way):
    return {name: places[axis] + way[axis] for axis, name in enumerate(AXES) if way[axis]}


class Top:
    number, ox, sets = 0, 2, 4

    def __init__(self, dims, places, counts, r, b, gr, gb, w, d, out, got, sems):
        self.dims, self.places, self.counts = dims, places, counts
        self.r, self.b, self.gr, self.gb, self.w, self.d = r, b, gr, gb, w, d
        self.out, self.got, self.sems = out, got, sems
        self.pairs, self.n = dims[0] // 2, dims[1]

    @staticmethod
    def weights(dims, places, counts, height, start, beyond):
        x, y, z = dims
        row, lane = row_iota(height) + (start - 8), signed(lane_iota(height))
        at_y, at_z = places[1] * y + row, places[2] * z + lane
        last_y, last_z = counts[1] * y - 1, counts[2] * z - 1
        valid = (lane >= -beyond) & (lane < z + beyond) & (at_y >= 0) & (at_y <= last_y) & (at_z >= 0) & (at_z <= last_z)
        one = lambda at, last: (at == 0).astype(jnp.float32) + (at == last).astype(jnp.float32)
        return valid, 6.0 + one(at_y, last_y) + one(at_z, last_z), (row + lane + LANES) % 2 == 0

    def clear(self):
        for ref in (self.r, self.b, self.gr, self.gb):
            ref[...] = jnp.zeros_like(ref)

    def prepare(self):
        valid, diagonal, even = self.weights(self.dims, self.places, self.counts, self.n + 8, 6, 4)
        plain, more = (jnp.where(valid, 1.0 / (diagonal + wall), 0.0) for wall in range(2))
        self.w[0] = plain
        self.w[1] = jnp.where(even, more, plain)
        self.w[2] = jnp.where(even, plain, more)
        self.w[3] = jnp.zeros_like(plain)
        write_diagonals(self.d, self.dims, self.places, self.counts)

    def missing(self):
        for way in WAYS:
            @pl.when(jnp.logical_not(exists(self.places, self.counts, way, -1)))
            def _(way=way):
                self.got[way][...] = jnp.zeros_like(self.got[way])

    def kind(self, pair):
        at = self.places[0] * self.pairs + pair
        last = self.counts[0] * self.pairs - 1
        return jnp.where((at < 0) | (at > last), 3, jnp.where(at == 0, 1, jnp.where(at == last, 2, 0)))

    def sweep(self, colour):
        start, height = 6, self.n + 8
        source, target, given = (self.r, self.b, self.gb) if colour else (self.b, self.r, self.gr)
        count = self.pairs + 2
        chunk = widest(count, 17)
        even = (row_iota(height) + lane_iota(height)) % 2 == 0

        def body(step):
            for i in range(chunk):
                k = step * chunk + i - 1
                at = k + 2
                total = around(source, at, start, height, even, colour)
                kind = self.kind(k)
                if colour:
                    kind = jnp.where(kind == 1, 2, jnp.where(kind == 2, 1, kind))
                target[at, pl.ds(start, height), :] = (given[at, pl.ds(start, height), :] + total) * self.w[kind]
        loop(count // chunk, body)

    def restrict_to(self, target, corner, pairs):
        n = self.n
        even = (row_iota(n) + lane_iota(n)) % 2 == 0
        chunk = 8

        def body(step):
            for i in range(chunk):
                k = step * chunk + i
                red, black = remainders(self.r, self.b, self.gr, self.gb, self.d, k + 2, self.kind(k), even, n)
                pairs[k] = red + black
        loop(self.pairs // chunk, body)
        narrow(self.dims[0], n, self.dims[2], 0, target, corner, pairs)

    @staticmethod
    def shapes(n):
        face = {0: (2, n, LANES), 1: (n // 4, 8, LANES), 2: (3, n, LANES)}
        sent = [face[0], face[0], face[1], face[1], face[2], face[2], (4, 8, LANES)]
        got = {}
        for way in WAYS:
            if sum(map(abs, way)) == 1:
                got[way] = face[[abs(part) for part in way].index(1)]
            elif not way[2]:
                got[way] = (2, 8, LANES)
            elif not way[0]:
                got[way] = (2, 8, LANES)
            else:
                got[way] = (8, LANES)
        return sent, got

    def copies(self, way, again):
        n, out, got = self.n, self.out, self.got[way]
        high = [part > 0 for part in way]
        if sum(map(abs, way)) == 1:
            axis = [abs(part) for part in way].index(1)
            source = out[2 * axis + high[axis]]
            if again and axis != 1:
                source, got = source.at[pl.ds(0, 1)], got.at[pl.ds(0, 1)]
        elif not way[2]:
            source = out[2 + high[1]].at[pl.ds(n // 4 - 2 if high[0] else 0, 2)]
        elif not way[0]:
            row = pl.ds(n - 8 if high[1] else 0, 8)
            source = out[4 + high[2]].at[pl.ds(0, 2), row]
        else:
            source = out[6].at[2 * high[0] + high[2]]
        k = WAYS.index(way)
        return pltpu.make_async_remote_copy(
            src_ref=source, dst_ref=got, send_sem=self.sems[0].at[k], recv_sem=self.sems[1].at[k],
            device_id=along(self.places, way), device_id_type=MESH)

    def pack(self, again):
        n, pairs = self.n, self.pairs
        arrays = [self.b] if again else [self.b, self.gr, self.gb]
        low, tile = lane_iota(n) < 64, lane_iota(8)
        row = row_iota(8)
        half = pairs // 2
        own = lambda ref, k: ref[k + 2, pl.ds(8, n), :]
        for high in range(2):
            near, far = (pairs - 1, pairs - 2) if high else (0, 1)
            self.out[high][0] = jnp.where(low, own(self.b, near), pltpu.roll(own(self.b, far), 64, 1))
            if not again:
                self.out[high][1] = jnp.where(low, own(self.gr, near), pltpu.roll(own(self.gb, near), 64, 1))

            def edge(k, high=high):
                first = 8 + n - 8 if high else 8
                b = self.b[k + 2, pl.ds(first, 8), :]
                if again:
                    return b
                red, black = (pltpu.roll(ref[k + 2, pl.ds(first, 8), :], by, 0) for ref, by in ((self.gr, 4), (self.gb, 2 if high else 6)))
                if high:
                    return jnp.where(row >= 4, b, jnp.where(row >= 2, red, black))
                return jnp.where(row < 4, b, jnp.where(row < 6, red, black))
            for k in range(half):
                self.out[2 + high][k] = jnp.where(tile < 64, edge(k), pltpu.roll(edge(k + half), 64, 1))
        def body(t):
            at = pl.ds(pl.multiple_of(t * 8, 8), 8)
            ahead = (tile + (LANES - 60)) % LANES
            first = [jnp.zeros((8, LANES), jnp.float32)] * len(arrays)
            last = list(first)
            for k in range(pairs):
                for index, ref in enumerate(arrays):
                    moved = turn(ref[k + 2, pl.ds(pl.multiple_of(t * 8 + 8, 8), 8), :], 4 * k)
                    first[index] = jnp.where((tile >= 4 * k) & (tile < 4 * k + 4), moved, first[index])
                    last[index] = jnp.where(ahead // 4 == k, moved, last[index])
            for index in range(len(arrays)):
                self.out[4][index, at] = first[index]
                self.out[5][index, at] = last[index]
        loop(n // 8, body)
        for high_x in range(2):
            for high_z in range(2):
                offset = 60 if high_z else 0
                pair, near = (pairs - 2, pairs - 1) if high_x else (0, 0)
                value = jnp.zeros((8, LANES), jnp.float32)
                for t in range(n // 8):
                    rows = pl.ds(8 * t, 8)
                    moved = turn(self.out[4 + high_z][0, rows], 16 * t - 4 * pair - offset)
                    value = jnp.where((tile >= 16 * t) & (tile < 16 * t + 8), moved, value)
                    if not again:
                        moved = turn(self.out[4 + high_z][1, rows], 16 * t + 8 - 4 * near - offset)
                        value = jnp.where((tile >= 16 * t + 8) & (tile < 16 * t + 16), moved, value)
                self.out[6][2 * high_x + high_z] = value

    def post(self, again=False):
        self.pack(again)
        self.send(again)

    def send(self, again=False):
        for way in WAYS:
            pl.when(exists(self.places, self.counts, way, 1))(self.copies(way, again).start)

    def sent(self, again=False):
        for way in WAYS:
            pl.when(exists(self.places, self.counts, way, 1))(self.copies(way, again).wait_send)

    def land(self, again=False):
        n, pairs, got = self.n, self.pairs, self.got
        half = pairs // 2
        for way in WAYS:
            pl.when(exists(self.places, self.counts, way, -1))(self.copies(way, again).wait_recv)
        arrays = [self.b] if again else [self.b, self.gr, self.gb]
        lane, tile = lane_iota(n), lane_iota(8)

        def ends(high, low, to, k):
            pick = to % 8 < 4
            return turn(jnp.where(pick, high, low) if k % 2 == 0 else jnp.where(pick, low, high), 64 - 4 * k)
        high, low = got[(0, 0, -1)], got[(0, 0, 1)]

        def body(t):
            at = pl.ds(pl.multiple_of(t * 8, 8), 8)
            packs = [(high[index, at], low[index, at]) for index in range(len(arrays))]
            for k in range(pairs):
                own = (k + 2, pl.ds(pl.multiple_of(t * 8 + 8, 8), 8), slice(None))
                for (h, l), ref in zip(packs, arrays):
                    ref[own] = jnp.where(tile < 64, ref[own], ends(h, l, tile, k))
        loop(n // 8, body)
        for side in (-1, 1):
            face = got[(0, -side, 0)]
            base = 8 + n if side > 0 else 0
            shifts = (0, 4, 2 if side > 0 else 6)
            for index, ref in enumerate(arrays):
                if index < 2:
                    h, l = got[(0, -side, -1)][index], got[(0, -side, 1)][index]
                for k in range(pairs):
                    value = face[k % half]
                    if k >= half:
                        value = pltpu.roll(value, 64, 1)
                    if shifts[index]:
                        value = pltpu.roll(value, shifts[index], 0)
                    if index < 2:
                        value = jnp.where(tile < 64, value, ends(h, l, tile, k))
                    ref[k + 2, pl.ds(base, 8), :] = value
        for side in (-1, 1):
            face = got[(-side, 0, 0)]
            near, far = (pairs + 2, pairs + 3) if side > 0 else (1, 0)
            high, low = got[(-side, 0, -1)], got[(-side, 0, 1)]
            near_lane, far_lane = (0, 4) if side > 0 else (4, 0)

            def beside(first, at, high=high, low=low):
                out = []
                for t in at:
                    up = turn(high[...], 64 - 16 * t - first)
                    out.append(jnp.where(tile < 96, up, turn(low[...], 124 - 16 * t - first)))
                return jnp.concatenate(out, axis=0) if len(out) > 1 else out[0]
            every = range(n // 8)
            both = face[0]
            self.b[near, pl.ds(8, n), :] = jnp.where(lane < 64, both, beside(near_lane, every))
            self.b[far, pl.ds(8, n), :] = jnp.where(lane < 64, pltpu.roll(both, 64, 1), beside(far_lane, every))
            if not again:
                both = face[1]
                self.gr[near, pl.ds(8, n), :] = jnp.where(lane < 64, both, beside(8, every))
                self.gb[near, pl.ds(8, n), :] = pltpu.roll(both, 64, 1)
            for up in (-1, 1):
                edge = got[(-side, -up, 0)]
                base = 8 + n if up > 0 else 0
                corner = (got[(-side, -up, -1)], got[(-side, -up, 1)])
                t = [0 if up > 0 else n // 8 - 1]
                if side > 0:
                    pieces = {near: (0, False), far: (1, False)}
                else:
                    pieces = {near: (1, True), far: (0, True)}
                for place, (group, upper) in pieces.items():
                    value = edge[group]
                    if upper:
                        value = pltpu.roll(value, 64, 1)
                    first = near_lane if place == near else far_lane
                    self.b[place, pl.ds(base, 8), :] = jnp.where(tile < 64, value, beside(first, t, *corner))
                    if place == near and not again:
                        self.gr[place, pl.ds(base, 8), :] = pltpu.roll(value, 4, 0)


def around(source, at, start, height, even, colour):
    s = source[at, pl.ds(start, height), :]
    left, right = source[at - 1, pl.ds(start, height), :], source[at + 1, pl.ds(start, height), :]
    across = jnp.where(even, right, left) if colour else jnp.where(even, left, right)
    total = (s + across) + (source[at, pl.ds(start + 1, height), :] + source[at, pl.ds(start - 1, height), :])
    return total + (pltpu.roll(s, 1, 1) + pltpu.roll(s, LANES - 1, 1))


def remainders(r, b, gr, gb, d, at, kind, even, n):
    rows = pl.ds(8, n)
    other = jnp.where(kind == 1, 2, jnp.where(kind == 2, 1, kind))
    red = gr[at, rows, :] - (d[kind] * r[at, rows, :] - around(b, at, 8, n, even, 0))
    black = gb[at, rows, :] - (d[other] * b[at, rows, :] - around(r, at, 8, n, even, 1))
    return red, black


def write_diagonals(d, dims, places, counts):
    _, diagonal, even = Top.weights(dims, places, counts, dims[1], 8, 0)
    d[0] = diagonal
    d[1] = jnp.where(even, diagonal + 1.0, diagonal)
    d[2] = jnp.where(even, diagonal, diagonal + 1.0)


class Ring:
    def __init__(self, level, refs, sems):
        self.level, self.sems = level, sems
        self.body, self.parts = refs[0], refs[1:-len(WAYS)]
        self.got = dict(zip(WAYS, refs[-len(WAYS):]))
        self.places, self.counts = level.places, level.counts

    @staticmethod
    def sizes(n):
        each = LANES // n
        cut = n if n <= 16 else 8
        return each, max(1, n // each), cut, LANES // cut, max(1, n * cut // LANES)

    @staticmethod
    def thick(n, reach, way):
        each, groups, _, _, cuts = Ring.sizes(n)
        if not way[0]:
            return cuts if way[2] else groups
        return 1 if way[2] else -(-reach // each)

    @staticmethod
    def shape(n, reach, way):
        return (Ring.thick(n, reach, way), 8 if way[1] else n, LANES)

    def clear(self):
        for way in WAYS:
            @pl.when(jnp.logical_not(exists(self.places, self.counts, way, -1)))
            def _(way=way):
                self.got[way][...] = jnp.zeros_like(self.got[way])

    def copy(self, way):
        n = self.level.dims[0]
        shape = Ring.shape(n, self.level.reach, way)
        source = self.body
        if way[2] and self.parts:
            source = self.parts[0] if way[2] < 0 else self.parts[1]
        groups = source.shape[0]
        group = 0 if way[0] <= 0 else groups - shape[0]
        row = 0 if way[1] <= 0 else n - 8
        k = WAYS.index(way)
        return pltpu.make_async_remote_copy(
            src_ref=source.at[pl.ds(group, shape[0]), pl.ds(row, shape[1])], dst_ref=self.got[way],
            send_sem=self.sems[0].at[k], recv_sem=self.sems[1].at[k],
            device_id={name: self.places[axis] + way[axis] for axis, name in enumerate(AXES) if way[axis]}, device_id_type=MESH)

    def post(self):
        n, s = self.level.dims[0], self.level.s
        each, groups, cut, cuts_each, cuts = Ring.sizes(n)

        def plane(x):
            value = s[EDGE + x, pl.ds(8, n), :]
            return jnp.where(lane_iota(n) < n, value, 0.0) if SPARE.get(self.level.number - 1) else value
        for g in range(groups):
            value = plane(g * each)
            for i in range(1, min(each, n)):
                value = value + turn(plane(g * each + i), i * n)
            self.body[g] = value
        if self.parts:
            lane = lane_iota(n)
            for g in range(cuts):
                low = high = jnp.zeros((n, LANES), jnp.float32)
                for i in range(cuts_each):
                    moved = turn(plane(g * cuts_each + i), cut * i)
                    low = jnp.where(lane // cut == i, moved, low)
                    high = jnp.where((lane + (LANES - n + cut)) % LANES // cut == i, moved, high)
                self.parts[0][g] = low
                self.parts[1][g] = high
        for way in WAYS:
            pl.when(exists(self.places, self.counts, way, 1))(self.copy(way).start)

    def land(self):
        n, s, reach = self.level.dims[0], self.level.s, self.level.reach
        each, groups, cut, cuts_each, cuts = Ring.sizes(n)
        for way in WAYS:
            pl.when(exists(self.places, self.counts, way, -1))(self.copy(way).wait_recv)
        for to_x, to_y in itertools.product((-1, 0, 1), repeat=2):
            height = 8 if to_y else n
            row = {-1: 0, 0: 8, 1: 8 + n}[to_y]
            lane = lane_iota(height)
            body = self.got[(-to_x, -to_y, 0)] if to_x or to_y else None
            high = self.got[(-to_x, -to_y, -1)]
            low = self.got[(-to_x, -to_y, 1)]
            for x in {-1: range(n - reach, n), 0: range(n), 1: range(reach)}[to_x]:
                at = (EDGE + to_x * n + x, pl.ds(row, height), slice(None))
                g, h = x // each, x // cuts_each
                if to_x < 0:
                    g, h = g - (groups - body.shape[0]), h - (cuts - high.shape[0])
                near = turn(body[g], -(x % each) * n) if body is not None else s[at]
                above = turn(high[h], n - cut * (x % cuts_each))
                under = turn(low[h], -n - cut * (x % cuts_each))
                s[at] = jnp.where(lane < n, near, jnp.where(lane < 64, above, under))

    def finish(self):
        for way in WAYS:
            pl.when(exists(self.places, self.counts, way, 1))(self.copy(way).wait_send)


def solve_kernel(counts, blocks, coarse, refs):
    right_side, guess, r, b, gr, gb = refs[:6]
    refs = list(refs[6:])
    take = lambda count=1: [refs.pop(0) for _ in range(count)] if count > 1 else refs.pop(0)
    places = tuple(lax.axis_index(axis) for axis in AXES)
    n0 = blocks[0][0]
    raw_g, raw_v, raw_sems = take(3)
    sent_shapes, got_shapes = Top.shapes(n0)
    w0, d0 = take(2)
    top = Top(blocks[0], places, counts, r, b, gr, gb, w0, d0, take(len(sent_shapes)), dict(zip(WAYS, take(len(WAYS)))), take(2))
    levels = [top]
    for number in range(1, LEVELS):
        if number < SHARED:
            levels.append(Grid(number, blocks[number], places, counts, *take(4)))
        else:
            levels.append(Grid(number, coarse[number - SHARED], (0, 0, 0), (1, 1, 1), *take(4)))
    rings = {}
    for number in REACH:
        n = blocks[number][0]
        members = take(1 + (2 if Ring.sizes(n)[2] != n else 0) + len(WAYS))
        rings[number] = Ring(levels[number], members, take(2))
    pairs = take(LEVELS - 1)
    spreads = take(LEVELS - 1)
    centres = take(LEVELS - 1)
    block_s, block_v, packet, line, joined, packets, line_send, line_recv, gather_send, gather_recv, spread_sem = refs

    loads = [pltpu.make_async_copy(source, target, raw_sems.at[i]) for i, (source, target) in enumerate(((right_side, raw_g), (guess, raw_v)))]
    for load in loads:
        load.start()
    barrier = pltpu.get_barrier_semaphore()
    nx, ny, nz = counts

    def greet(device):
        pl.semaphore_signal(barrier, inc=1, device_id=device, device_id_type=MESH)

    for way in WAYS:
        pl.when(exists(places, counts, way, 1))(lambda way=way: greet(along(places, way)))
    near = [jnp.where(place > 0, 1, 0) + jnp.where(place < count - 1, 1, 0) for place, count in zip(places, counts)]

    def tell(turn):
        for way in WAYS:
            if not way[2] or not (way[0] or way[1]):
                @pl.when(exists(places, counts, way, 1))
                def _(way=way):
                    pl.semaphore_signal(spread_sem.at[turn], inc=1, device_id=along(places, way), device_id_type=MESH)

    def hear(turn):
        pl.semaphore_wait(spread_sem.at[turn], (near[0] + 1) * (near[1] + 1) - 1 + near[2])

    top.clear()
    top.prepare()
    top.missing()
    for load in loads:
        load.wait()
    even = (lax.broadcasted_iota(jnp.int32, (n0, n0), 0) + lax.broadcasted_iota(jnp.int32, (n0, n0), 1)) % 2 == 0

    def convert(step):
        for i in range(4):
            k = step * 4 + i
            at = (k + 2, pl.ds(8, n0), pl.ds(0, n0))
            first, second = raw_g[2 * k], raw_g[2 * k + 1]
            gr[at] = jnp.where(even, first, second)
            gb[at] = jnp.where(even, second, first)
            b[at] = jnp.where(even, raw_v[2 * k + 1], raw_v[2 * k])
    loop(n0 // 8, convert)
    top.pack(False)
    pl.semaphore_wait(barrier, (near[0] + 1) * (near[1] + 1) * (near[2] + 1) - 1)
    top.send()
    for level in levels[1:]:
        level.prepare()
    for ring in rings.values():
        ring.clear()
    block_v[...] = jnp.zeros_like(block_v)
    top.land()
    tell(0)
    top.sweep(0)
    top.sweep(1)
    top.restrict_to(levels[1].s, (EDGE, 8), pairs[0])
    hear(0)
    for number in range(1, SHARED - 1):
        level = levels[number]
        rings[number].post()
        rings[number].land()
        tell(number)
        level.sweep(0, zero=True, beyond=level.reach)
        level.sweep(1, beyond=level.reach - 1)
        level.restrict_to(levels[number + 1].s, (EDGE, 8), pairs[number])
        hear(number)
    last = levels[SHARED - 1]
    last.sweep(0, zero=True, beyond=2)
    last.sweep(1, beyond=1)
    last.restrict_to(block_s, (0, 0), pairs[SHARED - 1])

    bx, by, bz = blocks[SHARED]
    wide = LANES // bx
    packed = jnp.zeros((rows_of(by), LANES), jnp.float32)
    for x in range(bx):
        packed = packed + pltpu.roll(block_s[x], x * wide + places[2] * bz, 1)
    packet[...] = packed[:by]

    def line_copy(source, target):
        return pltpu.make_async_remote_copy(
            src_ref=packet, dst_ref=line.at[source], send_sem=line_send.at[target], recv_sem=line_recv.at[source],
            device_id={AXES[2]: target}, device_id_type=MESH)

    for offset in range(1, nz):
        line_copy(places[2], lax.rem(places[2] + offset, nz)).start()
    rings[SHARED - 1].post()
    top.sent()
    top.post(True)
    merged = packed[:by]
    for offset in range(1, nz):
        source = lax.rem(places[2] + nz - offset, nz)
        line_copy(source, lax.rem(places[2] + offset, nz)).wait_recv()
        merged = merged + line[source]
    joined[...] = merged
    total = nx * ny
    me = places[0] * ny + places[1]

    def plane_copy(to_x, to_y):
        return pltpu.make_async_remote_copy(
            src_ref=joined, dst_ref=packets.at[me], send_sem=gather_send, recv_sem=gather_recv,
            device_id={AXES[0]: to_x, AXES[1]: to_y}, device_id_type=MESH)

    xs = [lax.rem(places[0] + step, nx) for step in range(nx)]
    ys = [lax.rem(places[1] + step, ny) for step in range(ny)]
    far = lambda at: min(at[0], nx - at[0]) + min(at[1], ny - at[1])
    for to_x, to_y in sorted(itertools.product(range(nx), range(ny)), key=far, reverse=True)[:-1]:
        plane_copy(xs[to_x], ys[to_y]).start()
    packets[me] = merged
    rings[SHARED - 1].land()
    last.sweep(0, zero=True, beyond=last.reach)
    last.sweep(1, beyond=last.reach - 1)
    top.land(True)
    everyone = pltpu.make_async_remote_copy(
        src_ref=packets.at[pl.ds(0, total - 1)], dst_ref=packets.at[pl.ds(0, total - 1)], send_sem=gather_send, recv_sem=gather_recv,
        device_id={AXES[0]: places[0]}, device_id_type=MESH)
    everyone.wait_recv()
    whole = levels[SHARED]

    def unpack(px):
        for py in range(0, ny, 2):
            pair = jnp.concatenate([packets[px * ny + py], packets[px * ny + py + 1]], axis=0)
            for x in range(bx):
                whole.s[px * bx + x, pl.ds(py * by, 2 * by), :] = turn(pair, -x * wide)
    loop(nx, unpack)

    for number in range(SHARED, LEVELS - 1):
        level = levels[number]
        level.sweep(0, zero=True)
        level.sweep(1)
        level.restrict_to(levels[number + 1].s, (0, 0), pairs[number])
    level = levels[LEVELS - 1]
    level.sweep(0, zero=True)
    level.sweep(1)
    for _ in range(COARSE_SWEEPS - 1):
        level.sweep(0)
        level.sweep(1)
    for number in reversed(range(SHARED, LEVELS - 1)):
        level, below = levels[number], levels[number + 1]
        below.reflect()
        lift(below.v, below.ox, below.dims, (0, 0, 0), (1, 1, 1), level, spreads[number], centres[number])
        level.sweep(0)
        level.sweep(1)

    whole.reflect()
    shift = lax.rem(LANES - places[2] * bz, LANES)
    odd = lax.rem(places[1] + 1, 2) == 1
    for x in range(bx + 8):
        part = whole.v[places[0] * bx + (x - 4 + whole.ox), pl.ds(pl.multiple_of((places[1] + 1) // 2 * 8, 8), 24), :]
        block_v[x, pl.ds(4, 16)] = pltpu.roll(jnp.where(odd, part[4:20], part[:16]), shift, 1)
    lift(block_v, 4, blocks[SHARED], places, counts, levels[SHARED - 1], spreads[SHARED - 1], centres[SHARED - 1])
    for number in reversed(range(1, SHARED)):
        level = levels[number]
        level.sweep(0, beyond=level.reach - (1 if number == 1 else 2))
        level.sweep(1, beyond=level.reach - 3)
        level.reflect()
        lift(level.v, level.ox, level.dims, places, counts, levels[number - 1], spreads[number - 1], centres[number - 1])
    top.sweep(0)
    top.sweep(1)

    top.sent(True)
    for ring in rings.values():
        ring.finish()
    for offset in range(1, nz):
        line_copy(places[2], lax.rem(places[2] + offset, nz)).wait_send()
    everyone.wait_send()


def finish_kernel(counts, dims, r, b, gr, gb, solution, residual, d):
    places = tuple(lax.axis_index(axis) for axis in AXES)
    step = pl.program_id(0)
    n, many = dims[1], dims[0] // 2 // pl.num_programs(0)

    @pl.when(step == 0)
    def _():
        write_diagonals(d, dims, places, counts)
    even = (row_iota(n) + lane_iota(n)) % 2 == 0
    last = counts[0] * (dims[0] // 2) - 1
    group = solution.shape[0] // 2
    for i in range(group):
        k = step * group + i
        at = places[0] * (dims[0] // 2) + k
        kind = jnp.where(at == 0, 1, jnp.where(at == last, 2, 0))
        red, black = remainders(r, b, gr, gb, d, k + 2, kind, even, n)
        own = (k + 2, pl.ds(8, n), slice(None))
        for out, x, y in ((solution, r[own], b[own]), (residual, red, black)):
            out[2 * i] = jnp.where(even, x, y)[:, :n]
            out[2 * i + 1] = jnp.where(even, y, x)[:, :n]


def solution(mesh):
    counts = tuple(mesh.shape[axis] for axis in AXES)

    def per_device(right_side, guess):
        shape = right_side.shape
        blocks = [tuple(side >> level for side in shape) for level in range(SHARED + 1)]
        whole = tuple(side * count for side, count in zip(blocks[SHARED], counts))
        coarse = [tuple(side >> level for side in whole) for level in range(LEVELS - SHARED)]
        grids = blocks[:SHARED] + coarse
        n0 = blocks[0][0]
        scratch = []
        vmem = lambda *dims: scratch.append(pltpu.VMEM(dims, jnp.float32))
        sems = lambda *dims: scratch.append(pltpu.SemaphoreType.DMA(dims))
        vmem(*shape)
        vmem(*shape)
        sems(2)
        vmem(4, n0 + 8, LANES)
        vmem(3, n0, LANES)
        sent, got = Top.shapes(n0)
        for dims in sent:
            vmem(*dims)
        for way in WAYS:
            vmem(*got[way])
        sems(len(WAYS))
        sems(len(WAYS))
        for number, (x, y, z) in enumerate(grids):
            if number == 0:
                continue
            _, _, height, planes, tall = layout(number, (x, y, z))
            vmem(planes, tall, LANES)
            if number in REACH:
                vmem(planes, tall, LANES)
            else:
                vmem(x, rows_of(y), LANES)
            vmem(3, max(height, rows_of(inner_height(number, (x, y, z)) + 1)) if number in REACH else height, LANES)
            vmem(2, spare_of(number, (x, y, z))[1], LANES)
        for number in REACH:
            n = blocks[number][0]
            _, groups, cut, _, cuts = Ring.sizes(n)
            vmem(groups, n, LANES)
            if cut != n:
                vmem(cuts, n, LANES)
                vmem(cuts, n, LANES)
            for way in WAYS:
                vmem(*Ring.shape(n, REACH[number], way))
            sems(len(WAYS))
            sems(len(WAYS))
        for number, (x, y, z) in enumerate(grids[:-1]):
            spare, tall = spare_of(number, (x, y, z))
            vmem(x // 2 + spare, max(16, tall), LANES)
        for _ in range(2):
            for number in range(LEVELS - 1):
                _, _, _, planes, tall = lift_shape(number, blocks[number + 1] if number < SHARED else grids[number + 1])
                vmem(planes, tall, LANES)
        bx, by, bz = blocks[SHARED]
        vmem(bx, rows_of(by), LANES)
        vmem(bx + 8, 24, LANES)
        vmem(by, LANES)
        vmem(counts[2], by, LANES)
        vmem(by, LANES)
        total = counts[0] * counts[1]
        vmem(total, by, LANES)
        sems(counts[2])
        sems(counts[2])
        scratch.append(pltpu.SemaphoreType.DMA)
        scratch.append(pltpu.SemaphoreType.DMA)
        scratch.append(pltpu.SemaphoreType.REGULAR((SHARED - 1,)))

        def kernel(*refs):
            solve_kernel(counts, blocks, coarse, refs)

        whole_block = pl.BlockSpec(memory_space=pltpu.VMEM)
        field = jax.ShapeDtypeStruct((n0 // 2 + 4, n0 + 24, LANES), jnp.float32)
        fields = pl.pallas_call(
            kernel,
            out_shape=(field,) * 4,
            in_specs=[pl.BlockSpec(memory_space=pltpu.HBM)] * 2,
            out_specs=(whole_block,) * 4,
            scratch_shapes=scratch,
            compiler_params=pltpu.CompilerParams(collective_id=0, has_side_effects=True, vmem_limit_bytes=VMEM_LIMIT * 2**20),
            name="vcycle",
        )(right_side, guess)

        def last(*refs):
            finish_kernel(counts, shape, *refs)
        block = pl.BlockSpec((16,) + shape[1:], lambda i: (i, 0, 0))
        return pl.pallas_call(
            last,
            grid=(n0 // 16,),
            out_shape=(jax.ShapeDtypeStruct(shape, jnp.float32),) * 2,
            in_specs=[whole_block] * 4,
            out_specs=(block,) * 2,
            scratch_shapes=[pltpu.VMEM((3, n0, LANES), jnp.float32)],
            compiler_params=pltpu.CompilerParams(vmem_limit_bytes=8 * 2**20),
            name="finish",
        )(*fields)

    spec = P(*AXES)
    return jax.shard_map(per_device, mesh=mesh, in_specs=(spec, spec), out_specs=(spec, spec), check_vma=False)
```

```python
import itertools

import jax
import jax.numpy as jnp
from jax import lax
from jax.experimental import pallas as pl
from jax.experimental.pallas import tpu as pltpu
from jax.sharding import PartitionSpec as P

LEVELS = 7
COARSE_SWEEPS = 4
SHARED = 4
VMEM_LIMIT = 46
SWEEP_SHARE, REST_SHARE, LAST_SHARE, GRID_SHARE = 0.4, 0.4, 0.0, 0.4
LANES = 128
EDGE = 8
AXES = ("gx", "gy", "gz")
MESH = pl.DeviceIdType.MESH
WAYS = [way for way in itertools.product((-1, 0, 1), repeat=3) if any(way)]
FLAT = [way for way in WAYS if not way[2] or not (way[0] or way[1])]
FINAL = {0: 1, 1: 2, 2: 3, 3: 3}
REACH = {level: FINAL[level] + 3 for level in range(1, SHARED)}
SPARE = {SHARED - 2: 4}


def rows_of(count):
    return max(8, -(-count // 8) * 8)


def lane_iota(rows):
    return lax.broadcasted_iota(jnp.int32, (rows, LANES), 1)


def row_iota(rows):
    return lax.broadcasted_iota(jnp.int32, (rows, LANES), 0)


def loop(count, body):
    if count == 1:
        body(0)
    else:
        def step(i, carry):
            body(i)
            return carry
        lax.fori_loop(0, count, step, 0)


def turn(value, amount):
    amount = amount % LANES
    return pltpu.roll(value, amount, 1) if amount else value


def near_dot(value, matrix):
    first = value.astype(jnp.bfloat16)
    second = (value - first.astype(jnp.float32)).astype(jnp.bfloat16)
    dot = lambda part: jnp.dot(part, matrix, preferred_element_type=jnp.float32)
    return dot(second) + dot(first)


def write_beside(beside):
    k = lax.broadcasted_iota(jnp.int32, (2 * LANES, LANES), 0)
    f = lax.broadcasted_iota(jnp.int32, (2 * LANES, LANES), 1)
    apart = (k - f + 2 * LANES) % LANES
    beside[...] = jnp.where((apart == 1) | (apart == LANES - 1), 1.0, 0.0).astype(jnp.bfloat16)


def lane_sums(values, beside, share):
    many = int(len(values) * share)
    out = []
    if many:
        height = values[0].shape[0]
        value = jnp.concatenate(values[:many], axis=0)
        first = value.astype(jnp.bfloat16)
        second = (value - first.astype(jnp.float32)).astype(jnp.bfloat16)
        sums = jnp.dot(jnp.concatenate([first, second], axis=1), beside[...], preferred_element_type=jnp.float32)
        out = [sums[i * height:(i + 1) * height] for i in range(many)]
    return out + [pltpu.roll(value, 1, 1) + pltpu.roll(value, LANES - 1, 1) for value in values[many:]]


def widest(count, most, step=1):
    return max(size for size in range(step, count + 1, step) if count % size == 0 and (size <= most or size == step))


def signed(lane):
    return jnp.where(lane < 96, lane, lane - LANES)


class Grid:
    def __init__(self, number, dims, places, counts, beside, v, s, w, d):
        self.number, self.dims, self.places, self.counts = number, dims, places, counts
        self.v, self.s, self.w, self.d, self.beside = v, s, w, d, beside
        self.reach = REACH.get(number, 0)
        self.ox, self.start, self.height, _, _ = layout(number, dims)
        self.sx, self.sy = (EDGE, 8) if self.reach else (0, 0)
        self.rows = rows_of(dims[1])
        self.spare, self.tall = spare_of(number, dims)

    def prepare(self):
        x, y, z = self.dims
        beyond = EDGE if self.reach else 0

        def base(height, start):
            row, lane = row_iota(height) + (start - 8), signed(lane_iota(height))
            at_y, at_z = self.places[1] * y + row, self.places[2] * z + lane
            last_y, last_z = self.counts[1] * y - 1, self.counts[2] * z - 1
            valid = (lane >= -beyond) & (lane < z + beyond) & (row >= -beyond) & (row < y + beyond)
            valid = valid & (at_y >= 0) & (at_y <= last_y) & (at_z >= 0) & (at_z <= last_z)
            one = lambda at, last: (at == 0).astype(jnp.float32) + (at == last).astype(jnp.float32)
            return valid, 6.0 + one(at_y, last_y) + one(at_z, last_z)
        valid, diagonal = base(self.w.shape[1], self.start)
        for wall in range(2):
            self.w[wall] = jnp.where(valid, 1.0 / (diagonal + wall), 0.0)
        self.w[2] = jnp.zeros_like(diagonal)
        valid, diagonal = base(self.tall, 8 - self.spare)
        for wall in range(2):
            self.d[wall] = jnp.where(valid, diagonal + wall, 0.0)
        self.v[...] = jnp.zeros_like(self.v)
        if self.reach:
            self.s[...] = jnp.zeros_like(self.s)

    def wall(self, plane, beyond=False):
        at = self.places[0] * self.dims[0] + plane
        last = self.counts[0] * self.dims[0] - 1
        if isinstance(at, int):
            return int(at in (0, last))
        kind = jnp.where((at == 0) | (at == last), 1, 0)
        return jnp.where((at < 0) | (at > last), 2, kind) if beyond else kind

    def total(self, plane, count, start, height):
        at = plane + self.ox
        slab = self.v[pl.ds(at - 1, count + 2), pl.ds(start, height), :]
        centre = slab[1:-1]
        total = slab[2:] + slab[:-2]
        total = total + self.v[pl.ds(at, count), pl.ds(start + 1, height), :] + self.v[pl.ds(at, count), pl.ds(start - 1, height), :]
        out = []
        centres = [centre[i] for i in range(count)]
        for i, beside in enumerate(lane_sums(centres, self.beside, GRID_SHARE)):
            out.append(total[i] + beside)
        return out, centres

    def sweep(self, colour, zero=False, beyond=0):
        start, height = self.start, self.height
        if self.reach and not zero:
            start, height = start + 1, inner_height(self.number, self.dims)
        planes = self.dims[0] + 2 * beyond
        chunk = widest(planes, 112 * 8 // height, 2)
        parity = (row_iota(height) + lane_iota(height) + start) % 2

        def body(step):
            first = step * chunk - beyond
            if not zero:
                totals, centres = self.total(first, chunk, start, height)
            results = []
            for i in range(chunk):
                weight = self.w[self.wall(first + i, beyond > 0), pl.ds(start - self.start, height), :]
                given = self.s[first + i + self.sx, pl.ds(start - 8 + self.sy, height), :]
                mine = parity == (i + colour + beyond) % 2
                if zero:
                    results.append(jnp.where(mine, given * weight, 0.0))
                else:
                    results.append(jnp.where(mine, (given + totals[i]) * weight, centres[i]))
            for i in range(chunk):
                self.v[first + i + self.ox, pl.ds(start, height), :] = results[i]
        loop(planes // chunk, body)

    def remainder(self, first, chunk):
        totals, centres = self.total(first, chunk, 8 - self.spare, self.tall)
        out = []
        for i in range(chunk):
            d = self.d[self.wall(first + i)]
            r = self.s[first + i + self.sx, pl.ds(self.sy - self.spare, self.tall), :] - (d * centres[i] - totals[i])
            out.append(r if self.dims[1] >= 8 else jnp.where(d > 0, r, 0.0))
        return out

    def restrict_to(self, target, corner, pairs):
        rows, planes = self.tall, self.dims[0] + 2 * self.spare
        chunk = widest(planes, 96 * 8 // rows, 2)
        half = chunk // 2
        if rows < 16:
            pairs[...] = jnp.zeros_like(pairs)

        def first(step):
            r = self.remainder(step * chunk - self.spare, chunk)
            for i in range(half):
                pairs[step * half + i, pl.ds(0, rows), :] = r[2 * i] + r[2 * i + 1]
        loop(planes // chunk, first)
        narrow(planes, rows, self.dims[2], self.spare, target, [at - self.spare // 2 for at in corner], pairs)

    def reflect(self):
        (x, y, z), v, ox = self.dims, self.v, self.ox
        margin = 3 if self.reach else 0
        for_all = pl.ds(ox - margin, x + 2 * margin)

        def low_x():
            v[ox - 1] = -v[ox]

        def high_x():
            v[ox + x] = -v[ox + x - 1]

        def low_y():
            v[for_all, pl.ds(7, 1), :] = -v[for_all, pl.ds(8, 1), :]

        def high_y():
            v[for_all, pl.ds(8 + y, 1), :] = -v[for_all, pl.ds(7 + y, 1), :]

        for axis, low, high in ((0, low_x, high_x), (1, low_y, high_y)):
            if isinstance(self.counts[axis], int) and isinstance(self.places[axis], int):
                low()
                high()
            else:
                pl.when(self.places[axis] == 0)(low)
                pl.when(self.places[axis] == self.counts[axis] - 1)(high)


def narrow(planes, rows, z, spare, target, corner, pairs):
    coarse_rows = rows_of(rows // 2)
    source_lane = signed(lax.broadcasted_iota(jnp.int32, (LANES, LANES), 0))
    target_lane = signed(lax.broadcasted_iota(jnp.int32, (LANES, LANES), 1))
    inside = (source_lane >= -spare) & (source_lane < z + spare)
    halve = jnp.where(((source_lane + LANES) // 2 - LANES // 2 == target_lane) & inside, 0.5, 0.0).astype(jnp.bfloat16)
    planes = planes // 2
    many = widest(planes, max(1, 512 // coarse_rows))

    def second(step):
        at = pl.ds(step * many, many)
        q = pairs[at, pl.ds(0, coarse_rows, stride=2), :] + pairs[at, pl.ds(1, coarse_rows, stride=2), :]
        q = near_dot(q.reshape(many * coarse_rows, LANES), halve)
        target[pl.ds(step * many + corner[0], many), pl.ds(corner[1], coarse_rows), :] = q.reshape(many, coarse_rows, LANES)
    loop(planes // many, second)


def spare_of(number, dims):
    spare = SPARE.get(number, 0)
    return spare, -(-(dims[1] + 2 * spare) // 16) * 16 if spare else rows_of(dims[1])


def layout(number, dims):
    x, y, z = dims
    if number in REACH:
        reach = REACH[number]
        height = rows_of(y + 2 * reach)
        return EDGE, 8 - reach, height, x + 2 * EDGE, max(40, y + 24)
    if number == SHARED:
        return EDGE, 8, rows_of(y), x + 2 * EDGE, rows_of(y) + 24
    return 1, 8, rows_of(y), x + 2, rows_of(y) + 16


def inner_height(number, dims):
    return rows_of(dims[1] + 2 * REACH[number] - 2)


def below_zero(number):
    return -((FINAL[number] + 3) // 2) if number in FINAL else 0


def lift_shape(number, coarse):
    low = below_zero(number)
    count = coarse[0] - 2 * low
    height = rows_of(coarse[1] - 2 * low)
    return low, count, height, count + 2, rows_of(8 + low + height + 1)


def widen(v, ox, dims, places, counts, number, spread, centre):
    z = dims[2]
    low, count, height, planes, tall = lift_shape(number, dims)
    beyond = EDGE if number in FINAL else 0
    k = signed(lax.broadcasted_iota(jnp.int32, (LANES, LANES), 0))
    f = signed(lax.broadcasted_iota(jnp.int32, (LANES, LANES), 1))
    at = places[2] * (2 * z) + f
    inside = (f >= -beyond) & (f < 2 * z + beyond) & (at >= 0) & (at < counts[2] * 2 * z)
    parent = (f + LANES) // 2 - LANES // 2
    near = parent + jnp.where((f + LANES) % 2 == 1, 1, -1)
    outside = (places[2] * z + near < 0) | (places[2] * z + near >= counts[2] * z)
    own = jnp.where((k == parent) & inside, 0.25, 0.0)
    beside = jnp.where((k == near) & inside, 0.25, 0.0)
    both = own + jnp.where(outside, -own, beside)
    matrix = jnp.concatenate([own, both], axis=1).astype(jnp.bfloat16)
    many = widest(planes, max(1, 1024 // tall))

    def first(step):
        e = v[pl.ds(step * many + (ox + low - 1), many), pl.ds(0, tall), :]
        product = near_dot(e.reshape(many * tall, LANES), matrix)
        at = pl.ds(step * many, many)
        spread[at] = product[:, :LANES].reshape(many, tall, LANES)
        centre[at] = product[:, LANES:].reshape(many, tall, LANES)
    loop(planes // many, first)


def lift(v, ox, dims, places, counts, fine, spread, centre):
    x, y, z = dims
    number = fine.number
    low, count, height, planes, tall = lift_shape(number, dims)
    beyond = EDGE if number in FINAL else 0
    widen(v, ox, dims, places, counts, number, spread, centre)
    group = widest(count, max(1, 256 // height))
    row = places[1] * y + row_iota(height) + low
    valid = (row >= 0) & (row < counts[1] * y)
    if not beyond:
        valid = row_iota(height) < y
    masked = beyond > 0 or y < height
    even = lane_iota(height) % 2 == 0

    def second(step):
        for i in range(group):
            plane = step * group + i
            middle = centre[plane + 1, pl.ds(8 + low, height), :]
            ys = (spread[plane + 1, pl.ds(7 + low, height), :], spread[plane + 1, pl.ds(9 + low, height), :])
            xs = [spread[plane + 2 * up_x, pl.ds(8 + low, height), :] for up_x in range(2)]
            here = valid
            if beyond:
                at = places[0] * x + plane + low
                here = valid & ((at >= 0) & (at < counts[0] * x))
            for up_y in range(2):
                rows = pl.ds(8 + 2 * low + up_y, height, stride=2)
                middle_y = middle + ys[up_y]
                if number == 0:
                    q = middle_y + jnp.where(even, xs[1 - up_y], xs[up_y])
                    q = jnp.where(here, q, 0.0)
                    at = (plane + low + fine.ox, rows, slice(None))
                    fine.b[at] = fine.b[at] + q
                    continue
                for up_x in range(2):
                    q = middle_y + xs[up_x]
                    if masked:
                        q = jnp.where(here, q, 0.0)
                    at = (2 * (plane + low) + up_x + fine.ox, rows, slice(None))
                    fine.v[at] = fine.v[at] + q
    loop(count // group, second)


def exists(places, counts, way, sign):
    found = None
    for axis in range(3):
        if way[axis]:
            other = places[axis] + sign * way[axis]
            one = (other >= 0) if sign * way[axis] < 0 else (other < counts[axis])
            found = one if found is None else found & one
    return found


def along(places, way):
    return {name: places[axis] + way[axis] for axis, name in enumerate(AXES) if way[axis]}


class Top:
    number, ox, sets = 0, 2, 4

    def __init__(self, dims, places, counts, beside, r, b, gr, gb, w, d, out, got, sems):
        self.beside = beside
        self.dims, self.places, self.counts = dims, places, counts
        self.r, self.b, self.gr, self.gb, self.w, self.d = r, b, gr, gb, w, d
        self.out, self.got, self.sems = out, got, sems
        self.pairs, self.n = dims[0] // 2, dims[1]

    @staticmethod
    def weights(dims, places, counts, height, start, beyond):
        x, y, z = dims
        row, lane = row_iota(height) + (start - 8), signed(lane_iota(height))
        at_y, at_z = places[1] * y + row, places[2] * z + lane
        last_y, last_z = counts[1] * y - 1, counts[2] * z - 1
        valid = (lane >= -beyond) & (lane < z + beyond) & (at_y >= 0) & (at_y <= last_y) & (at_z >= 0) & (at_z <= last_z)
        one = lambda at, last: (at == 0).astype(jnp.float32) + (at == last).astype(jnp.float32)
        return valid, 6.0 + one(at_y, last_y) + one(at_z, last_z), (row + lane + LANES) % 2 == 0

    def clear(self):
        for ref in (self.r, self.b, self.gr, self.gb):
            ref[...] = jnp.zeros_like(ref)

    def prepare(self):
        valid, diagonal, even = self.weights(self.dims, self.places, self.counts, self.n + 8, 6, 4)
        plain, more = (jnp.where(valid, 1.0 / (diagonal + wall), 0.0) for wall in range(2))
        self.w[0] = plain
        self.w[1] = jnp.where(even, more, plain)
        self.w[2] = jnp.where(even, plain, more)
        self.w[3] = jnp.zeros_like(plain)
        write_diagonals(self.d, self.dims, self.places, self.counts)

    def missing(self):
        for way in WAYS:
            @pl.when(jnp.logical_not(exists(self.places, self.counts, way, -1)))
            def _(way=way):
                self.got[way][...] = jnp.zeros_like(self.got[way])

    def kind(self, pair):
        at = self.places[0] * self.pairs + pair
        last = self.counts[0] * self.pairs - 1
        return jnp.where((at < 0) | (at > last), 3, jnp.where(at == 0, 1, jnp.where(at == last, 2, 0)))

    def sweep(self, colour):
        start, height = 6, self.n + 8
        source, target, given = (self.r, self.b, self.gb) if colour else (self.b, self.r, self.gr)
        count = self.pairs + 2
        chunk = widest(count, 17)
        even = (row_iota(height) + lane_iota(height)) % 2 == 0

        def body(step):
            ats = [step * chunk + i + 1 for i in range(chunk)]
            for at, total in zip(ats, around(source, ats, start, height, even, colour, self.beside, SWEEP_SHARE)):
                k = at - 2
                kind = self.kind(k)
                if colour:
                    kind = jnp.where(kind == 1, 2, jnp.where(kind == 2, 1, kind))
                target[at, pl.ds(start, height), :] = (given[at, pl.ds(start, height), :] + total) * self.w[kind]
        loop(count // chunk, body)

    def restrict_to(self, target, corner, pairs):
        n = self.n
        even = (row_iota(n) + lane_iota(n)) % 2 == 0
        chunk = 8

        def body(step):
            ks = [step * chunk + i for i in range(chunk)]
            kinds = [self.kind(k) for k in ks]
            ats = [k + 2 for k in ks]
            for k, (red, black) in zip(ks, remainders(self.r, self.b, self.gr, self.gb, self.d, ats, kinds, even, n, self.beside, REST_SHARE)):
                pairs[k] = red + black
        loop(self.pairs // chunk, body)
        narrow(self.dims[0], n, self.dims[2], 0, target, corner, pairs)

    @staticmethod
    def shapes(n):
        face = {0: (2, n, LANES), 1: (n // 4, 8, LANES), 2: (3, n, LANES)}
        sent = [face[0], face[0], face[1], face[1], face[2], face[2], (4, 8, LANES)]
        got = {}
        for way in WAYS:
            if sum(map(abs, way)) == 1:
                got[way] = face[[abs(part) for part in way].index(1)]
            elif not way[2]:
                got[way] = (2, 8, LANES)
            elif not way[0]:
                got[way] = (2, 8, LANES)
            else:
                got[way] = (8, LANES)
        return sent, got

    def copies(self, way, again):
        n, out, got = self.n, self.out, self.got[way]
        high = [part > 0 for part in way]
        if sum(map(abs, way)) == 1:
            axis = [abs(part) for part in way].index(1)
            source = out[2 * axis + high[axis]]
            if again and axis != 1:
                source, got = source.at[pl.ds(0, 1)], got.at[pl.ds(0, 1)]
        elif not way[2]:
            source = out[2 + high[1]].at[pl.ds(n // 4 - 2 if high[0] else 0, 2)]
        elif not way[0]:
            row = pl.ds(n - 8 if high[1] else 0, 8)
            source = out[4 + high[2]].at[pl.ds(0, 2), row]
        else:
            source = out[6].at[2 * high[0] + high[2]]
        k = WAYS.index(way)
        return pltpu.make_async_remote_copy(
            src_ref=source, dst_ref=got, send_sem=self.sems[0].at[k], recv_sem=self.sems[1].at[k],
            device_id=along(self.places, way), device_id_type=MESH)

    def pack_ends(self, part, again):
        tile = lane_iota(8)
        many = self.pairs // self.sets
        ahead = (tile + (LANES - 60)) % LANES
        wide = 4 * many
        for t in range(self.n // 8):
            at = pl.ds(8 * t, 8)
            for index, ref in enumerate([self.b] if again else [self.b, self.gr, self.gb]):
                first = last = None
                for k in range(part * many, part * many + many):
                    moved = turn(ref[k + 2, pl.ds(8 * t + 8, 8), :], 4 * k)
                    first = moved if first is None else jnp.where(tile // 4 == k, moved, first)
                    last = moved if last is None else jnp.where(ahead // 4 == k, moved, last)
                if part:
                    first = jnp.where(tile // wide == part, first, self.out[4][index, at])
                    last = jnp.where(ahead // wide == part, last, self.out[5][index, at])
                self.out[4][index, at] = first
                self.out[5][index, at] = last

    def pack(self, again):
        n, pairs = self.n, self.pairs
        low, tile = lane_iota(n) < 64, lane_iota(8)
        row = row_iota(8)
        half = pairs // 2
        own = lambda ref, k: ref[k + 2, pl.ds(8, n), :]
        for high in range(2):
            near, far = (pairs - 1, pairs - 2) if high else (0, 1)
            self.out[high][0] = jnp.where(low, own(self.b, near), pltpu.roll(own(self.b, far), 64, 1))
            if not again:
                self.out[high][1] = jnp.where(low, own(self.gr, near), pltpu.roll(own(self.gb, near), 64, 1))

            def edge(k, high=high):
                first = 8 + n - 8 if high else 8
                b = self.b[k + 2, pl.ds(first, 8), :]
                if again:
                    return b
                red, black = (pltpu.roll(ref[k + 2, pl.ds(first, 8), :], by, 0) for ref, by in ((self.gr, 4), (self.gb, 2 if high else 6)))
                if high:
                    return jnp.where(row >= 4, b, jnp.where(row >= 2, red, black))
                return jnp.where(row < 4, b, jnp.where(row < 6, red, black))
            for k in range(half):
                self.out[2 + high][k] = jnp.where(tile < 64, edge(k), pltpu.roll(edge(k + half), 64, 1))
        for high_x in range(2):
            for high_z in range(2):
                offset = 60 if high_z else 0
                pair, near = (pairs - 2, pairs - 1) if high_x else (0, 0)
                value = jnp.zeros((8, LANES), jnp.float32)
                for t in range(n // 8):
                    rows = pl.ds(8 * t, 8)
                    moved = turn(self.out[4 + high_z][0, rows], 16 * t - 4 * pair - offset)
                    value = jnp.where((tile >= 16 * t) & (tile < 16 * t + 8), moved, value)
                    if not again:
                        moved = turn(self.out[4 + high_z][1, rows], 16 * t + 8 - 4 * near - offset)
                        value = jnp.where((tile >= 16 * t + 8) & (tile < 16 * t + 16), moved, value)
                self.out[6][2 * high_x + high_z] = value

    def post(self, again=False):
        for part in range(self.sets):
            self.pack_ends(part, again)
        self.pack(again)
        self.send(again)

    def send(self, again=False):
        for way in WAYS:
            pl.when(exists(self.places, self.counts, way, 1))(self.copies(way, again).start)

    def sent(self, again=False):
        for way in WAYS:
            pl.when(exists(self.places, self.counts, way, 1))(self.copies(way, again).wait_send)

    def wait(self, ways, again):
        for way in ways:
            pl.when(exists(self.places, self.counts, way, -1))(self.copies(way, again).wait_recv)

    def land(self, again=False):
        n, pairs, got = self.n, self.pairs, self.got
        half = pairs // 2
        arrays = [self.b] if again else [self.b, self.gr, self.gb]
        lane, tile = lane_iota(n), lane_iota(8)

        def ends(high, low, to, k):
            pick = to % 8 < 4
            return turn(jnp.where(pick, high, low) if k % 2 == 0 else jnp.where(pick, low, high), 64 - 4 * k)
        self.wait([way for way in WAYS if not (way[0] or way[1])], again)
        high, low = got[(0, 0, -1)], got[(0, 0, 1)]

        def body(t):
            at = pl.ds(pl.multiple_of(t * 8, 8), 8)
            packs = [(high[index, at], low[index, at]) for index in range(len(arrays))]
            for k in range(pairs):
                own = (k + 2, pl.ds(pl.multiple_of(t * 8 + 8, 8), 8), slice(None))
                for (h, l), ref in zip(packs, arrays):
                    ref[own] = jnp.where(tile < 64, ref[own], ends(h, l, tile, k))
        loop(n // 8, body)
        self.wait([way for way in WAYS if way[1] and not way[0]], again)
        for side in (-1, 1):
            face = got[(0, -side, 0)]
            base = 8 + n if side > 0 else 0
            shifts = (0, 4, 2 if side > 0 else 6)
            for index, ref in enumerate(arrays):
                if index < 2:
                    h, l = got[(0, -side, -1)][index], got[(0, -side, 1)][index]
                for k in range(pairs):
                    value = face[k % half]
                    if k >= half:
                        value = pltpu.roll(value, 64, 1)
                    if shifts[index]:
                        value = pltpu.roll(value, shifts[index], 0)
                    if index < 2:
                        value = jnp.where(tile < 64, value, ends(h, l, tile, k))
                    ref[k + 2, pl.ds(base, 8), :] = value
        self.wait([way for way in WAYS if way[0]], again)
        for side in (-1, 1):
            face = got[(-side, 0, 0)]
            near, far = (pairs + 2, pairs + 3) if side > 0 else (1, 0)
            high, low = got[(-side, 0, -1)], got[(-side, 0, 1)]
            near_lane, far_lane = (0, 4) if side > 0 else (4, 0)

            def beside(first, at, high=high, low=low):
                out = []
                for t in at:
                    up = turn(high[...], 64 - 16 * t - first)
                    out.append(jnp.where(tile < 96, up, turn(low[...], 124 - 16 * t - first)))
                return jnp.concatenate(out, axis=0) if len(out) > 1 else out[0]
            every = range(n // 8)
            both = face[0]
            self.b[near, pl.ds(8, n), :] = jnp.where(lane < 64, both, beside(near_lane, every))
            self.b[far, pl.ds(8, n), :] = jnp.where(lane < 64, pltpu.roll(both, 64, 1), beside(far_lane, every))
            if not again:
                both = face[1]
                self.gr[near, pl.ds(8, n), :] = jnp.where(lane < 64, both, beside(8, every))
                self.gb[near, pl.ds(8, n), :] = pltpu.roll(both, 64, 1)
            for up in (-1, 1):
                edge = got[(-side, -up, 0)]
                base = 8 + n if up > 0 else 0
                corner = (got[(-side, -up, -1)], got[(-side, -up, 1)])
                t = [0 if up > 0 else n // 8 - 1]
                if side > 0:
                    pieces = {near: (0, False), far: (1, False)}
                else:
                    pieces = {near: (1, True), far: (0, True)}
                for place, (group, upper) in pieces.items():
                    value = edge[group]
                    if upper:
                        value = pltpu.roll(value, 64, 1)
                    first = near_lane if place == near else far_lane
                    self.b[place, pl.ds(base, 8), :] = jnp.where(tile < 64, value, beside(first, t, *corner))
                    if place == near and not again:
                        self.gr[place, pl.ds(base, 8), :] = pltpu.roll(value, 4, 0)


def around(source, ats, start, height, even, colour, beside, share):
    rows = pl.ds(start, height)
    centres = [source[at, rows, :] for at in ats]
    out = []
    for at, s, z_sum in zip(ats, centres, lane_sums(centres, beside, share)):
        left, right = source[at - 1, rows, :], source[at + 1, rows, :]
        across = jnp.where(even, right, left) if colour else jnp.where(even, left, right)
        total = (s + across) + (source[at, pl.ds(start + 1, height), :] + source[at, pl.ds(start - 1, height), :])
        out.append(total + z_sum)
    return out


def remainders(r, b, gr, gb, d, ats, kinds, even, n, beside, share):
    rows = pl.ds(8, n)
    out = []
    for at, kind, reds, blacks in zip(ats, kinds, around(b, ats, 8, n, even, 0, beside, share), around(r, ats, 8, n, even, 1, beside, share)):
        other = jnp.where(kind == 1, 2, jnp.where(kind == 2, 1, kind))
        out.append((gr[at, rows, :] - (d[kind] * r[at, rows, :] - reds), gb[at, rows, :] - (d[other] * b[at, rows, :] - blacks)))
    return out


def write_diagonals(d, dims, places, counts):
    _, diagonal, even = Top.weights(dims, places, counts, dims[1], 8, 0)
    d[0] = diagonal
    d[1] = jnp.where(even, diagonal + 1.0, diagonal)
    d[2] = jnp.where(even, diagonal, diagonal + 1.0)


class Ring:
    def __init__(self, level, refs, sems):
        self.level, self.sems = level, sems
        self.body, self.parts = refs[0], refs[1:-len(WAYS)]
        self.got = dict(zip(WAYS, refs[-len(WAYS):]))
        self.places, self.counts = level.places, level.counts

    @staticmethod
    def sizes(n):
        each = LANES // n
        cut = n if n <= 16 else 8
        return each, max(1, n // each), cut, LANES // cut, max(1, n * cut // LANES)

    @staticmethod
    def thick(n, reach, way):
        each, groups, _, _, cuts = Ring.sizes(n)
        if not way[0]:
            return cuts if way[2] else groups
        return 1 if way[2] else -(-reach // each)

    @staticmethod
    def shape(n, reach, way):
        return (Ring.thick(n, reach, way), 8 if way[1] else n, LANES)

    def clear(self):
        for way in WAYS:
            @pl.when(jnp.logical_not(exists(self.places, self.counts, way, -1)))
            def _(way=way):
                self.got[way][...] = jnp.zeros_like(self.got[way])

    def copy(self, way):
        n = self.level.dims[0]
        shape = Ring.shape(n, self.level.reach, way)
        source = self.body
        if way[2] and self.parts:
            source = self.parts[0] if way[2] < 0 else self.parts[1]
        groups = source.shape[0]
        group = 0 if way[0] <= 0 else groups - shape[0]
        row = 0 if way[1] <= 0 else n - 8
        k = WAYS.index(way)
        return pltpu.make_async_remote_copy(
            src_ref=source.at[pl.ds(group, shape[0]), pl.ds(row, shape[1])], dst_ref=self.got[way],
            send_sem=self.sems[0].at[k], recv_sem=self.sems[1].at[k],
            device_id={name: self.places[axis] + way[axis] for axis, name in enumerate(AXES) if way[axis]}, device_id_type=MESH)

    def post(self):
        n, s = self.level.dims[0], self.level.s
        each, groups, cut, cuts_each, cuts = Ring.sizes(n)

        def plane(x):
            value = s[EDGE + x, pl.ds(8, n), :]
            return jnp.where(lane_iota(n) < n, value, 0.0) if SPARE.get(self.level.number - 1) else value
        for g in range(groups):
            value = plane(g * each)
            for i in range(1, min(each, n)):
                value = value + turn(plane(g * each + i), i * n)
            self.body[g] = value
        if self.parts:
            lane = lane_iota(n)
            for g in range(cuts):
                low = high = jnp.zeros((n, LANES), jnp.float32)
                for i in range(cuts_each):
                    moved = turn(plane(g * cuts_each + i), cut * i)
                    low = jnp.where(lane // cut == i, moved, low)
                    high = jnp.where((lane + (LANES - n + cut)) % LANES // cut == i, moved, high)
                self.parts[0][g] = low
                self.parts[1][g] = high
        for way in WAYS:
            pl.when(exists(self.places, self.counts, way, 1))(self.copy(way).start)

    def land(self):
        n, s, reach = self.level.dims[0], self.level.s, self.level.reach
        each, groups, cut, cuts_each, cuts = Ring.sizes(n)
        for to_x, to_y in sorted(itertools.product((-1, 0, 1), repeat=2), key=lambda at: abs(at[0]) * 3 + abs(at[1])):
            for way in WAYS:
                if way[:2] == (-to_x, -to_y):
                    pl.when(exists(self.places, self.counts, way, -1))(self.copy(way).wait_recv)
            height = 8 if to_y else n
            row = {-1: 0, 0: 8, 1: 8 + n}[to_y]
            lane = lane_iota(height)
            body = self.got[(-to_x, -to_y, 0)] if to_x or to_y else None
            high = self.got[(-to_x, -to_y, -1)]
            low = self.got[(-to_x, -to_y, 1)]

            made = {}

            def merged(h, flip, made=made, high=high, low=low, lane=lane):
                if (h, flip) not in made:
                    both = (high[h], turn(low[h], -2 * n))
                    made[h, flip] = jnp.where(lane % 16 < 8, both[flip], both[1 - flip])
                return made[h, flip]
            for x in {-1: range(n - reach, n), 0: range(n), 1: range(reach)}[to_x]:
                at = (EDGE + to_x * n + x, pl.ds(row, height), slice(None))
                g, h = x // each, x // cuts_each
                if to_x < 0:
                    g, h = g - (groups - body.shape[0]), h - (cuts - high.shape[0])
                near = turn(body[g], -(x % each) * n) if body is not None else s[at]
                if n == 8:
                    ends = jnp.where(lane < 64, turn(high[h], n - cut * (x % cuts_each)), turn(low[h], -n - cut * (x % cuts_each)))
                else:
                    ends = turn(merged(h, x % 2 if n == 32 else 0), n - cut * (x % cuts_each))
                s[at] = jnp.where(lane < n, near, ends)

    def finish(self):
        for way in WAYS:
            pl.when(exists(self.places, self.counts, way, 1))(self.copy(way).wait_send)


def solve_kernel(counts, blocks, coarse, refs):
    right_side, guess, r, b, gr, gb = refs[:6]
    refs = list(refs[6:])
    take = lambda count=1: [refs.pop(0) for _ in range(count)] if count > 1 else refs.pop(0)
    places = tuple(lax.axis_index(axis) for axis in AXES)
    n0 = blocks[0][0]
    raw_g, raw_v, raw_sems = take(3)
    sent_shapes, got_shapes = Top.shapes(n0)
    w0, d0, beside = take(3)
    top = Top(blocks[0], places, counts, beside, r, b, gr, gb, w0, d0, take(len(sent_shapes)), dict(zip(WAYS, take(len(WAYS)))), take(2))
    levels = [top]
    for number in range(1, LEVELS):
        if number < SHARED:
            levels.append(Grid(number, blocks[number], places, counts, beside, *take(4)))
        else:
            levels.append(Grid(number, coarse[number - SHARED], (0, 0, 0), (1, 1, 1), beside, *take(4)))
    rings = {}
    for number in REACH:
        n = blocks[number][0]
        members = take(1 + (2 if Ring.sizes(n)[2] != n else 0) + len(WAYS))
        rings[number] = Ring(levels[number], members, take(2) if number < SHARED - 1 else rings[1].sems)
    pairs = take(LEVELS - 1)
    spreads = take(LEVELS - 1)
    centres = take(LEVELS - 1)
    block_s, block_v, packet, line, joined, packets, line_send, line_recv, gather_send, gather_recv, spread_sem = refs

    cut = n0 // top.sets
    loads = [[pltpu.make_async_copy(source.at[pl.ds(part * cut, cut)], target.at[pl.ds(part * cut, cut)], raw_sems.at[i, part])
              for i, (source, target) in enumerate(((right_side, raw_g), (guess, raw_v)))] for part in range(top.sets)]
    for load in sum(loads, []):
        load.start()
    barrier = pltpu.get_barrier_semaphore()
    nx, ny, nz = counts

    def greet(device):
        pl.semaphore_signal(barrier, inc=1, device_id=device, device_id_type=MESH)

    def around_torus(way, far):
        return {name: lax.rem(places[axis] + way[axis] * far + counts[axis], counts[axis]) for axis, name in enumerate(AXES) if way[axis]}

    for way in WAYS:
        greet(around_torus(way, 1))

    def tell(turn):
        for way in FLAT:
            pl.semaphore_signal(spread_sem.at[turn], inc=1, device_id=around_torus(way, turn + 1), device_id_type=MESH)

    def hear(turn):
        pl.semaphore_wait(spread_sem.at[turn], len(FLAT))

    top.clear()
    top.prepare()
    write_beside(beside)
    top.missing()
    even = (lax.broadcasted_iota(jnp.int32, (n0, n0), 0) + lax.broadcasted_iota(jnp.int32, (n0, n0), 1)) % 2 == 0
    for part in range(top.sets):
        for load in loads[part]:
            load.wait()
        for k in range(part * cut // 2, (part + 1) * cut // 2):
            at = (k + 2, pl.ds(8, n0), pl.ds(0, n0))
            first, second = raw_g[2 * k], raw_g[2 * k + 1]
            gr[at] = jnp.where(even, first, second)
            gb[at] = jnp.where(even, second, first)
            b[at] = jnp.where(even, raw_v[2 * k + 1], raw_v[2 * k])
        top.pack_ends(part, False)
    top.pack(False)
    pl.semaphore_wait(barrier, len(WAYS))
    top.send()
    tell(0)
    for level in levels[1:]:
        level.prepare()
    for ring in rings.values():
        ring.clear()
    block_v[...] = jnp.zeros_like(block_v)
    top.land()
    hear(0)
    tell(1)
    top.sweep(0)
    top.sweep(1)
    top.restrict_to(levels[1].s, (EDGE, 8), pairs[0])
    for number in range(1, SHARED - 1):
        level = levels[number]
        rings[number].post()
        rings[number].land()
        level.sweep(0, zero=True, beyond=level.reach)
        level.sweep(1, beyond=level.reach - 1)
        level.restrict_to(levels[number + 1].s, (EDGE, 8), pairs[number])
    last = levels[SHARED - 1]
    last.sweep(0, zero=True, beyond=2)
    last.sweep(1, beyond=1)
    last.restrict_to(block_s, (0, 0), pairs[SHARED - 1])
    hear(1)

    bx, by, bz = blocks[SHARED]
    wide = LANES // bx
    packed = jnp.zeros((rows_of(by), LANES), jnp.float32)
    for x in range(bx):
        packed = packed + pltpu.roll(block_s[x], x * wide + places[2] * bz, 1)
    packet[...] = packed[:by]

    def line_copy(source, target):
        return pltpu.make_async_remote_copy(
            src_ref=packet, dst_ref=line.at[source], send_sem=line_send.at[target], recv_sem=line_recv.at[source],
            device_id={AXES[2]: target}, device_id_type=MESH)

    for offset in range(1, nz):
        line_copy(places[2], lax.rem(places[2] + offset, nz)).start()
    rings[1].finish()
    rings[SHARED - 1].post()
    top.sent()
    top.post(True)
    merged = packed[:by]
    for offset in range(1, nz):
        source = lax.rem(places[2] + nz - offset, nz)
        line_copy(source, lax.rem(places[2] + offset, nz)).wait_recv()
        merged = merged + line[source]
    joined[...] = merged
    total = nx * ny
    me = places[0] * ny + places[1]

    def plane_copy(to_x, to_y):
        return pltpu.make_async_remote_copy(
            src_ref=joined, dst_ref=packets.at[me], send_sem=gather_send, recv_sem=gather_recv,
            device_id={AXES[0]: to_x, AXES[1]: to_y}, device_id_type=MESH)

    xs = [lax.rem(places[0] + step, nx) for step in range(nx)]
    ys = [lax.rem(places[1] + step, ny) for step in range(ny)]
    far = lambda at: min(at[0], nx - at[0]) + min(at[1], ny - at[1])
    for to_x, to_y in sorted(itertools.product(range(nx), range(ny)), key=far, reverse=True)[:-1]:
        plane_copy(xs[to_x], ys[to_y]).start()
    packets[me] = merged
    rings[SHARED - 1].land()
    last.sweep(0, zero=True, beyond=last.reach)
    last.sweep(1, beyond=last.reach - 1)
    top.land(True)
    top.sent(True)
    for number in (SHARED - 2, SHARED - 1):
        rings[number].finish()
    for offset in range(1, nz):
        line_copy(places[2], lax.rem(places[2] + offset, nz)).wait_send()
    everyone = pltpu.make_async_remote_copy(
        src_ref=packets.at[pl.ds(0, total - 1)], dst_ref=packets.at[pl.ds(0, total - 1)], send_sem=gather_send, recv_sem=gather_recv,
        device_id={AXES[0]: places[0]}, device_id_type=MESH)
    everyone.wait_recv()
    whole = levels[SHARED]

    def unpack(px):
        for py in range(0, ny, 2):
            pair = jnp.concatenate([packets[px * ny + py], packets[px * ny + py + 1]], axis=0)
            for x in range(bx):
                whole.s[px * bx + x, pl.ds(py * by, 2 * by), :] = turn(pair, -x * wide)
    loop(nx, unpack)

    for number in range(SHARED, LEVELS - 1):
        level = levels[number]
        level.sweep(0, zero=True)
        level.sweep(1)
        level.restrict_to(levels[number + 1].s, (0, 0), pairs[number])
    level = levels[LEVELS - 1]
    level.sweep(0, zero=True)
    level.sweep(1)
    for _ in range(COARSE_SWEEPS - 1):
        level.sweep(0)
        level.sweep(1)
    for number in reversed(range(SHARED, LEVELS - 1)):
        level, below = levels[number], levels[number + 1]
        below.reflect()
        lift(below.v, below.ox, below.dims, (0, 0, 0), (1, 1, 1), level, spreads[number], centres[number])
        level.sweep(0)
        level.sweep(1)

    whole.reflect()
    shift = lax.rem(LANES - places[2] * bz, LANES)
    odd = lax.rem(places[1] + 1, 2) == 1
    for x in range(bx + 8):
        part = whole.v[places[0] * bx + (x - 4 + whole.ox), pl.ds(pl.multiple_of((places[1] + 1) // 2 * 8, 8), 24), :]
        block_v[x, pl.ds(4, 16)] = pltpu.roll(jnp.where(odd, part[4:20], part[:16]), shift, 1)
    lift(block_v, 4, blocks[SHARED], places, counts, levels[SHARED - 1], spreads[SHARED - 1], centres[SHARED - 1])
    for number in reversed(range(1, SHARED)):
        level = levels[number]
        level.sweep(0, beyond=level.reach - (1 if number == 1 else 2))
        level.sweep(1, beyond=level.reach - 3)
        level.reflect()
        lift(level.v, level.ox, level.dims, places, counts, levels[number - 1], spreads[number - 1], centres[number - 1])
    top.sweep(0)
    top.sweep(1)

    everyone.wait_send()


def finish_kernel(counts, dims, r, b, gr, gb, solution, residual, d, beside):
    places = tuple(lax.axis_index(axis) for axis in AXES)
    step = pl.program_id(0)
    n, many = dims[1], dims[0] // 2 // pl.num_programs(0)

    @pl.when(step == 0)
    def _():
        write_diagonals(d, dims, places, counts)
        write_beside(beside)
    even = (row_iota(n) + lane_iota(n)) % 2 == 0
    last = counts[0] * (dims[0] // 2) - 1
    group = solution.shape[0] // 2
    ks = [step * group + i for i in range(group)]
    globally = [places[0] * (dims[0] // 2) + k for k in ks]
    kinds = [jnp.where(at == 0, 1, jnp.where(at == last, 2, 0)) for at in globally]
    results = remainders(r, b, gr, gb, d, [k + 2 for k in ks], kinds, even, n, beside, LAST_SHARE)
    for i, (k, (red, black)) in enumerate(zip(ks, results)):
        own = (k + 2, pl.ds(8, n), slice(None))
        for out, x, y in ((solution, r[own], b[own]), (residual, red, black)):
            out[2 * i] = jnp.where(even, x, y)[:, :n]
            out[2 * i + 1] = jnp.where(even, y, x)[:, :n]


def solution(mesh):
    counts = tuple(mesh.shape[axis] for axis in AXES)

    def per_device(right_side, guess):
        shape = right_side.shape
        blocks = [tuple(side >> level for side in shape) for level in range(SHARED + 1)]
        whole = tuple(side * count for side, count in zip(blocks[SHARED], counts))
        coarse = [tuple(side >> level for side in whole) for level in range(LEVELS - SHARED)]
        grids = blocks[:SHARED] + coarse
        n0 = blocks[0][0]
        scratch = []
        vmem = lambda *dims: scratch.append(pltpu.VMEM(dims, jnp.float32))
        sems = lambda *dims: scratch.append(pltpu.SemaphoreType.DMA(dims))
        vmem(*shape)
        vmem(*shape)
        sems(2, Top.sets)
        vmem(4, n0 + 8, LANES)
        vmem(3, n0, LANES)
        scratch.append(pltpu.VMEM((2 * LANES, LANES), jnp.bfloat16))
        sent, got = Top.shapes(n0)
        for dims in sent:
            vmem(*dims)
        for way in WAYS:
            vmem(*got[way])
        sems(len(WAYS))
        sems(len(WAYS))
        for number, (x, y, z) in enumerate(grids):
            if number == 0:
                continue
            _, _, height, planes, tall = layout(number, (x, y, z))
            vmem(planes, tall, LANES)
            if number in REACH:
                vmem(planes, tall, LANES)
            else:
                vmem(x, rows_of(y), LANES)
            vmem(3, max(height, rows_of(inner_height(number, (x, y, z)) + 1)) if number in REACH else height, LANES)
            vmem(2, spare_of(number, (x, y, z))[1], LANES)
        for number in REACH:
            n = blocks[number][0]
            _, groups, cut, _, cuts = Ring.sizes(n)
            vmem(groups, n, LANES)
            if cut != n:
                vmem(cuts, n, LANES)
                vmem(cuts, n, LANES)
            for way in WAYS:
                vmem(*Ring.shape(n, REACH[number], way))
            if number < SHARED - 1:
                sems(len(WAYS))
                sems(len(WAYS))
        for number, (x, y, z) in enumerate(grids[:-1]):
            spare, tall = spare_of(number, (x, y, z))
            vmem(x // 2 + spare, max(16, tall), LANES)
        for _ in range(2):
            for number in range(LEVELS - 1):
                _, _, _, planes, tall = lift_shape(number, blocks[number + 1] if number < SHARED else grids[number + 1])
                vmem(planes, tall, LANES)
        bx, by, bz = blocks[SHARED]
        vmem(bx, rows_of(by), LANES)
        vmem(bx + 8, 24, LANES)
        vmem(by, LANES)
        vmem(counts[2], by, LANES)
        vmem(by, LANES)
        total = counts[0] * counts[1]
        vmem(total, by, LANES)
        sems(counts[2])
        sems(counts[2])
        scratch.append(pltpu.SemaphoreType.DMA)
        scratch.append(pltpu.SemaphoreType.DMA)
        scratch.append(pltpu.SemaphoreType.REGULAR((2,)))

        def kernel(*refs):
            solve_kernel(counts, blocks, coarse, refs)

        whole_block = pl.BlockSpec(memory_space=pltpu.VMEM)
        field = jax.ShapeDtypeStruct((n0 // 2 + 4, n0 + 24, LANES), jnp.float32)
        fields = pl.pallas_call(
            kernel,
            out_shape=(field,) * 4,
            in_specs=[pl.BlockSpec(memory_space=pltpu.HBM)] * 2,
            out_specs=(whole_block,) * 4,
            scratch_shapes=scratch,
            compiler_params=pltpu.CompilerParams(collective_id=0, has_side_effects=True, vmem_limit_bytes=VMEM_LIMIT * 2**20),
            name="vcycle",
        )(right_side, guess)

        def last(*refs):
            finish_kernel(counts, shape, *refs)
        block = pl.BlockSpec((16,) + shape[1:], lambda i: (i, 0, 0))
        return pl.pallas_call(
            last,
            grid=(n0 // 16,),
            out_shape=(jax.ShapeDtypeStruct(shape, jnp.float32),) * 2,
            in_specs=[whole_block] * 4,
            out_specs=(block,) * 2,
            scratch_shapes=[pltpu.VMEM((3, n0, LANES), jnp.float32), pltpu.VMEM((2 * LANES, LANES), jnp.bfloat16)],
            compiler_params=pltpu.CompilerParams(vmem_limit_bytes=8 * 2**20),
            name="finish",
        )(*fields)

    spec = P(*AXES)
    return jax.shard_map(per_device, mesh=mesh, in_specs=(spec, spec), out_specs=(spec, spec), check_vma=False)
```

```python
import itertools

import jax
import jax.numpy as jnp
from jax import lax
from jax.experimental import pallas as pl
from jax.experimental.pallas import tpu as pltpu
from jax.sharding import PartitionSpec as P

LEVELS = 7
COARSE_SWEEPS = 4
SHARED = 4
VMEM_LIMIT = 46
SWEEP_SHARE, REST_SHARE, LAST_SHARE, GRID_SHARE = 0.4, 0.4, 0.0, 0.4
LANES = 128
EDGE = 8
AXES = ("gx", "gy", "gz")
MESH = pl.DeviceIdType.MESH
WAYS = [way for way in itertools.product((-1, 0, 1), repeat=3) if any(way)]
FLAT = [way for way in WAYS if not way[2] or not (way[0] or way[1])]
FINAL = {0: 1, 1: 2, 2: 3, 3: 3}
REACH = {level: FINAL[level] + 3 for level in range(1, SHARED)}
SPARE = {SHARED - 2: 4}


def rows_of(count):
    return max(8, -(-count // 8) * 8)


def lane_iota(rows):
    return lax.broadcasted_iota(jnp.int32, (rows, LANES), 1)


def row_iota(rows):
    return lax.broadcasted_iota(jnp.int32, (rows, LANES), 0)


def loop(count, body):
    if count == 1:
        body(0)
    else:
        def step(i, carry):
            body(i)
            return carry
        lax.fori_loop(0, count, step, 0)


def turn(value, amount):
    amount = amount % LANES
    return pltpu.roll(value, amount, 1) if amount else value


def near_dot(value, matrix):
    first = value.astype(jnp.bfloat16)
    second = (value - first.astype(jnp.float32)).astype(jnp.bfloat16)
    dot = lambda part: jnp.dot(part, matrix, preferred_element_type=jnp.float32)
    return dot(second) + dot(first)


def write_beside(beside):
    k = lax.broadcasted_iota(jnp.int32, (2 * LANES, LANES), 0)
    f = lax.broadcasted_iota(jnp.int32, (2 * LANES, LANES), 1)
    apart = (k - f + 2 * LANES) % LANES
    beside[...] = jnp.where((apart == 1) | (apart == LANES - 1), 1.0, 0.0).astype(jnp.bfloat16)


def lane_sums(values, beside, share):
    many = int(len(values) * share)
    out = []
    if many:
        height = values[0].shape[0]
        value = jnp.concatenate(values[:many], axis=0)
        first = value.astype(jnp.bfloat16)
        second = (value - first.astype(jnp.float32)).astype(jnp.bfloat16)
        sums = jnp.dot(jnp.concatenate([first, second], axis=1), beside[...], preferred_element_type=jnp.float32)
        out = [sums[i * height:(i + 1) * height] for i in range(many)]
    return out + [pltpu.roll(value, 1, 1) + pltpu.roll(value, LANES - 1, 1) for value in values[many:]]


def widest(count, most, step=1):
    return max(size for size in range(step, count + 1, step) if count % size == 0 and (size <= most or size == step))


def signed(lane):
    return jnp.where(lane < 96, lane, lane - LANES)


def even_cells(height, start=0):
    return (row_iota(height) + lane_iota(height) + start) % 2 == 0


class Grid:
    def __init__(self, number, dims, places, counts, beside, r, b, gr, gb, w, d):
        self.number, self.dims, self.places, self.counts = number, dims, places, counts
        self.r, self.b, self.gr, self.gb, self.w, self.d, self.beside = r, b, gr, gb, w, d, beside
        self.reach = REACH.get(number, 0)
        self.ox, self.start, self.height, _, _ = layout(number, dims)
        self.sx, self.sy = (EDGE // 2, 8) if self.reach else (0, 0)
        self.pairs = dims[0] // 2
        self.spare, self.tall = spare_of(number, dims)

    def prepare(self):
        x, y, z = self.dims
        beyond = EDGE if self.reach else 0

        def base(height, start):
            row, lane = row_iota(height) + (start - 8), signed(lane_iota(height))
            at_y, at_z = self.places[1] * y + row, self.places[2] * z + lane
            last_y, last_z = self.counts[1] * y - 1, self.counts[2] * z - 1
            valid = (lane >= -beyond) & (lane < z + beyond) & (row >= -beyond) & (row < y + beyond)
            valid = valid & (at_y >= 0) & (at_y <= last_y) & (at_z >= 0) & (at_z <= last_z)
            one = lambda at, last: (at == 0).astype(jnp.float32) + (at == last).astype(jnp.float32)
            return valid, 6.0 + one(at_y, last_y) + one(at_z, last_z), even_cells(height, start)
        valid, diagonal, even = base(self.w.shape[1], self.start)
        plain, more = (jnp.where(valid, 1.0 / (diagonal + wall), 0.0) for wall in range(2))
        self.w[0] = plain
        self.w[1] = jnp.where(even, more, plain)
        self.w[2] = jnp.where(even, plain, more)
        self.w[3] = jnp.zeros_like(plain)
        valid, diagonal, even = base(self.tall, 8 - self.spare)
        self.d[0] = jnp.where(valid, diagonal, 0.0)
        self.d[1] = jnp.where(valid, jnp.where(even, diagonal + 1.0, diagonal), 0.0)
        self.d[2] = jnp.where(valid, jnp.where(even, diagonal, diagonal + 1.0), 0.0)
        for ref in (self.r, self.b) + ((self.gr, self.gb) if self.reach else ()):
            ref[...] = jnp.zeros_like(ref)

    def kind(self, pair, beyond):
        at = self.places[0] * self.pairs + pair
        last = self.counts[0] * self.pairs - 1
        if isinstance(at, int):
            return {0: 1, last: 2}.get(at, 0)
        kind = jnp.where(at == 0, 1, jnp.where(at == last, 2, 0))
        return jnp.where((at < 0) | (at > last), 3, kind) if beyond else kind

    def sweep(self, colour, zero=False, beyond=0):
        start, height = self.start, self.height
        if self.reach and not zero:
            start, height = start + 1, inner_height(self.number, self.dims)
        beyond = -(-beyond // 2)
        source, target, given = (self.r, self.b, self.gb) if colour else (self.b, self.r, self.gr)
        even = even_cells(height, start)
        ks = list(range(-beyond, self.pairs + beyond))
        if not zero:
            totals = around(source, [k + self.ox for k in ks], start, height, even, colour, self.beside, GRID_SHARE)
        for i, k in enumerate(ks):
            kind = self.kind(k, beyond > 0)
            weight = self.w[swapped(kind) if colour else kind, pl.ds(start - self.start, height), :]
            value = given[k + self.sx, pl.ds(start - 8 + self.sy, height), :]
            target[k + self.ox, pl.ds(start, height), :] = (value if zero else value + totals[i]) * weight

    def restrict_to(self, target, corner, pairs):
        rows, extra = self.tall, self.spare // 2
        if rows < 16:
            pairs[...] = jnp.zeros_like(pairs)
        ks = list(range(-extra, self.pairs + extra))
        ats = [k + self.ox for k in ks]
        first = 8 - self.spare
        even = even_cells(rows, first)
        reds = around(self.b, ats, first, rows, even, 0, self.beside, GRID_SHARE)
        blacks = around(self.r, ats, first, rows, even, 1, self.beside, GRID_SHARE)
        for i, k in enumerate(ks):
            kind = self.kind(k, False)
            at = (k + self.ox, pl.ds(first, rows), slice(None))
            own = (k + self.sx, pl.ds(self.sy - self.spare, rows), slice(None))
            red = self.gr[own] - (self.d[kind] * self.r[at] - reds[i])
            black = self.gb[own] - (self.d[swapped(kind)] * self.b[at] - blacks[i])
            pairs[i, pl.ds(0, rows), :] = red + black
        narrow(2 * len(ks), rows, self.dims[2], self.spare, target, [at - self.spare // 2 for at in corner], pairs)

    def reflect(self):
        (x, y, z), r, b, ox = self.dims, self.r, self.b, self.ox
        margin = 2 if self.reach else 0
        for_all = pl.ds(ox - margin, self.pairs + 2 * margin)

        def across(to, at):
            r[to] = -b[at]
            b[to] = -r[at]
        sides = (
            (0, 0, lambda: across(ox - 1, ox)),
            (0, 1, lambda: across(ox + self.pairs, ox + self.pairs - 1)),
            (1, 0, lambda: across((for_all, pl.ds(7, 1)), (for_all, pl.ds(8, 1)))),
            (1, 1, lambda: across((for_all, pl.ds(8 + y, 1)), (for_all, pl.ds(7 + y, 1)))),
        )
        for axis, high, step in sides:
            if isinstance(self.places[axis], int):
                step()
            else:
                pl.when(self.places[axis] == (self.counts[axis] - 1 if high else 0))(step)

    def planes(self, step, many, low, tall):
        even = even_cells(tall)
        out = []
        for i in range(many // 2):
            at = (step * (many // 2) + (low // 2 + i + self.ox), pl.ds(0, tall), slice(None))
            r, b = self.r[at], self.b[at]
            out += [jnp.where(even, r, b), jnp.where(even, b, r)]
        return out


def swapped(kind):
    if isinstance(kind, int):
        return {1: 2, 2: 1}.get(kind, kind)
    return jnp.where(kind == 1, 2, jnp.where(kind == 2, 1, kind))


class Block:
    def __init__(self, v, dims, places, counts):
        self.v, self.dims, self.places, self.counts = v, dims, places, counts

    def planes(self, step, many, low, tall):
        return [self.v[step * many + (low + 4 + i), pl.ds(0, tall), :] for i in range(many)]


def narrow(planes, rows, z, spare, target, corner, pairs):
    coarse_rows = rows_of(rows // 2)
    source_lane = signed(lax.broadcasted_iota(jnp.int32, (LANES, LANES), 0))
    target_lane = signed(lax.broadcasted_iota(jnp.int32, (LANES, LANES), 1))
    inside = (source_lane >= -spare) & (source_lane < z + spare)
    halve = jnp.where(((source_lane + LANES) // 2 - LANES // 2 == target_lane) & inside, 0.5, 0.0).astype(jnp.bfloat16)
    planes = planes // 2
    many = widest(planes, max(2, 512 // coarse_rows), 2)

    def second(step):
        at = pl.ds(step * many, many)
        q = pairs[at, pl.ds(0, coarse_rows, stride=2), :] + pairs[at, pl.ds(1, coarse_rows, stride=2), :]
        q = near_dot(q.reshape(many * coarse_rows, LANES), halve)
        q = q.reshape(many, coarse_rows, LANES)
        if not isinstance(target, tuple):
            target[pl.ds(step * many + corner[0], many), pl.ds(corner[1], coarse_rows), :] = q
            return
        even = even_cells(coarse_rows, corner[1])
        for i in range(many // 2):
            at = (step * (many // 2) + (corner[0] // 2 + i), pl.ds(corner[1], coarse_rows), slice(None))
            target[0][at] = jnp.where(even, q[2 * i], q[2 * i + 1])
            target[1][at] = jnp.where(even, q[2 * i + 1], q[2 * i])
    loop(planes // many, second)


def spare_of(number, dims):
    spare = SPARE.get(number, 0)
    return spare, -(-(dims[1] + 2 * spare) // 16) * 16 if spare else rows_of(dims[1])


def layout(number, dims):
    x, y, z = dims
    if number in REACH:
        reach = REACH[number]
        height = rows_of(y + 2 * reach)
        return EDGE // 2, 8 - reach, height, x // 2 + EDGE, max(40, y + 24)
    if number == SHARED:
        return EDGE // 2, 8, rows_of(y), x // 2 + EDGE, rows_of(y) + 24
    return 1, 8, rows_of(y), x // 2 + 2, rows_of(y) + 16


def inner_height(number, dims):
    return rows_of(dims[1] + 2 * REACH[number] - 2)


def below_zero(number):
    return -((FINAL[number] + 3) // 2) if number in FINAL else 0


def lift_shape(number, coarse):
    low = below_zero(number)
    count = coarse[0] - 2 * low
    height = rows_of(coarse[1] - 2 * low)
    first = (low - 1) // 2 * 2
    return low, count, height, first, -(-(low + count + 1 - first) // 2) * 2, rows_of(8 + low + height + 1)


def widen(below, number, spread, centre):
    dims, places, counts = below.dims, below.places, below.counts
    z = dims[2]
    _, _, _, start, planes, tall = lift_shape(number, dims)
    beyond = EDGE if number in FINAL else 0
    k = signed(lax.broadcasted_iota(jnp.int32, (LANES, LANES), 0))
    f = signed(lax.broadcasted_iota(jnp.int32, (LANES, LANES), 1))
    at = places[2] * (2 * z) + f
    inside = (f >= -beyond) & (f < 2 * z + beyond) & (at >= 0) & (at < counts[2] * 2 * z)
    parent = (f + LANES) // 2 - LANES // 2
    near = parent + jnp.where((f + LANES) % 2 == 1, 1, -1)
    outside = (places[2] * z + near < 0) | (places[2] * z + near >= counts[2] * z)
    own = jnp.where((k == parent) & inside, 0.25, 0.0)
    beside = jnp.where((k == near) & inside, 0.25, 0.0)
    both = own + jnp.where(outside, -own, beside)
    matrix = jnp.concatenate([own, both], axis=1).astype(jnp.bfloat16)
    many = widest(planes, max(2, 1024 // tall), 2)

    def first(step):
        e = jnp.concatenate(below.planes(step, many, start, tall), axis=0)
        product = near_dot(e, matrix)
        at = pl.ds(step * many, many)
        spread[at] = product[:, :LANES].reshape(many, tall, LANES)
        centre[at] = product[:, LANES:].reshape(many, tall, LANES)
    loop(planes // many, first)


def lift(below, fine, spread, centre):
    (x, y, z), places, counts = below.dims, below.places, below.counts
    number = fine.number
    low, count, height, start, _, _ = lift_shape(number, below.dims)
    beyond = number in FINAL
    widen(below, number, spread, centre)
    group = widest(count, max(1, 512 // height))
    row = places[1] * y + row_iota(height) + low
    valid = (row >= 0) & (row < counts[1] * y)
    even = lane_iota(height) % 2 == 0
    skip = low - start

    def second(step):
        for i in range(group):
            plane = step * group + i
            middle = centre[plane + skip, pl.ds(8 + low, height), :]
            ys = (spread[plane + skip, pl.ds(7 + low, height), :], spread[plane + skip, pl.ds(9 + low, height), :])
            xs = [spread[plane + skip + 2 * up_x - 1, pl.ds(8 + low, height), :] for up_x in range(2)]
            here = valid
            if beyond:
                at = places[0] * x + plane + low
                here = valid & ((at >= 0) & (at < counts[0] * x))
            for up_y in range(2):
                q = (middle + ys[up_y]) + jnp.where(even, xs[1 - up_y], xs[up_y])
                if beyond or y < height:
                    q = jnp.where(here, q, 0.0)
                at = (plane + low + fine.ox, pl.ds(8 + 2 * low + up_y, height, stride=2), slice(None))
                fine.b[at] = fine.b[at] + q
    loop(count // group, second)


def exists(places, counts, way, sign):
    found = None
    for axis in range(3):
        if way[axis]:
            other = places[axis] + sign * way[axis]
            one = (other >= 0) if sign * way[axis] < 0 else (other < counts[axis])
            found = one if found is None else found & one
    return found


def along(places, way):
    return {name: places[axis] + way[axis] for axis, name in enumerate(AXES) if way[axis]}


class Top:
    number, ox, sets = 0, 2, 4

    def __init__(self, dims, places, counts, beside, r, b, gr, gb, w, d, out, got, sems):
        self.beside = beside
        self.dims, self.places, self.counts = dims, places, counts
        self.r, self.b, self.gr, self.gb, self.w, self.d = r, b, gr, gb, w, d
        self.out, self.got, self.sems = out, got, sems
        self.pairs, self.n = dims[0] // 2, dims[1]

    @staticmethod
    def weights(dims, places, counts, height, start, beyond):
        x, y, z = dims
        row, lane = row_iota(height) + (start - 8), signed(lane_iota(height))
        at_y, at_z = places[1] * y + row, places[2] * z + lane
        last_y, last_z = counts[1] * y - 1, counts[2] * z - 1
        valid = (lane >= -beyond) & (lane < z + beyond) & (at_y >= 0) & (at_y <= last_y) & (at_z >= 0) & (at_z <= last_z)
        one = lambda at, last: (at == 0).astype(jnp.float32) + (at == last).astype(jnp.float32)
        return valid, 6.0 + one(at_y, last_y) + one(at_z, last_z), (row + lane + LANES) % 2 == 0

    def clear(self):
        for ref in (self.r, self.b, self.gr, self.gb):
            ref[...] = jnp.zeros_like(ref)

    def prepare(self):
        valid, diagonal, even = self.weights(self.dims, self.places, self.counts, self.n + 8, 6, 4)
        plain, more = (jnp.where(valid, 1.0 / (diagonal + wall), 0.0) for wall in range(2))
        self.w[0] = plain
        self.w[1] = jnp.where(even, more, plain)
        self.w[2] = jnp.where(even, plain, more)
        self.w[3] = jnp.zeros_like(plain)
        write_diagonals(self.d, self.dims, self.places, self.counts)

    def missing(self):
        for way in WAYS:
            @pl.when(jnp.logical_not(exists(self.places, self.counts, way, -1)))
            def _(way=way):
                self.got[way][...] = jnp.zeros_like(self.got[way])

    def kind(self, pair):
        at = self.places[0] * self.pairs + pair
        last = self.counts[0] * self.pairs - 1
        return jnp.where((at < 0) | (at > last), 3, jnp.where(at == 0, 1, jnp.where(at == last, 2, 0)))

    def sweep(self, colour):
        start, height = 6, self.n + 8
        source, target, given = (self.r, self.b, self.gb) if colour else (self.b, self.r, self.gr)
        count = self.pairs + 2
        chunk = widest(count, 17)
        even = (row_iota(height) + lane_iota(height)) % 2 == 0

        def body(step):
            ats = [step * chunk + i + 1 for i in range(chunk)]
            for at, total in zip(ats, around(source, ats, start, height, even, colour, self.beside, SWEEP_SHARE)):
                k = at - 2
                kind = self.kind(k)
                if colour:
                    kind = jnp.where(kind == 1, 2, jnp.where(kind == 2, 1, kind))
                target[at, pl.ds(start, height), :] = (given[at, pl.ds(start, height), :] + total) * self.w[kind]
        loop(count // chunk, body)

    def restrict_to(self, target, corner, pairs):
        n = self.n
        even = (row_iota(n) + lane_iota(n)) % 2 == 0
        chunk = 8

        def body(step):
            ks = [step * chunk + i for i in range(chunk)]
            kinds = [self.kind(k) for k in ks]
            ats = [k + 2 for k in ks]
            for k, (red, black) in zip(ks, remainders(self.r, self.b, self.gr, self.gb, self.d, ats, kinds, even, n, self.beside, REST_SHARE)):
                pairs[k] = red + black
        loop(self.pairs // chunk, body)
        narrow(self.dims[0], n, self.dims[2], 0, target, corner, pairs)

    @staticmethod
    def shapes(n):
        face = {0: (2, n, LANES), 1: (n // 4, 8, LANES), 2: (3, n, LANES)}
        sent = [face[0], face[0], face[1], face[1], face[2], face[2], (4, 8, LANES)]
        got = {}
        for way in WAYS:
            if sum(map(abs, way)) == 1:
                got[way] = face[[abs(part) for part in way].index(1)]
            elif not way[2]:
                got[way] = (2, 8, LANES)
            elif not way[0]:
                got[way] = (2, 8, LANES)
            else:
                got[way] = (8, LANES)
        return sent, got

    def copies(self, way, again):
        n, out, got = self.n, self.out, self.got[way]
        high = [part > 0 for part in way]
        if sum(map(abs, way)) == 1:
            axis = [abs(part) for part in way].index(1)
            source = out[2 * axis + high[axis]]
            if again and axis != 1:
                source, got = source.at[pl.ds(0, 1)], got.at[pl.ds(0, 1)]
        elif not way[2]:
            source = out[2 + high[1]].at[pl.ds(n // 4 - 2 if high[0] else 0, 2)]
        elif not way[0]:
            row = pl.ds(n - 8 if high[1] else 0, 8)
            source = out[4 + high[2]].at[pl.ds(0, 2), row]
        else:
            source = out[6].at[2 * high[0] + high[2]]
        k = WAYS.index(way)
        return pltpu.make_async_remote_copy(
            src_ref=source, dst_ref=got, send_sem=self.sems[0].at[k], recv_sem=self.sems[1].at[k],
            device_id=along(self.places, way), device_id_type=MESH)

    def pack_ends(self, part, again):
        tile = lane_iota(8)
        many = self.pairs // self.sets
        ahead = (tile + (LANES - 60)) % LANES
        wide = 4 * many
        for t in range(self.n // 8):
            at = pl.ds(8 * t, 8)
            for index, ref in enumerate([self.b] if again else [self.b, self.gr, self.gb]):
                first = last = None
                for k in range(part * many, part * many + many):
                    moved = turn(ref[k + 2, pl.ds(8 * t + 8, 8), :], 4 * k)
                    first = moved if first is None else jnp.where(tile // 4 == k, moved, first)
                    last = moved if last is None else jnp.where(ahead // 4 == k, moved, last)
                if part:
                    first = jnp.where(tile // wide == part, first, self.out[4][index, at])
                    last = jnp.where(ahead // wide == part, last, self.out[5][index, at])
                self.out[4][index, at] = first
                self.out[5][index, at] = last

    def pack(self, again):
        n, pairs = self.n, self.pairs
        low, tile = lane_iota(n) < 64, lane_iota(8)
        row = row_iota(8)
        half = pairs // 2
        own = lambda ref, k: ref[k + 2, pl.ds(8, n), :]
        for high in range(2):
            near, far = (pairs - 1, pairs - 2) if high else (0, 1)
            self.out[high][0] = jnp.where(low, own(self.b, near), pltpu.roll(own(self.b, far), 64, 1))
            if not again:
                self.out[high][1] = jnp.where(low, own(self.gr, near), pltpu.roll(own(self.gb, near), 64, 1))

            def edge(k, high=high):
                first = 8 + n - 8 if high else 8
                b = self.b[k + 2, pl.ds(first, 8), :]
                if again:
                    return b
                red, black = (pltpu.roll(ref[k + 2, pl.ds(first, 8), :], by, 0) for ref, by in ((self.gr, 4), (self.gb, 2 if high else 6)))
                if high:
                    return jnp.where(row >= 4, b, jnp.where(row >= 2, red, black))
                return jnp.where(row < 4, b, jnp.where(row < 6, red, black))
            for k in range(half):
                self.out[2 + high][k] = jnp.where(tile < 64, edge(k), pltpu.roll(edge(k + half), 64, 1))
        for high_x in range(2):
            for high_z in range(2):
                offset = 60 if high_z else 0
                pair, near = (pairs - 2, pairs - 1) if high_x else (0, 0)
                value = jnp.zeros((8, LANES), jnp.float32)
                for t in range(n // 8):
                    rows = pl.ds(8 * t, 8)
                    moved = turn(self.out[4 + high_z][0, rows], 16 * t - 4 * pair - offset)
                    value = jnp.where((tile >= 16 * t) & (tile < 16 * t + 8), moved, value)
                    if not again:
                        moved = turn(self.out[4 + high_z][1, rows], 16 * t + 8 - 4 * near - offset)
                        value = jnp.where((tile >= 16 * t + 8) & (tile < 16 * t + 16), moved, value)
                self.out[6][2 * high_x + high_z] = value

    def post(self, again=False):
        for part in range(self.sets):
            self.pack_ends(part, again)
        self.pack(again)
        self.send(again)

    def send(self, again=False):
        for way in WAYS:
            pl.when(exists(self.places, self.counts, way, 1))(self.copies(way, again).start)

    def sent(self, again=False):
        for way in WAYS:
            pl.when(exists(self.places, self.counts, way, 1))(self.copies(way, again).wait_send)

    def wait(self, ways, again):
        for way in ways:
            pl.when(exists(self.places, self.counts, way, -1))(self.copies(way, again).wait_recv)

    def land(self, again=False):
        n, pairs, got = self.n, self.pairs, self.got
        half = pairs // 2
        arrays = [self.b] if again else [self.b, self.gr, self.gb]
        lane, tile = lane_iota(n), lane_iota(8)

        def ends(high, low, to, k):
            pick = to % 8 < 4
            return turn(jnp.where(pick, high, low) if k % 2 == 0 else jnp.where(pick, low, high), 64 - 4 * k)
        self.wait([way for way in WAYS if not (way[0] or way[1])], again)
        high, low = got[(0, 0, -1)], got[(0, 0, 1)]

        def body(t):
            at = pl.ds(pl.multiple_of(t * 8, 8), 8)
            packs = [(high[index, at], low[index, at]) for index in range(len(arrays))]
            for k in range(pairs):
                own = (k + 2, pl.ds(pl.multiple_of(t * 8 + 8, 8), 8), slice(None))
                for (h, l), ref in zip(packs, arrays):
                    ref[own] = jnp.where(tile < 64, ref[own], ends(h, l, tile, k))
        loop(n // 8, body)
        self.wait([way for way in WAYS if way[1] and not way[0]], again)
        for side in (-1, 1):
            face = got[(0, -side, 0)]
            base = 8 + n if side > 0 else 0
            shifts = (0, 4, 2 if side > 0 else 6)
            for index, ref in enumerate(arrays):
                if index < 2:
                    h, l = got[(0, -side, -1)][index], got[(0, -side, 1)][index]
                for k in range(pairs):
                    value = face[k % half]
                    if k >= half:
                        value = pltpu.roll(value, 64, 1)
                    if shifts[index]:
                        value = pltpu.roll(value, shifts[index], 0)
                    if index < 2:
                        value = jnp.where(tile < 64, value, ends(h, l, tile, k))
                    ref[k + 2, pl.ds(base, 8), :] = value
        self.wait([way for way in WAYS if way[0]], again)
        for side in (-1, 1):
            face = got[(-side, 0, 0)]
            near, far = (pairs + 2, pairs + 3) if side > 0 else (1, 0)
            high, low = got[(-side, 0, -1)], got[(-side, 0, 1)]
            near_lane, far_lane = (0, 4) if side > 0 else (4, 0)

            def beside(first, at, high=high, low=low):
                out = []
                for t in at:
                    up = turn(high[...], 64 - 16 * t - first)
                    out.append(jnp.where(tile < 96, up, turn(low[...], 124 - 16 * t - first)))
                return jnp.concatenate(out, axis=0) if len(out) > 1 else out[0]
            every = range(n // 8)
            both = face[0]
            self.b[near, pl.ds(8, n), :] = jnp.where(lane < 64, both, beside(near_lane, every))
            self.b[far, pl.ds(8, n), :] = jnp.where(lane < 64, pltpu.roll(both, 64, 1), beside(far_lane, every))
            if not again:
                both = face[1]
                self.gr[near, pl.ds(8, n), :] = jnp.where(lane < 64, both, beside(8, every))
                self.gb[near, pl.ds(8, n), :] = pltpu.roll(both, 64, 1)
            for up in (-1, 1):
                edge = got[(-side, -up, 0)]
                base = 8 + n if up > 0 else 0
                corner = (got[(-side, -up, -1)], got[(-side, -up, 1)])
                t = [0 if up > 0 else n // 8 - 1]
                if side > 0:
                    pieces = {near: (0, False), far: (1, False)}
                else:
                    pieces = {near: (1, True), far: (0, True)}
                for place, (group, upper) in pieces.items():
                    value = edge[group]
                    if upper:
                        value = pltpu.roll(value, 64, 1)
                    first = near_lane if place == near else far_lane
                    self.b[place, pl.ds(base, 8), :] = jnp.where(tile < 64, value, beside(first, t, *corner))
                    if place == near and not again:
                        self.gr[place, pl.ds(base, 8), :] = pltpu.roll(value, 4, 0)


def around(source, ats, start, height, even, colour, beside, share):
    rows = pl.ds(start, height)
    centres = [source[at, rows, :] for at in ats]
    out = []
    for at, s, z_sum in zip(ats, centres, lane_sums(centres, beside, share)):
        left, right = source[at - 1, rows, :], source[at + 1, rows, :]
        across = jnp.where(even, right, left) if colour else jnp.where(even, left, right)
        total = (s + across) + (source[at, pl.ds(start + 1, height), :] + source[at, pl.ds(start - 1, height), :])
        out.append(total + z_sum)
    return out


def remainders(r, b, gr, gb, d, ats, kinds, even, n, beside, share):
    rows = pl.ds(8, n)
    out = []
    for at, kind, reds, blacks in zip(ats, kinds, around(b, ats, 8, n, even, 0, beside, share), around(r, ats, 8, n, even, 1, beside, share)):
        other = swapped(kind)
        out.append((gr[at, rows, :] - (d[kind] * r[at, rows, :] - reds), gb[at, rows, :] - (d[other] * b[at, rows, :] - blacks)))
    return out


def write_diagonals(d, dims, places, counts):
    _, diagonal, even = Top.weights(dims, places, counts, dims[1], 8, 0)
    d[0] = diagonal
    d[1] = jnp.where(even, diagonal + 1.0, diagonal)
    d[2] = jnp.where(even, diagonal, diagonal + 1.0)


class Ring:
    def __init__(self, level, refs, sems):
        self.level, self.sems = level, sems
        self.body, self.parts = refs[0], refs[1:-len(WAYS)]
        self.got = dict(zip(WAYS, refs[-len(WAYS):]))
        self.places, self.counts = level.places, level.counts

    @staticmethod
    def sizes(n):
        each = LANES // n
        cut = n if n <= 16 else 8
        return each, max(1, n // each), cut, LANES // cut, max(1, n * cut // LANES)

    @staticmethod
    def thick(n, reach, way):
        each, groups, _, _, cuts = Ring.sizes(n)
        if not way[0]:
            return cuts if way[2] else groups
        return 1 if way[2] else -(-reach // each)

    @staticmethod
    def shape(n, reach, way):
        return (Ring.thick(n, reach, way), 8 if way[1] else n, LANES)

    def clear(self):
        for way in WAYS:
            @pl.when(jnp.logical_not(exists(self.places, self.counts, way, -1)))
            def _(way=way):
                self.got[way][...] = jnp.zeros_like(self.got[way])

    def copy(self, way):
        n = self.level.dims[0]
        shape = Ring.shape(n, self.level.reach, way)
        source = self.body
        if way[2] and self.parts:
            source = self.parts[0] if way[2] < 0 else self.parts[1]
        groups = source.shape[0]
        group = 0 if way[0] <= 0 else groups - shape[0]
        row = 0 if way[1] <= 0 else n - 8
        k = WAYS.index(way)
        return pltpu.make_async_remote_copy(
            src_ref=source.at[pl.ds(group, shape[0]), pl.ds(row, shape[1])], dst_ref=self.got[way],
            send_sem=self.sems[0].at[k], recv_sem=self.sems[1].at[k],
            device_id={name: self.places[axis] + way[axis] for axis, name in enumerate(AXES) if way[axis]}, device_id_type=MESH)

    def post(self):
        n, gr, gb = self.level.dims[0], self.level.gr, self.level.gb
        each, groups, cut, cuts_each, cuts = Ring.sizes(n)
        even = even_cells(n)

        def plane(x):
            at = (x // 2 + EDGE // 2, pl.ds(8, n), slice(None))
            value = jnp.where(even, gb[at], gr[at]) if x % 2 else jnp.where(even, gr[at], gb[at])
            return jnp.where(lane_iota(n) < n, value, 0.0) if SPARE.get(self.level.number - 1) else value
        for g in range(groups):
            value = plane(g * each)
            for i in range(1, min(each, n)):
                value = value + turn(plane(g * each + i), i * n)
            self.body[g] = value
        if self.parts:
            lane = lane_iota(n)
            for g in range(cuts):
                low = high = jnp.zeros((n, LANES), jnp.float32)
                for i in range(cuts_each):
                    moved = turn(plane(g * cuts_each + i), cut * i)
                    low = jnp.where(lane // cut == i, moved, low)
                    high = jnp.where((lane + (LANES - n + cut)) % LANES // cut == i, moved, high)
                self.parts[0][g] = low
                self.parts[1][g] = high
        for way in WAYS:
            pl.when(exists(self.places, self.counts, way, 1))(self.copy(way).start)

    def land(self):
        n, gr, gb, reach = self.level.dims[0], self.level.gr, self.level.gb, self.level.reach
        reach += reach % 2
        each, groups, cut, cuts_each, cuts = Ring.sizes(n)
        for to_x, to_y in sorted(itertools.product((-1, 0, 1), repeat=2), key=lambda at: abs(at[0]) * 3 + abs(at[1])):
            for way in WAYS:
                if way[:2] == (-to_x, -to_y):
                    pl.when(exists(self.places, self.counts, way, -1))(self.copy(way).wait_recv)
            height = 8 if to_y else n
            row = {-1: 0, 0: 8, 1: 8 + n}[to_y]
            lane = lane_iota(height)
            body = self.got[(-to_x, -to_y, 0)] if to_x or to_y else None
            high = self.got[(-to_x, -to_y, -1)]
            low = self.got[(-to_x, -to_y, 1)]

            made = {}

            def merged(h, flip, made=made, high=high, low=low, lane=lane):
                if (h, flip) not in made:
                    both = (high[h], turn(low[h], -2 * n))
                    made[h, flip] = jnp.where(lane % 16 < 8, both[flip], both[1 - flip])
                return made[h, flip]
            even = even_cells(height, row)

            def value(x, body=body, high=high, low=low, lane=lane, merged=merged, to_x=to_x):
                g, h = x // each, x // cuts_each
                if to_x < 0:
                    g, h = g - (groups - body.shape[0]), h - (cuts - high.shape[0])
                if n == 8:
                    ends = jnp.where(lane < 64, turn(high[h], n - cut * (x % cuts_each)), turn(low[h], -n - cut * (x % cuts_each)))
                else:
                    ends = turn(merged(h, x % 2 if n == 32 else 0), n - cut * (x % cuts_each))
                return ends if body is None else jnp.where(lane < n, turn(body[g], -(x % each) * n), ends)
            for x in {-1: range(n - reach, n, 2), 0: range(0, n, 2), 1: range(0, reach, 2)}[to_x]:
                at = (EDGE // 2 + (to_x * n + x) // 2, pl.ds(row, height), slice(None))
                first, second = value(x), value(x + 1)
                red, black = jnp.where(even, first, second), jnp.where(even, second, first)
                if body is None:
                    red, black = jnp.where(lane < n, gr[at], red), jnp.where(lane < n, gb[at], black)
                gr[at] = red
                gb[at] = black

    def finish(self):
        for way in WAYS:
            pl.when(exists(self.places, self.counts, way, 1))(self.copy(way).wait_send)


def solve_kernel(counts, blocks, coarse, refs):
    right_side, guess, r, b, gr, gb = refs[:6]
    refs = list(refs[6:])
    take = lambda count=1: [refs.pop(0) for _ in range(count)] if count > 1 else refs.pop(0)
    places = tuple(lax.axis_index(axis) for axis in AXES)
    n0 = blocks[0][0]
    raw_g, raw_v, raw_sems = take(3)
    sent_shapes, got_shapes = Top.shapes(n0)
    w0, d0, beside = take(3)
    top = Top(blocks[0], places, counts, beside, r, b, gr, gb, w0, d0, take(len(sent_shapes)), dict(zip(WAYS, take(len(WAYS)))), take(2))
    levels = [top]
    for number in range(1, LEVELS):
        if number < SHARED:
            levels.append(Grid(number, blocks[number], places, counts, beside, *take(6)))
        else:
            levels.append(Grid(number, coarse[number - SHARED], (0, 0, 0), (1, 1, 1), beside, *take(6)))
    rings = {}
    for number in REACH:
        n = blocks[number][0]
        members = take(1 + (2 if Ring.sizes(n)[2] != n else 0) + len(WAYS))
        rings[number] = Ring(levels[number], members, take(2) if number < SHARED - 1 else rings[1].sems)
    pairs = take(LEVELS - 1)
    spreads = take(LEVELS - 1)
    centres = take(LEVELS - 1)
    block_s, block_v, packet, line, joined, packets, line_send, line_recv, gather_send, gather_recv, spread_sem = refs

    cut = n0 // top.sets
    loads = [[pltpu.make_async_copy(source.at[pl.ds(part * cut, cut)], target.at[pl.ds(part * cut, cut)], raw_sems.at[i, part])
              for i, (source, target) in enumerate(((right_side, raw_g), (guess, raw_v)))] for part in range(top.sets)]
    for load in sum(loads, []):
        load.start()
    barrier = pltpu.get_barrier_semaphore()
    nx, ny, nz = counts

    def greet(device):
        pl.semaphore_signal(barrier, inc=1, device_id=device, device_id_type=MESH)

    def around_torus(way, far):
        return {name: lax.rem(places[axis] + way[axis] * far + counts[axis], counts[axis]) for axis, name in enumerate(AXES) if way[axis]}

    for way in WAYS:
        greet(around_torus(way, 1))

    def tell(turn):
        for way in FLAT:
            pl.semaphore_signal(spread_sem.at[turn], inc=1, device_id=around_torus(way, turn + 1), device_id_type=MESH)

    def hear(turn):
        pl.semaphore_wait(spread_sem.at[turn], len(FLAT))

    top.clear()
    top.prepare()
    write_beside(beside)
    top.missing()
    even = (lax.broadcasted_iota(jnp.int32, (n0, n0), 0) + lax.broadcasted_iota(jnp.int32, (n0, n0), 1)) % 2 == 0
    for part in range(top.sets):
        for load in loads[part]:
            load.wait()
        for k in range(part * cut // 2, (part + 1) * cut // 2):
            at = (k + 2, pl.ds(8, n0), pl.ds(0, n0))
            first, second = raw_g[2 * k], raw_g[2 * k + 1]
            gr[at] = jnp.where(even, first, second)
            gb[at] = jnp.where(even, second, first)
            b[at] = jnp.where(even, raw_v[2 * k + 1], raw_v[2 * k])
        top.pack_ends(part, False)
    top.pack(False)
    pl.semaphore_wait(barrier, len(WAYS))
    top.send()
    tell(0)
    for level in levels[1:]:
        level.prepare()
    for ring in rings.values():
        ring.clear()
    block_v[...] = jnp.zeros_like(block_v)
    top.land()
    hear(0)
    tell(1)
    top.sweep(0)
    top.sweep(1)
    top.restrict_to((levels[1].gr, levels[1].gb), (EDGE, 8), pairs[0])
    for number in range(1, SHARED - 1):
        level = levels[number]
        rings[number].post()
        rings[number].land()
        level.sweep(0, zero=True, beyond=level.reach)
        level.sweep(1, beyond=level.reach - 1)
        level.restrict_to((levels[number + 1].gr, levels[number + 1].gb), (EDGE, 8), pairs[number])
    last = levels[SHARED - 1]
    last.sweep(0, zero=True, beyond=2)
    last.sweep(1, beyond=1)
    last.restrict_to(block_s, (0, 0), pairs[SHARED - 1])
    hear(1)

    bx, by, bz = blocks[SHARED]
    wide = LANES // bx
    packed = jnp.zeros((rows_of(by), LANES), jnp.float32)
    for x in range(bx):
        packed = packed + pltpu.roll(block_s[x], x * wide + places[2] * bz, 1)
    packet[...] = packed[:by]

    def line_copy(source, target):
        return pltpu.make_async_remote_copy(
            src_ref=packet, dst_ref=line.at[source], send_sem=line_send.at[target], recv_sem=line_recv.at[source],
            device_id={AXES[2]: target}, device_id_type=MESH)

    for offset in range(1, nz):
        line_copy(places[2], lax.rem(places[2] + offset, nz)).start()
    rings[1].finish()
    rings[SHARED - 1].post()
    top.sent()
    top.post(True)
    merged = packed[:by]
    for offset in range(1, nz):
        source = lax.rem(places[2] + nz - offset, nz)
        line_copy(source, lax.rem(places[2] + offset, nz)).wait_recv()
        merged = merged + line[source]
    joined[...] = merged
    total = nx * ny
    me = places[0] * ny + places[1]

    def plane_copy(to_x, to_y):
        return pltpu.make_async_remote_copy(
            src_ref=joined, dst_ref=packets.at[me], send_sem=gather_send, recv_sem=gather_recv,
            device_id={AXES[0]: to_x, AXES[1]: to_y}, device_id_type=MESH)

    xs = [lax.rem(places[0] + step, nx) for step in range(nx)]
    ys = [lax.rem(places[1] + step, ny) for step in range(ny)]
    far = lambda at: min(at[0], nx - at[0]) + min(at[1], ny - at[1])
    for to_x, to_y in sorted(itertools.product(range(nx), range(ny)), key=far, reverse=True)[:-1]:
        plane_copy(xs[to_x], ys[to_y]).start()
    packets[me] = merged
    rings[SHARED - 1].land()
    last.sweep(0, zero=True, beyond=last.reach)
    last.sweep(1, beyond=last.reach - 1)
    top.land(True)
    top.sent(True)
    for number in (SHARED - 2, SHARED - 1):
        rings[number].finish()
    for offset in range(1, nz):
        line_copy(places[2], lax.rem(places[2] + offset, nz)).wait_send()
    everyone = pltpu.make_async_remote_copy(
        src_ref=packets.at[pl.ds(0, total - 1)], dst_ref=packets.at[pl.ds(0, total - 1)], send_sem=gather_send, recv_sem=gather_recv,
        device_id={AXES[0]: places[0]}, device_id_type=MESH)
    everyone.wait_recv()
    whole = levels[SHARED]

    def unpack(px):
        for py in range(0, ny, 2):
            pair = jnp.concatenate([packets[px * ny + py], packets[px * ny + py + 1]], axis=0)
            cells = even_cells(2 * by)
            for x in range(0, bx, 2):
                first, second = turn(pair, -x * wide), turn(pair, -(x + 1) * wide)
                at = (px * (bx // 2) + x // 2, pl.ds(py * by, 2 * by), slice(None))
                whole.gr[at] = jnp.where(cells, first, second)
                whole.gb[at] = jnp.where(cells, second, first)
    loop(nx, unpack)

    for number in range(SHARED, LEVELS - 1):
        level = levels[number]
        level.sweep(0, zero=True)
        level.sweep(1)
        level.restrict_to((levels[number + 1].gr, levels[number + 1].gb), (0, 0), pairs[number])
    level = levels[LEVELS - 1]
    level.sweep(0, zero=True)
    level.sweep(1)
    for _ in range(COARSE_SWEEPS - 1):
        level.sweep(0)
        level.sweep(1)
    for number in reversed(range(SHARED, LEVELS - 1)):
        level, below = levels[number], levels[number + 1]
        below.reflect()
        lift(below, level, spreads[number], centres[number])
        level.sweep(0)
        level.sweep(1)

    whole.reflect()
    shift = lax.rem(LANES - places[2] * bz, LANES)
    odd = lax.rem(places[1] + 1, 2) == 1
    cells = even_cells(24)
    for x in range(0, bx + 8, 2):
        at = (places[0] * (bx // 2) + (x // 2 - 2 + whole.ox), pl.ds(pl.multiple_of((places[1] + 1) // 2 * 8, 8), 24), slice(None))
        r_part, b_part = whole.r[at], whole.b[at]
        for i, part in enumerate((jnp.where(cells, r_part, b_part), jnp.where(cells, b_part, r_part))):
            block_v[x + i, pl.ds(4, 16)] = pltpu.roll(jnp.where(odd, part[4:20], part[:16]), shift, 1)
    around_block = Block(block_v, blocks[SHARED], places, counts)
    lift(around_block, levels[SHARED - 1], spreads[SHARED - 1], centres[SHARED - 1])
    for number in reversed(range(1, SHARED)):
        level = levels[number]
        level.sweep(0, beyond=level.reach - 2)
        level.sweep(1, beyond=level.reach - 3)
        level.reflect()
        lift(level, levels[number - 1], spreads[number - 1], centres[number - 1])
    top.sweep(0)
    top.sweep(1)

    everyone.wait_send()


def finish_kernel(counts, dims, r, b, gr, gb, solution, residual, d, beside):
    places = tuple(lax.axis_index(axis) for axis in AXES)
    step = pl.program_id(0)
    n, many = dims[1], dims[0] // 2 // pl.num_programs(0)

    @pl.when(step == 0)
    def _():
        write_diagonals(d, dims, places, counts)
        write_beside(beside)
    even = (row_iota(n) + lane_iota(n)) % 2 == 0
    last = counts[0] * (dims[0] // 2) - 1
    group = solution.shape[0] // 2
    ks = [step * group + i for i in range(group)]
    globally = [places[0] * (dims[0] // 2) + k for k in ks]
    kinds = [jnp.where(at == 0, 1, jnp.where(at == last, 2, 0)) for at in globally]
    results = remainders(r, b, gr, gb, d, [k + 2 for k in ks], kinds, even, n, beside, LAST_SHARE)
    for i, (k, (red, black)) in enumerate(zip(ks, results)):
        own = (k + 2, pl.ds(8, n), slice(None))
        for out, x, y in ((solution, r[own], b[own]), (residual, red, black)):
            out[2 * i] = jnp.where(even, x, y)[:, :n]
            out[2 * i + 1] = jnp.where(even, y, x)[:, :n]


def solution(mesh):
    counts = tuple(mesh.shape[axis] for axis in AXES)

    def per_device(right_side, guess):
        shape = right_side.shape
        blocks = [tuple(side >> level for side in shape) for level in range(SHARED + 1)]
        whole = tuple(side * count for side, count in zip(blocks[SHARED], counts))
        coarse = [tuple(side >> level for side in whole) for level in range(LEVELS - SHARED)]
        grids = blocks[:SHARED] + coarse
        n0 = blocks[0][0]
        scratch = []
        vmem = lambda *dims: scratch.append(pltpu.VMEM(dims, jnp.float32))
        sems = lambda *dims: scratch.append(pltpu.SemaphoreType.DMA(dims))
        vmem(*shape)
        vmem(*shape)
        sems(2, Top.sets)
        vmem(4, n0 + 8, LANES)
        vmem(3, n0, LANES)
        scratch.append(pltpu.VMEM((2 * LANES, LANES), jnp.bfloat16))
        sent, got = Top.shapes(n0)
        for dims in sent:
            vmem(*dims)
        for way in WAYS:
            vmem(*got[way])
        sems(len(WAYS))
        sems(len(WAYS))
        for number, (x, y, z) in enumerate(grids):
            if number == 0:
                continue
            _, _, height, extent, tall = layout(number, (x, y, z))
            vmem(extent, tall, LANES)
            vmem(extent, tall, LANES)
            for _ in range(2):
                vmem(*((extent, tall) if number in REACH else (x // 2, rows_of(y))), LANES)
            vmem(4, max(height, rows_of(inner_height(number, (x, y, z)) + 1)) if number in REACH else height, LANES)
            vmem(3, spare_of(number, (x, y, z))[1], LANES)
        for number in REACH:
            n = blocks[number][0]
            _, groups, cut, _, cuts = Ring.sizes(n)
            vmem(groups, n, LANES)
            if cut != n:
                vmem(cuts, n, LANES)
                vmem(cuts, n, LANES)
            for way in WAYS:
                vmem(*Ring.shape(n, REACH[number], way))
            if number < SHARED - 1:
                sems(len(WAYS))
                sems(len(WAYS))
        for number, (x, y, z) in enumerate(grids[:-1]):
            spare, tall = spare_of(number, (x, y, z))
            vmem(x // 2 + spare, max(16, tall), LANES)
        for _ in range(2):
            for number in range(LEVELS - 1):
                _, _, _, _, planes, tall = lift_shape(number, blocks[number + 1] if number < SHARED else grids[number + 1])
                vmem(planes, tall, LANES)
        bx, by, bz = blocks[SHARED]
        vmem(bx, rows_of(by), LANES)
        vmem(bx + 8, 24, LANES)
        vmem(by, LANES)
        vmem(counts[2], by, LANES)
        vmem(by, LANES)
        total = counts[0] * counts[1]
        vmem(total, by, LANES)
        sems(counts[2])
        sems(counts[2])
        scratch.append(pltpu.SemaphoreType.DMA)
        scratch.append(pltpu.SemaphoreType.DMA)
        scratch.append(pltpu.SemaphoreType.REGULAR((2,)))

        def kernel(*refs):
            solve_kernel(counts, blocks, coarse, refs)

        whole_block = pl.BlockSpec(memory_space=pltpu.VMEM)
        field = jax.ShapeDtypeStruct((n0 // 2 + 4, n0 + 24, LANES), jnp.float32)
        fields = pl.pallas_call(
            kernel,
            out_shape=(field,) * 4,
            in_specs=[pl.BlockSpec(memory_space=pltpu.HBM)] * 2,
            out_specs=(whole_block,) * 4,
            scratch_shapes=scratch,
            compiler_params=pltpu.CompilerParams(collective_id=0, has_side_effects=True, vmem_limit_bytes=VMEM_LIMIT * 2**20),
            name="vcycle",
        )(right_side, guess)

        def last(*refs):
            finish_kernel(counts, shape, *refs)
        block = pl.BlockSpec((16,) + shape[1:], lambda i: (i, 0, 0))
        return pl.pallas_call(
            last,
            grid=(n0 // 16,),
            out_shape=(jax.ShapeDtypeStruct(shape, jnp.float32),) * 2,
            in_specs=[whole_block] * 4,
            out_specs=(block,) * 2,
            scratch_shapes=[pltpu.VMEM((3, n0, LANES), jnp.float32), pltpu.VMEM((2 * LANES, LANES), jnp.bfloat16)],
            compiler_params=pltpu.CompilerParams(vmem_limit_bytes=8 * 2**20),
            name="finish",
        )(*fields)

    spec = P(*AXES)
    return jax.shard_map(per_device, mesh=mesh, in_specs=(spec, spec), out_specs=(spec, spec), check_vma=False)
```

```python
import itertools

import jax
import jax.numpy as jnp
from jax import lax
from jax.experimental import pallas as pl
from jax.experimental.pallas import tpu as pltpu
from jax.sharding import PartitionSpec as P

LEVELS = 7
COARSE_SWEEPS = 4
SHARED = 4
VMEM_LIMIT = 46
SWEEP_SHARE, REST_SHARE, LAST_SHARE, GRID_SHARE = 0.4, 0.4, 0.0, 0.4
LANES = 128
EDGE = 8
AXES = ("gx", "gy", "gz")
MESH = pl.DeviceIdType.MESH
WAYS = [way for way in itertools.product((-1, 0, 1), repeat=3) if any(way)]
FLAT = [way for way in WAYS if not way[2] or not (way[0] or way[1])]
FINAL = {0: 1, 1: 2, 2: 3, 3: 3}
REACH = {level: FINAL[level] + 3 for level in range(1, SHARED)}
SPARE = {SHARED - 2: 4}


def rows_of(count):
    return max(8, -(-count // 8) * 8)


def lane_iota(rows):
    return lax.broadcasted_iota(jnp.int32, (rows, LANES), 1)


def row_iota(rows):
    return lax.broadcasted_iota(jnp.int32, (rows, LANES), 0)


def loop(count, body):
    if count == 1:
        body(0)
    else:
        def step(i, carry):
            body(i)
            return carry
        lax.fori_loop(0, count, step, 0)


def turn(value, amount):
    amount = amount % LANES
    return pltpu.roll(value, amount, 1) if amount else value


def near_dot(value, matrix):
    first = value.astype(jnp.bfloat16)
    second = (value - first.astype(jnp.float32)).astype(jnp.bfloat16)
    both = jnp.concatenate([first, second], axis=1)
    return jnp.dot(both, jnp.concatenate([matrix, matrix], axis=0), preferred_element_type=jnp.float32)


def write_beside(beside):
    k = lax.broadcasted_iota(jnp.int32, (2 * LANES, LANES), 0)
    f = lax.broadcasted_iota(jnp.int32, (2 * LANES, LANES), 1)
    apart = (k - f + 2 * LANES) % LANES
    beside[...] = jnp.where((apart == 1) | (apart == LANES - 1), 1.0, 0.0).astype(jnp.bfloat16)


def lane_sums(values, beside, share):
    many = int(len(values) * share) if len(values) * values[0].shape[0] >= 60 * 8 else 0
    out = []
    if many:
        height = values[0].shape[0]
        value = jnp.concatenate(values[:many], axis=0)
        first = value.astype(jnp.bfloat16)
        second = (value - first.astype(jnp.float32)).astype(jnp.bfloat16)
        sums = jnp.dot(jnp.concatenate([first, second], axis=1), beside[...], preferred_element_type=jnp.float32)
        out = [sums[i * height:(i + 1) * height] for i in range(many)]
    return out + [pltpu.roll(value, 1, 1) + pltpu.roll(value, LANES - 1, 1) for value in values[many:]]


def widest(count, most, step=1):
    return max(size for size in range(step, count + 1, step) if count % size == 0 and (size <= most or size == step))


def signed(lane):
    return jnp.where(lane < 96, lane, lane - LANES)


def even_cells(height, start=0):
    return (row_iota(height) + lane_iota(height) + start) % 2 == 0


class Grid:
    def __init__(self, number, dims, places, counts, beside, r, b, gr, gb, w, d):
        self.number, self.dims, self.places, self.counts = number, dims, places, counts
        self.r, self.b, self.gr, self.gb, self.w, self.d, self.beside = r, b, gr, gb, w, d, beside
        self.reach = REACH.get(number, 0)
        self.ox, self.start, self.height, _, _ = layout(number, dims)
        self.sx, self.sy = (EDGE // 2, 8) if self.reach else (0, 0)
        self.pairs = dims[0] // 2
        self.spare, self.tall = spare_of(number, dims)

    def prepare(self):
        x, y, z = self.dims
        beyond = EDGE if self.reach else 0

        def base(height, start):
            row, lane = row_iota(height) + (start - 8), signed(lane_iota(height))
            at_y, at_z = self.places[1] * y + row, self.places[2] * z + lane
            last_y, last_z = self.counts[1] * y - 1, self.counts[2] * z - 1
            valid = (lane >= -beyond) & (lane < z + beyond) & (row >= -beyond) & (row < y + beyond)
            valid = valid & (at_y >= 0) & (at_y <= last_y) & (at_z >= 0) & (at_z <= last_z)
            one = lambda at, last: (at == 0).astype(jnp.float32) + (at == last).astype(jnp.float32)
            return valid, 6.0 + one(at_y, last_y) + one(at_z, last_z), even_cells(height, start)
        valid, diagonal, even = base(self.w.shape[1], self.start)
        plain, more = (jnp.where(valid, 1.0 / (diagonal + wall), 0.0) for wall in range(2))
        self.w[0] = plain
        self.w[1] = jnp.where(even, more, plain)
        self.w[2] = jnp.where(even, plain, more)
        self.w[3] = jnp.zeros_like(plain)
        valid, diagonal, even = base(self.tall, 8 - self.spare)
        self.d[0] = jnp.where(valid, diagonal, 0.0)
        self.d[1] = jnp.where(valid, jnp.where(even, diagonal + 1.0, diagonal), 0.0)
        self.d[2] = jnp.where(valid, jnp.where(even, diagonal, diagonal + 1.0), 0.0)
        for ref in (self.r, self.b) + ((self.gr, self.gb) if self.reach else ()):
            ref[...] = jnp.zeros_like(ref)

    def kind(self, pair, beyond):
        at = self.places[0] * self.pairs + pair
        last = self.counts[0] * self.pairs - 1
        if isinstance(at, int):
            return {0: 1, last: 2}.get(at, 0)
        kind = jnp.where(at == 0, 1, jnp.where(at == last, 2, 0))
        return jnp.where((at < 0) | (at > last), 3, kind) if beyond else kind

    def sweep(self, colour, zero=False, beyond=0):
        start, height = self.start, self.height
        if self.reach and not zero:
            start, height = start + 1, inner_height(self.number, self.dims)
        beyond = -(-beyond // 2)
        source, target, given = (self.r, self.b, self.gb) if colour else (self.b, self.r, self.gr)
        even = even_cells(height, start)
        ks = list(range(-beyond, self.pairs + beyond))
        if not zero:
            totals = around(source, [k + self.ox for k in ks], start, height, even, colour, self.beside, GRID_SHARE)
        for i, k in enumerate(ks):
            kind = self.kind(k, beyond > 0)
            weight = self.w[swapped(kind) if colour else kind, pl.ds(start - self.start, height), :]
            value = given[k + self.sx, pl.ds(start - 8 + self.sy, height), :]
            target[k + self.ox, pl.ds(start, height), :] = (value if zero else value + totals[i]) * weight

    def restrict_to(self, target, corner, pairs):
        rows, extra = self.tall, self.spare // 2
        if rows < 16:
            pairs[...] = jnp.zeros_like(pairs)
        ks = list(range(-extra, self.pairs + extra))
        ats = [k + self.ox for k in ks]
        first = 8 - self.spare
        even = even_cells(rows, first)
        reds = around(self.b, ats, first, rows, even, 0, self.beside, GRID_SHARE)
        blacks = around(self.r, ats, first, rows, even, 1, self.beside, GRID_SHARE)
        for i, k in enumerate(ks):
            kind = self.kind(k, False)
            at = (k + self.ox, pl.ds(first, rows), slice(None))
            own = (k + self.sx, pl.ds(self.sy - self.spare, rows), slice(None))
            red = self.gr[own] - (self.d[kind] * self.r[at] - reds[i])
            black = self.gb[own] - (self.d[swapped(kind)] * self.b[at] - blacks[i])
            pairs[i, pl.ds(0, rows), :] = red + black
        narrow(2 * len(ks), rows, self.dims[2], self.spare, target, [at - self.spare // 2 for at in corner], pairs)

    def reflect(self):
        (x, y, z), r, b, ox = self.dims, self.r, self.b, self.ox
        margin = 2 if self.reach else 0
        for_all = pl.ds(ox - margin, self.pairs + 2 * margin)

        def across(to, at):
            r[to] = -b[at]
            b[to] = -r[at]
        sides = (
            (0, 0, lambda: across(ox - 1, ox)),
            (0, 1, lambda: across(ox + self.pairs, ox + self.pairs - 1)),
            (1, 0, lambda: across((for_all, pl.ds(7, 1)), (for_all, pl.ds(8, 1)))),
            (1, 1, lambda: across((for_all, pl.ds(8 + y, 1)), (for_all, pl.ds(7 + y, 1)))),
        )
        for axis, high, step in sides:
            if isinstance(self.places[axis], int):
                step()
            else:
                pl.when(self.places[axis] == (self.counts[axis] - 1 if high else 0))(step)

    def planes(self, step, many, low, tall):
        even = even_cells(tall)
        out = []
        for i in range(many // 2):
            at = (step * (many // 2) + (low // 2 + i + self.ox), pl.ds(0, tall), slice(None))
            r, b = self.r[at], self.b[at]
            out += [jnp.where(even, r, b), jnp.where(even, b, r)]
        return out


def swapped(kind):
    if isinstance(kind, int):
        return {1: 2, 2: 1}.get(kind, kind)
    return jnp.where(kind == 1, 2, jnp.where(kind == 2, 1, kind))


class Block:
    def __init__(self, v, dims, places, counts):
        self.v, self.dims, self.places, self.counts = v, dims, places, counts

    def planes(self, step, many, low, tall):
        return [self.v[step * many + (low + 4 + i), pl.ds(0, tall), :] for i in range(many)]


def narrow(planes, rows, z, spare, target, corner, pairs):
    coarse_rows = rows_of(rows // 2)
    source_lane = signed(lax.broadcasted_iota(jnp.int32, (LANES, LANES), 0))
    target_lane = signed(lax.broadcasted_iota(jnp.int32, (LANES, LANES), 1))
    inside = (source_lane >= -spare) & (source_lane < z + spare)
    halve = jnp.where(((source_lane + LANES) // 2 - LANES // 2 == target_lane) & inside, 0.5, 0.0).astype(jnp.bfloat16)
    planes = planes // 2
    many = widest(planes, max(2, 512 // coarse_rows), 2)

    def second(step):
        at = pl.ds(step * many, many)
        q = pairs[at, pl.ds(0, coarse_rows, stride=2), :] + pairs[at, pl.ds(1, coarse_rows, stride=2), :]
        q = near_dot(q.reshape(many * coarse_rows, LANES), halve)
        q = q.reshape(many, coarse_rows, LANES)
        if not isinstance(target, tuple):
            target[pl.ds(step * many + corner[0], many), pl.ds(corner[1], coarse_rows), :] = q
            return
        even = even_cells(coarse_rows, corner[1])
        for i in range(many // 2):
            at = (step * (many // 2) + (corner[0] // 2 + i), pl.ds(corner[1], coarse_rows), slice(None))
            target[0][at] = jnp.where(even, q[2 * i], q[2 * i + 1])
            target[1][at] = jnp.where(even, q[2 * i + 1], q[2 * i])
    loop(planes // many, second)


def spare_of(number, dims):
    spare = SPARE.get(number, 0)
    return spare, -(-(dims[1] + 2 * spare) // 16) * 16 if spare else rows_of(dims[1])


def layout(number, dims):
    x, y, z = dims
    if number in REACH:
        reach = REACH[number]
        height = rows_of(y + 2 * reach)
        return EDGE // 2, 8 - reach, height, x // 2 + EDGE, max(40, y + 24)
    if number == SHARED:
        return EDGE // 2, 8, rows_of(y), x // 2 + EDGE, rows_of(y) + 24
    return 1, 8, rows_of(y), x // 2 + 2, rows_of(y) + 16


def inner_height(number, dims):
    return rows_of(dims[1] + 2 * REACH[number] - 2)


def below_zero(number):
    return -((FINAL[number] + 3) // 2) if number in FINAL else 0


def lift_shape(number, coarse):
    low = below_zero(number)
    count = coarse[0] - 2 * low
    height = rows_of(coarse[1] - 2 * low)
    first = (low - 1) // 2 * 2
    return low, count, height, first, -(-(low + count + 1 - first) // 2) * 2, rows_of(8 + low + height + 1)


def widen(below, number, spread, centre):
    dims, places, counts = below.dims, below.places, below.counts
    z = dims[2]
    _, _, _, start, planes, tall = lift_shape(number, dims)
    beyond = EDGE if number in FINAL else 0
    k = signed(lax.broadcasted_iota(jnp.int32, (LANES, LANES), 0))
    f = signed(lax.broadcasted_iota(jnp.int32, (LANES, LANES), 1))
    at = places[2] * (2 * z) + f
    inside = (f >= -beyond) & (f < 2 * z + beyond) & (at >= 0) & (at < counts[2] * 2 * z)
    parent = (f + LANES) // 2 - LANES // 2
    near = parent + jnp.where((f + LANES) % 2 == 1, 1, -1)
    outside = (places[2] * z + near < 0) | (places[2] * z + near >= counts[2] * z)
    own = jnp.where((k == parent) & inside, 0.25, 0.0)
    beside = jnp.where((k == near) & inside, 0.25, 0.0)
    both = own + jnp.where(outside, -own, beside)
    matrix = jnp.concatenate([own, both], axis=1).astype(jnp.bfloat16)
    many = widest(planes, max(2, 1024 // tall), 2)

    def first(step):
        e = jnp.concatenate(below.planes(step, many, start, tall), axis=0)
        product = near_dot(e, matrix)
        at = pl.ds(step * many, many)
        spread[at] = product[:, :LANES].reshape(many, tall, LANES)
        centre[at] = product[:, LANES:].reshape(many, tall, LANES)
    loop(planes // many, first)


def lift(below, fine, spread, centre):
    (x, y, z), places, counts = below.dims, below.places, below.counts
    number = fine.number
    low, count, height, start, _, _ = lift_shape(number, below.dims)
    beyond = number in FINAL
    widen(below, number, spread, centre)
    group = widest(count, max(1, 512 // height))
    row = places[1] * y + row_iota(height) + low
    valid = (row >= 0) & (row < counts[1] * y)
    even = lane_iota(height) % 2 == 0
    skip = low - start

    def second(step):
        for i in range(group):
            plane = step * group + i
            middle = centre[plane + skip, pl.ds(8 + low, height), :]
            ys = (spread[plane + skip, pl.ds(7 + low, height), :], spread[plane + skip, pl.ds(9 + low, height), :])
            xs = [spread[plane + skip + 2 * up_x - 1, pl.ds(8 + low, height), :] for up_x in range(2)]
            here = valid
            if beyond:
                at = places[0] * x + plane + low
                here = valid & ((at >= 0) & (at < counts[0] * x))
            for up_y in range(2):
                q = (middle + ys[up_y]) + jnp.where(even, xs[1 - up_y], xs[up_y])
                if beyond or y < height:
                    q = jnp.where(here, q, 0.0)
                at = (plane + low + fine.ox, pl.ds(8 + 2 * low + up_y, height, stride=2), slice(None))
                fine.b[at] = fine.b[at] + q
    loop(count // group, second)


def exists(places, counts, way, sign):
    found = None
    for axis in range(3):
        if way[axis]:
            other = places[axis] + sign * way[axis]
            one = (other >= 0) if sign * way[axis] < 0 else (other < counts[axis])
            found = one if found is None else found & one
    return found


def along(places, way):
    return {name: places[axis] + way[axis] for axis, name in enumerate(AXES) if way[axis]}


class Top:
    number, ox, sets = 0, 2, 4

    def __init__(self, dims, places, counts, beside, r, b, gr, gb, w, d, out, got, sems):
        self.beside = beside
        self.dims, self.places, self.counts = dims, places, counts
        self.r, self.b, self.gr, self.gb, self.w, self.d = r, b, gr, gb, w, d
        self.out, self.got, self.sems = out, got, sems
        self.pairs, self.n = dims[0] // 2, dims[1]

    @staticmethod
    def weights(dims, places, counts, height, start, beyond):
        x, y, z = dims
        row, lane = row_iota(height) + (start - 8), signed(lane_iota(height))
        at_y, at_z = places[1] * y + row, places[2] * z + lane
        last_y, last_z = counts[1] * y - 1, counts[2] * z - 1
        valid = (lane >= -beyond) & (lane < z + beyond) & (at_y >= 0) & (at_y <= last_y) & (at_z >= 0) & (at_z <= last_z)
        one = lambda at, last: (at == 0).astype(jnp.float32) + (at == last).astype(jnp.float32)
        return valid, 6.0 + one(at_y, last_y) + one(at_z, last_z), (row + lane + LANES) % 2 == 0

    def clear(self):
        for ref in (self.r, self.b, self.gr, self.gb):
            ref[...] = jnp.zeros_like(ref)

    def prepare(self):
        valid, diagonal, even = self.weights(self.dims, self.places, self.counts, self.n + 8, 6, 4)
        plain, more = (jnp.where(valid, 1.0 / (diagonal + wall), 0.0) for wall in range(2))
        self.w[0] = plain
        self.w[1] = jnp.where(even, more, plain)
        self.w[2] = jnp.where(even, plain, more)
        self.w[3] = jnp.zeros_like(plain)
        write_diagonals(self.d, self.dims, self.places, self.counts)

    def missing(self):
        for way in WAYS:
            @pl.when(jnp.logical_not(exists(self.places, self.counts, way, -1)))
            def _(way=way):
                self.got[way][...] = jnp.zeros_like(self.got[way])

    def kind(self, pair):
        at = self.places[0] * self.pairs + pair
        last = self.counts[0] * self.pairs - 1
        return jnp.where((at < 0) | (at > last), 3, jnp.where(at == 0, 1, jnp.where(at == last, 2, 0)))

    def sweep(self, colour):
        start, height = 6, self.n + 8
        source, target, given = (self.r, self.b, self.gb) if colour else (self.b, self.r, self.gr)
        count = self.pairs + 2
        chunk = widest(count, 17)
        even = (row_iota(height) + lane_iota(height)) % 2 == 0

        def body(step):
            ats = [step * chunk + i + 1 for i in range(chunk)]
            for at, total in zip(ats, around(source, ats, start, height, even, colour, self.beside, SWEEP_SHARE)):
                k = at - 2
                kind = self.kind(k)
                if colour:
                    kind = jnp.where(kind == 1, 2, jnp.where(kind == 2, 1, kind))
                target[at, pl.ds(start, height), :] = (given[at, pl.ds(start, height), :] + total) * self.w[kind]
        loop(count // chunk, body)

    def restrict_to(self, target, corner, pairs):
        n = self.n
        even = (row_iota(n) + lane_iota(n)) % 2 == 0
        chunk = 8

        def body(step):
            ks = [step * chunk + i for i in range(chunk)]
            kinds = [self.kind(k) for k in ks]
            ats = [k + 2 for k in ks]
            for k, (red, black) in zip(ks, remainders(self.r, self.b, self.gr, self.gb, self.d, ats, kinds, even, n, self.beside, REST_SHARE)):
                pairs[k] = red + black
        loop(self.pairs // chunk, body)
        narrow(self.dims[0], n, self.dims[2], 0, target, corner, pairs)

    @staticmethod
    def shapes(n):
        face = {0: (2, n, LANES), 1: (n // 4, 8, LANES), 2: (3, n, LANES)}
        sent = [face[0], face[0], face[1], face[1], face[2], face[2], (4, 8, LANES)]
        got = {}
        for way in WAYS:
            if sum(map(abs, way)) == 1:
                got[way] = face[[abs(part) for part in way].index(1)]
            elif not way[2]:
                got[way] = (2, 8, LANES)
            elif not way[0]:
                got[way] = (2, 8, LANES)
            else:
                got[way] = (8, LANES)
        return sent, got

    def copies(self, way, again):
        n, out, got = self.n, self.out, self.got[way]
        high = [part > 0 for part in way]
        if sum(map(abs, way)) == 1:
            axis = [abs(part) for part in way].index(1)
            source = out[2 * axis + high[axis]]
            if again and axis != 1:
                source, got = source.at[pl.ds(0, 1)], got.at[pl.ds(0, 1)]
        elif not way[2]:
            source = out[2 + high[1]].at[pl.ds(n // 4 - 2 if high[0] else 0, 2)]
        elif not way[0]:
            row = pl.ds(n - 8 if high[1] else 0, 8)
            source = out[4 + high[2]].at[pl.ds(0, 2), row]
        else:
            source = out[6].at[2 * high[0] + high[2]]
        k = WAYS.index(way)
        return pltpu.make_async_remote_copy(
            src_ref=source, dst_ref=got, send_sem=self.sems[0].at[k], recv_sem=self.sems[1].at[k],
            device_id=along(self.places, way), device_id_type=MESH)

    def pack_ends(self, part, again):
        tile = lane_iota(8)
        many = self.pairs // self.sets
        ahead = (tile + (LANES - 60)) % LANES
        wide = 4 * many
        for t in range(self.n // 8):
            at = pl.ds(8 * t, 8)
            for index, ref in enumerate([self.b] if again else [self.b, self.gr, self.gb]):
                first = last = None
                for k in range(part * many, part * many + many):
                    moved = turn(ref[k + 2, pl.ds(8 * t + 8, 8), :], 4 * k)
                    first = moved if first is None else jnp.where(tile // 4 == k, moved, first)
                    last = moved if last is None else jnp.where(ahead // 4 == k, moved, last)
                if part:
                    first = jnp.where(tile // wide == part, first, self.out[4][index, at])
                    last = jnp.where(ahead // wide == part, last, self.out[5][index, at])
                self.out[4][index, at] = first
                self.out[5][index, at] = last

    def pack(self, again):
        n, pairs = self.n, self.pairs
        low, tile = lane_iota(n) < 64, lane_iota(8)
        row = row_iota(8)
        half = pairs // 2
        own = lambda ref, k: ref[k + 2, pl.ds(8, n), :]
        for high in range(2):
            near, far = (pairs - 1, pairs - 2) if high else (0, 1)
            self.out[high][0] = jnp.where(low, own(self.b, near), pltpu.roll(own(self.b, far), 64, 1))
            if not again:
                self.out[high][1] = jnp.where(low, own(self.gr, near), pltpu.roll(own(self.gb, near), 64, 1))

            def edge(k, high=high):
                first = 8 + n - 8 if high else 8
                b = self.b[k + 2, pl.ds(first, 8), :]
                if again:
                    return b
                red, black = (pltpu.roll(ref[k + 2, pl.ds(first, 8), :], by, 0) for ref, by in ((self.gr, 4), (self.gb, 2 if high else 6)))
                if high:
                    return jnp.where(row >= 4, b, jnp.where(row >= 2, red, black))
                return jnp.where(row < 4, b, jnp.where(row < 6, red, black))
            for k in range(half):
                self.out[2 + high][k] = jnp.where(tile < 64, edge(k), pltpu.roll(edge(k + half), 64, 1))
        for high_x in range(2):
            for high_z in range(2):
                offset = 60 if high_z else 0
                pair, near = (pairs - 2, pairs - 1) if high_x else (0, 0)
                value = jnp.zeros((8, LANES), jnp.float32)
                for t in range(n // 8):
                    rows = pl.ds(8 * t, 8)
                    moved = turn(self.out[4 + high_z][0, rows], 16 * t - 4 * pair - offset)
                    value = jnp.where((tile >= 16 * t) & (tile < 16 * t + 8), moved, value)
                    if not again:
                        moved = turn(self.out[4 + high_z][1, rows], 16 * t + 8 - 4 * near - offset)
                        value = jnp.where((tile >= 16 * t + 8) & (tile < 16 * t + 16), moved, value)
                self.out[6][2 * high_x + high_z] = value

    def post(self, again=False):
        for part in range(self.sets):
            self.pack_ends(part, again)
        self.pack(again)
        self.send(again)

    def send(self, again=False):
        for way in WAYS:
            pl.when(exists(self.places, self.counts, way, 1))(self.copies(way, again).start)

    def sent(self, again=False):
        for way in WAYS:
            pl.when(exists(self.places, self.counts, way, 1))(self.copies(way, again).wait_send)

    def wait(self, ways, again):
        for way in ways:
            pl.when(exists(self.places, self.counts, way, -1))(self.copies(way, again).wait_recv)

    def land(self, again=False):
        n, pairs, got = self.n, self.pairs, self.got
        half = pairs // 2
        arrays = [self.b] if again else [self.b, self.gr, self.gb]
        lane, tile = lane_iota(n), lane_iota(8)

        def ends(high, low, to, k):
            pick = to % 8 < 4
            return turn(jnp.where(pick, high, low) if k % 2 == 0 else jnp.where(pick, low, high), 64 - 4 * k)
        self.wait([way for way in WAYS if not (way[0] or way[1])], again)
        high, low = got[(0, 0, -1)], got[(0, 0, 1)]

        def body(t):
            at = pl.ds(t * 8, 8)
            packs = [(high[index, at], low[index, at]) for index in range(len(arrays))]
            for k in range(pairs):
                own = (k + 2, pl.ds(t * 8 + 8, 8), slice(None))
                for (h, l), ref in zip(packs, arrays):
                    ref[own] = jnp.where(tile < 64, ref[own], ends(h, l, tile, k))
        for t in range(n // 8):
            body(t)
        self.wait([way for way in WAYS if way[1] and not way[0]], again)
        for side in (-1, 1):
            face = got[(0, -side, 0)]
            base = 8 + n if side > 0 else 0
            shifts = (0, 4, 2 if side > 0 else 6)
            for index, ref in enumerate(arrays):
                if index < 2:
                    h, l = got[(0, -side, -1)][index], got[(0, -side, 1)][index]
                for k in range(pairs):
                    value = face[k % half]
                    if k >= half:
                        value = pltpu.roll(value, 64, 1)
                    if shifts[index]:
                        value = pltpu.roll(value, shifts[index], 0)
                    if index < 2:
                        value = jnp.where(tile < 64, value, ends(h, l, tile, k))
                    ref[k + 2, pl.ds(base, 8), :] = value
        self.wait([way for way in WAYS if way[0]], again)
        for side in (-1, 1):
            face = got[(-side, 0, 0)]
            near, far = (pairs + 2, pairs + 3) if side > 0 else (1, 0)
            high, low = got[(-side, 0, -1)], got[(-side, 0, 1)]
            near_lane, far_lane = (0, 4) if side > 0 else (4, 0)

            def beside(first, at, high=high, low=low):
                out = []
                for t in at:
                    up = turn(high[...], 64 - 16 * t - first)
                    out.append(jnp.where(tile < 96, up, turn(low[...], 124 - 16 * t - first)))
                return jnp.concatenate(out, axis=0) if len(out) > 1 else out[0]
            every = range(n // 8)
            both = face[0]
            self.b[near, pl.ds(8, n), :] = jnp.where(lane < 64, both, beside(near_lane, every))
            self.b[far, pl.ds(8, n), :] = jnp.where(lane < 64, pltpu.roll(both, 64, 1), beside(far_lane, every))
            if not again:
                both = face[1]
                self.gr[near, pl.ds(8, n), :] = jnp.where(lane < 64, both, beside(8, every))
                self.gb[near, pl.ds(8, n), :] = pltpu.roll(both, 64, 1)
            for up in (-1, 1):
                edge = got[(-side, -up, 0)]
                base = 8 + n if up > 0 else 0
                corner = (got[(-side, -up, -1)], got[(-side, -up, 1)])
                t = [0 if up > 0 else n // 8 - 1]
                if side > 0:
                    pieces = {near: (0, False), far: (1, False)}
                else:
                    pieces = {near: (1, True), far: (0, True)}
                for place, (group, upper) in pieces.items():
                    value = edge[group]
                    if upper:
                        value = pltpu.roll(value, 64, 1)
                    first = near_lane if place == near else far_lane
                    self.b[place, pl.ds(base, 8), :] = jnp.where(tile < 64, value, beside(first, t, *corner))
                    if place == near and not again:
                        self.gr[place, pl.ds(base, 8), :] = pltpu.roll(value, 4, 0)


def around(source, ats, start, height, even, colour, beside, share):
    rows = pl.ds(start, height)
    centres = [source[at, rows, :] for at in ats]
    out = []
    for at, s, z_sum in zip(ats, centres, lane_sums(centres, beside, share)):
        left, right = source[at - 1, rows, :], source[at + 1, rows, :]
        across = jnp.where(even, right, left) if colour else jnp.where(even, left, right)
        total = (s + across) + (source[at, pl.ds(start + 1, height), :] + source[at, pl.ds(start - 1, height), :])
        out.append(total + z_sum)
    return out


def remainders(r, b, gr, gb, d, ats, kinds, even, n, beside, share):
    rows = pl.ds(8, n)
    out = []
    for at, kind, reds, blacks in zip(ats, kinds, around(b, ats, 8, n, even, 0, beside, share), around(r, ats, 8, n, even, 1, beside, share)):
        other = swapped(kind)
        out.append((gr[at, rows, :] - (d[kind] * r[at, rows, :] - reds), gb[at, rows, :] - (d[other] * b[at, rows, :] - blacks)))
    return out


def write_diagonals(d, dims, places, counts):
    _, diagonal, even = Top.weights(dims, places, counts, dims[1], 8, 0)
    d[0] = diagonal
    d[1] = jnp.where(even, diagonal + 1.0, diagonal)
    d[2] = jnp.where(even, diagonal, diagonal + 1.0)


class Ring:
    def __init__(self, level, refs, sems):
        self.level, self.sems = level, sems
        self.body, self.parts = refs[0], refs[1:-len(WAYS)]
        self.got = dict(zip(WAYS, refs[-len(WAYS):]))
        self.places, self.counts = level.places, level.counts

    @staticmethod
    def sizes(n):
        each = LANES // n
        cut = n if n <= 16 else 8
        return each, max(1, n // each), cut, LANES // cut, max(1, n * cut // LANES)

    @staticmethod
    def thick(n, reach, way):
        each, groups, _, _, cuts = Ring.sizes(n)
        if not way[0]:
            return cuts if way[2] else groups
        return 1 if way[2] else -(-reach // each)

    @staticmethod
    def shape(n, reach, way):
        return (Ring.thick(n, reach, way), 8 if way[1] else n, LANES)

    def clear(self):
        for way in WAYS:
            @pl.when(jnp.logical_not(exists(self.places, self.counts, way, -1)))
            def _(way=way):
                self.got[way][...] = jnp.zeros_like(self.got[way])

    def copy(self, way):
        n = self.level.dims[0]
        shape = Ring.shape(n, self.level.reach, way)
        source = self.body
        if way[2] and self.parts:
            source = self.parts[0] if way[2] < 0 else self.parts[1]
        groups = source.shape[0]
        group = 0 if way[0] <= 0 else groups - shape[0]
        row = 0 if way[1] <= 0 else n - 8
        k = WAYS.index(way)
        return pltpu.make_async_remote_copy(
            src_ref=source.at[pl.ds(group, shape[0]), pl.ds(row, shape[1])], dst_ref=self.got[way],
            send_sem=self.sems[0].at[k], recv_sem=self.sems[1].at[k],
            device_id={name: self.places[axis] + way[axis] for axis, name in enumerate(AXES) if way[axis]}, device_id_type=MESH)

    def post(self):
        n, gr, gb = self.level.dims[0], self.level.gr, self.level.gb
        each, groups, cut, cuts_each, cuts = Ring.sizes(n)
        even = even_cells(n)

        def plane(x):
            at = (x // 2 + EDGE // 2, pl.ds(8, n), slice(None))
            value = jnp.where(even, gb[at], gr[at]) if x % 2 else jnp.where(even, gr[at], gb[at])
            return jnp.where(lane_iota(n) < n, value, 0.0) if SPARE.get(self.level.number - 1) else value
        for g in range(groups):
            value = plane(g * each)
            for i in range(1, min(each, n)):
                value = value + turn(plane(g * each + i), i * n)
            self.body[g] = value
        if self.parts:
            lane = lane_iota(n)
            for g in range(cuts):
                low = high = jnp.zeros((n, LANES), jnp.float32)
                for i in range(cuts_each):
                    moved = turn(plane(g * cuts_each + i), cut * i)
                    low = jnp.where(lane // cut == i, moved, low)
                    high = jnp.where((lane + (LANES - n + cut)) % LANES // cut == i, moved, high)
                self.parts[0][g] = low
                self.parts[1][g] = high
        for way in sorted(WAYS, key=all):
            pl.when(exists(self.places, self.counts, way, 1))(self.copy(way).start)

    def land(self, near=False, rest=False):
        n, gr, gb, reach = self.level.dims[0], self.level.gr, self.level.gb, self.level.reach
        reach = 2 if near else reach + reach % 2
        each, groups, cut, cuts_each, cuts = Ring.sizes(n)
        for to_x, to_y in sorted(itertools.product((-1, 0, 1), repeat=2), key=lambda at: abs(at[0]) * 3 + abs(at[1])):
            for way in WAYS:
                if way[:2] == (-to_x, -to_y) and not (near and all(way)) and (all(way) or not rest):
                    pl.when(exists(self.places, self.counts, way, -1))(self.copy(way).wait_recv)
            height = 8 if to_y else n
            row = {-1: 0, 0: 8, 1: 8 + n}[to_y]
            lane = lane_iota(height)
            body = self.got[(-to_x, -to_y, 0)] if to_x or to_y else None
            high = self.got[(-to_x, -to_y, -1)]
            low = self.got[(-to_x, -to_y, 1)]

            made = {}

            def merged(h, flip, made=made, high=high, low=low, lane=lane):
                if (h, flip) not in made:
                    both = (high[h], turn(low[h], -2 * n))
                    made[h, flip] = jnp.where(lane % 16 < 8, both[flip], both[1 - flip])
                return made[h, flip]
            even = even_cells(height, row)

            def value(x, body=body, high=high, low=low, lane=lane, merged=merged, to_x=to_x):
                g, h = x // each, x // cuts_each
                if to_x < 0:
                    g, h = g - (groups - body.shape[0]), h - (cuts - high.shape[0])
                if near and to_x and to_y:
                    return jnp.where(lane < n, turn(body[g], -(x % each) * n), 0.0)
                if n == 8:
                    ends = jnp.where(lane < 64, turn(high[h], n - cut * (x % cuts_each)), turn(low[h], -n - cut * (x % cuts_each)))
                else:
                    ends = turn(merged(h, x % 2 if n == 32 else 0), n - cut * (x % cuts_each))
                return ends if body is None else jnp.where(lane < n, turn(body[g], -(x % each) * n), ends)
            for x in {-1: range(n - reach, n, 2), 0: range(0, n, 2), 1: range(0, reach, 2)}[to_x]:
                at = (EDGE // 2 + (to_x * n + x) // 2, pl.ds(row, height), slice(None))
                first, second = value(x), value(x + 1)
                red, black = jnp.where(even, first, second), jnp.where(even, second, first)
                if body is None:
                    red, black = jnp.where(lane < n, gr[at], red), jnp.where(lane < n, gb[at], black)
                gr[at] = red
                gb[at] = black

    def finish(self):
        for way in WAYS:
            pl.when(exists(self.places, self.counts, way, 1))(self.copy(way).wait_send)


def solve_kernel(counts, blocks, coarse, refs):
    right_side, guess, r, b, gr, gb = refs[:6]
    refs = list(refs[6:])
    take = lambda count=1: [refs.pop(0) for _ in range(count)] if count > 1 else refs.pop(0)
    places = tuple(lax.axis_index(axis) for axis in AXES)
    n0 = blocks[0][0]
    raw_g, raw_v, raw_sems = take(3)
    sent_shapes, got_shapes = Top.shapes(n0)
    w0, d0, beside = take(3)
    top = Top(blocks[0], places, counts, beside, r, b, gr, gb, w0, d0, take(len(sent_shapes)), dict(zip(WAYS, take(len(WAYS)))), take(2))
    levels = [top]
    for number in range(1, LEVELS):
        if number < SHARED:
            levels.append(Grid(number, blocks[number], places, counts, beside, *take(6)))
        else:
            levels.append(Grid(number, coarse[number - SHARED], (0, 0, 0), (1, 1, 1), beside, *take(6)))
    rings = {}
    for number in REACH:
        n = blocks[number][0]
        members = take(1 + (2 if Ring.sizes(n)[2] != n else 0) + len(WAYS))
        rings[number] = Ring(levels[number], members, take(2))
    pairs = take(LEVELS - 1)
    spreads = take(LEVELS - 1)
    centres = take(LEVELS - 1)
    block_s, block_v, packet, line, joined, packets, line_send, line_recv, gather_send, gather_recv, spread_sem = refs

    cut = n0 // top.sets
    loads = [[pltpu.make_async_copy(source.at[pl.ds(part * cut, cut)], target.at[pl.ds(part * cut, cut)], raw_sems.at[i, part])
              for i, (source, target) in enumerate(((right_side, raw_g), (guess, raw_v)))] for part in range(top.sets)]
    for load in sum(loads, []):
        load.start()
    barrier = pltpu.get_barrier_semaphore()
    nx, ny, nz = counts

    def greet(device):
        pl.semaphore_signal(barrier, inc=1, device_id=device, device_id_type=MESH)

    def around_torus(way, far):
        return {name: lax.rem(places[axis] + way[axis] * far + counts[axis], counts[axis]) for axis, name in enumerate(AXES) if way[axis]}

    for way in WAYS:
        greet(around_torus(way, 1))

    def tell(turn):
        for way in FLAT:
            pl.semaphore_signal(spread_sem.at[turn], inc=1, device_id=around_torus(way, turn + 1), device_id_type=MESH)

    def hear(turn):
        pl.semaphore_wait(spread_sem.at[turn], len(FLAT))

    top.clear()
    top.prepare()
    write_beside(beside)
    top.missing()
    even = (lax.broadcasted_iota(jnp.int32, (n0, n0), 0) + lax.broadcasted_iota(jnp.int32, (n0, n0), 1)) % 2 == 0
    for part in range(top.sets):
        for load in loads[part]:
            load.wait()
        for k in range(part * cut // 2, (part + 1) * cut // 2):
            at = (k + 2, pl.ds(8, n0), pl.ds(0, n0))
            first, second = raw_g[2 * k], raw_g[2 * k + 1]
            gr[at] = jnp.where(even, first, second)
            gb[at] = jnp.where(even, second, first)
            b[at] = jnp.where(even, raw_v[2 * k + 1], raw_v[2 * k])
        top.pack_ends(part, False)
    top.pack(False)
    pl.semaphore_wait(barrier, len(WAYS))
    top.send()
    tell(0)
    for level in levels[1:]:
        level.prepare()
    for ring in rings.values():
        ring.clear()
    block_v[...] = jnp.zeros_like(block_v)
    top.land()
    hear(0)
    tell(1)
    top.sweep(0)
    top.sweep(1)
    top.restrict_to((levels[1].gr, levels[1].gb), (EDGE, 8), pairs[0])
    for number in range(1, SHARED - 1):
        level = levels[number]
        rings[number].post()
        if number == 1:
            rings[1].land(near=True)
            level.sweep(0, zero=True, beyond=2)
            level.sweep(1, beyond=1)
        else:
            rings[1].land(rest=True)
            levels[1].sweep(0, zero=True, beyond=levels[1].reach)
            levels[1].sweep(1, beyond=levels[1].reach - 1)
            rings[number].land()
            level.sweep(0, zero=True, beyond=level.reach)
            level.sweep(1, beyond=level.reach - 1)
        level.restrict_to((levels[number + 1].gr, levels[number + 1].gb), (EDGE, 8), pairs[number])
    last = levels[SHARED - 1]
    last.sweep(0, zero=True, beyond=2)
    last.sweep(1, beyond=1)
    last.restrict_to(block_s, (0, 0), pairs[SHARED - 1])
    hear(1)

    bx, by, bz = blocks[SHARED]
    wide = LANES // bx
    packed = jnp.zeros((rows_of(by), LANES), jnp.float32)
    for x in range(bx):
        packed = packed + pltpu.roll(block_s[x], x * wide + places[2] * bz, 1)
    packet[...] = packed[:by]

    def line_copy(source, target):
        return pltpu.make_async_remote_copy(
            src_ref=packet, dst_ref=line.at[source], send_sem=line_send.at[target], recv_sem=line_recv.at[source],
            device_id={AXES[2]: target}, device_id_type=MESH)

    for offset in range(1, nz):
        line_copy(places[2], lax.rem(places[2] + offset, nz)).start()
    rings[1].finish()
    rings[SHARED - 1].post()
    top.sent()
    top.post(True)
    merged = packed[:by]
    for offset in range(1, nz):
        source = lax.rem(places[2] + nz - offset, nz)
        line_copy(source, lax.rem(places[2] + offset, nz)).wait_recv()
        merged = merged + line[source]
    joined[...] = merged
    total = nx * ny
    me = places[0] * ny + places[1]

    def plane_copy(to_x, to_y):
        return pltpu.make_async_remote_copy(
            src_ref=joined, dst_ref=packets.at[me], send_sem=gather_send, recv_sem=gather_recv,
            device_id={AXES[0]: to_x, AXES[1]: to_y}, device_id_type=MESH)

    xs = [lax.rem(places[0] + step, nx) for step in range(nx)]
    ys = [lax.rem(places[1] + step, ny) for step in range(ny)]
    far = lambda at: min(at[0], nx - at[0]) + min(at[1], ny - at[1])
    for to_x, to_y in sorted(itertools.product(range(nx), range(ny)), key=far, reverse=True)[:-1]:
        plane_copy(xs[to_x], ys[to_y]).start()
    packets[me] = merged
    rings[SHARED - 1].land()
    last.sweep(0, zero=True, beyond=last.reach)
    last.sweep(1, beyond=last.reach - 1)
    top.land(True)
    top.sent(True)
    for number in (SHARED - 2, SHARED - 1):
        rings[number].finish()
    for offset in range(1, nz):
        line_copy(places[2], lax.rem(places[2] + offset, nz)).wait_send()
    everyone = pltpu.make_async_remote_copy(
        src_ref=packets.at[pl.ds(0, total - 1)], dst_ref=packets.at[pl.ds(0, total - 1)], send_sem=gather_send, recv_sem=gather_recv,
        device_id={AXES[0]: places[0]}, device_id_type=MESH)
    everyone.wait_recv()
    whole = levels[SHARED]

    def unpack(px):
        for py in range(0, ny, 2):
            pair = jnp.concatenate([packets[px * ny + py], packets[px * ny + py + 1]], axis=0)
            cells = even_cells(2 * by)
            for x in range(0, bx, 2):
                first, second = turn(pair, -x * wide), turn(pair, -(x + 1) * wide)
                at = (px * (bx // 2) + x // 2, pl.ds(py * by, 2 * by), slice(None))
                whole.gr[at] = jnp.where(cells, first, second)
                whole.gb[at] = jnp.where(cells, second, first)
    loop(nx, unpack)

    for number in range(SHARED, LEVELS - 1):
        level = levels[number]
        level.sweep(0, zero=True)
        level.sweep(1)
        level.restrict_to((levels[number + 1].gr, levels[number + 1].gb), (0, 0), pairs[number])
    level = levels[LEVELS - 1]
    level.sweep(0, zero=True)
    level.sweep(1)
    for _ in range(COARSE_SWEEPS - 1):
        level.sweep(0)
        level.sweep(1)
    for number in reversed(range(SHARED, LEVELS - 1)):
        level, below = levels[number], levels[number + 1]
        below.reflect()
        lift(below, level, spreads[number], centres[number])
        level.sweep(0)
        level.sweep(1)

    whole.reflect()
    shift = lax.rem(LANES - places[2] * bz, LANES)
    odd = lax.rem(places[1] + 1, 2) == 1
    cells = even_cells(24)
    for x in range(0, bx + 8, 2):
        at = (places[0] * (bx // 2) + (x // 2 - 2 + whole.ox), pl.ds(pl.multiple_of((places[1] + 1) // 2 * 8, 8), 24), slice(None))
        r_part, b_part = whole.r[at], whole.b[at]
        for i, part in enumerate((jnp.where(cells, r_part, b_part), jnp.where(cells, b_part, r_part))):
            block_v[x + i, pl.ds(4, 16)] = pltpu.roll(jnp.where(odd, part[4:20], part[:16]), shift, 1)
    around_block = Block(block_v, blocks[SHARED], places, counts)
    lift(around_block, levels[SHARED - 1], spreads[SHARED - 1], centres[SHARED - 1])
    for number in reversed(range(1, SHARED)):
        level = levels[number]
        level.sweep(0, beyond=level.reach - 2)
        level.sweep(1, beyond=level.reach - 3)
        level.reflect()
        lift(level, levels[number - 1], spreads[number - 1], centres[number - 1])
    top.sweep(0)
    top.sweep(1)

    everyone.wait_send()


def finish_kernel(counts, dims, r, b, gr, gb, solution, residual, out_v, out_r, d, beside, sems):
    places = tuple(lax.axis_index(axis) for axis in AXES)
    n, half = dims[1], dims[0] // 2
    write_diagonals(d, dims, places, counts)
    write_beside(beside)
    even = even_cells(n)
    last = counts[0] * half - 1
    group = 8

    def copies(step):
        part = pl.ds(step * 2 * group, 2 * group)
        return [pltpu.make_async_copy(source.at[part], target.at[part], sems.at[i, step])
                for i, (source, target) in enumerate(((out_v, solution), (out_r, residual)))]

    def compute(step):
        ks = [step * group + i for i in range(group)]
        globally = [places[0] * half + k for k in ks]
        kinds = [jnp.where(at == 0, 1, jnp.where(at == last, 2, 0)) for at in globally]
        results = remainders(r, b, gr, gb, d, [k + 2 for k in ks], kinds, even, n, beside, LAST_SHARE)
        for k, (red, black) in zip(ks, results):
            own = (k + 2, pl.ds(8, n), slice(None))
            for out, x, y in ((out_v, r[own], b[own]), (out_r, red, black)):
                out[2 * k] = jnp.where(even, x, y)[:, :n]
                out[2 * k + 1] = jnp.where(even, y, x)[:, :n]
        for copy in copies(step):
            copy.start()
    loop(half // group, compute)
    for step in range(half // group):
        for copy in copies(step):
            copy.wait()


def solution(mesh):
    counts = tuple(mesh.shape[axis] for axis in AXES)

    def per_device(right_side, guess):
        shape = right_side.shape
        blocks = [tuple(side >> level for side in shape) for level in range(SHARED + 1)]
        whole = tuple(side * count for side, count in zip(blocks[SHARED], counts))
        coarse = [tuple(side >> level for side in whole) for level in range(LEVELS - SHARED)]
        grids = blocks[:SHARED] + coarse
        n0 = blocks[0][0]
        scratch = []
        vmem = lambda *dims: scratch.append(pltpu.VMEM(dims, jnp.float32))
        sems = lambda *dims: scratch.append(pltpu.SemaphoreType.DMA(dims))
        vmem(*shape)
        vmem(*shape)
        sems(2, Top.sets)
        vmem(4, n0 + 8, LANES)
        vmem(3, n0, LANES)
        scratch.append(pltpu.VMEM((2 * LANES, LANES), jnp.bfloat16))
        sent, got = Top.shapes(n0)
        for dims in sent:
            vmem(*dims)
        for way in WAYS:
            vmem(*got[way])
        sems(len(WAYS))
        sems(len(WAYS))
        for number, (x, y, z) in enumerate(grids):
            if number == 0:
                continue
            _, _, height, extent, tall = layout(number, (x, y, z))
            vmem(extent, tall, LANES)
            vmem(extent, tall, LANES)
            for _ in range(2):
                vmem(*((extent, tall) if number in REACH else (x // 2, rows_of(y))), LANES)
            vmem(4, max(height, rows_of(inner_height(number, (x, y, z)) + 1)) if number in REACH else height, LANES)
            vmem(3, spare_of(number, (x, y, z))[1], LANES)
        for number in REACH:
            n = blocks[number][0]
            _, groups, cut, _, cuts = Ring.sizes(n)
            vmem(groups, n, LANES)
            if cut != n:
                vmem(cuts, n, LANES)
                vmem(cuts, n, LANES)
            for way in WAYS:
                vmem(*Ring.shape(n, REACH[number], way))
            sems(len(WAYS))
            sems(len(WAYS))
        for number, (x, y, z) in enumerate(grids[:-1]):
            spare, tall = spare_of(number, (x, y, z))
            vmem(x // 2 + spare, max(16, tall), LANES)
        for _ in range(2):
            for number in range(LEVELS - 1):
                _, _, _, _, planes, tall = lift_shape(number, blocks[number + 1] if number < SHARED else grids[number + 1])
                vmem(planes, tall, LANES)
        bx, by, bz = blocks[SHARED]
        vmem(bx, rows_of(by), LANES)
        vmem(bx + 8, 24, LANES)
        vmem(by, LANES)
        vmem(counts[2], by, LANES)
        vmem(by, LANES)
        total = counts[0] * counts[1]
        vmem(total, by, LANES)
        sems(counts[2])
        sems(counts[2])
        scratch.append(pltpu.SemaphoreType.DMA)
        scratch.append(pltpu.SemaphoreType.DMA)
        scratch.append(pltpu.SemaphoreType.REGULAR((2,)))

        def kernel(*refs):
            solve_kernel(counts, blocks, coarse, refs)

        whole_block = pl.BlockSpec(memory_space=pltpu.VMEM)
        field = jax.ShapeDtypeStruct((n0 // 2 + 4, n0 + 24, LANES), jnp.float32)
        fields = pl.pallas_call(
            kernel,
            out_shape=(field,) * 4,
            in_specs=[pl.BlockSpec(memory_space=pltpu.HBM)] * 2,
            out_specs=(whole_block,) * 4,
            scratch_shapes=scratch,
            compiler_params=pltpu.CompilerParams(collective_id=0, has_side_effects=True, vmem_limit_bytes=VMEM_LIMIT * 2**20),
            name="vcycle",
        )(right_side, guess)

        def last(*refs):
            finish_kernel(counts, shape, *refs)
        in_hbm = pl.BlockSpec(memory_space=pltpu.HBM)
        return pl.pallas_call(
            last,
            out_shape=(jax.ShapeDtypeStruct(shape, jnp.float32),) * 2,
            in_specs=[whole_block] * 4,
            out_specs=(in_hbm,) * 2,
            scratch_shapes=[
                pltpu.VMEM(shape, jnp.float32), pltpu.VMEM(shape, jnp.float32), pltpu.VMEM((3, n0, LANES), jnp.float32),
                pltpu.VMEM((2 * LANES, LANES), jnp.bfloat16), pltpu.SemaphoreType.DMA((2, n0 // 16))],
            compiler_params=pltpu.CompilerParams(vmem_limit_bytes=8 * 2**20),
            name="finish",
        )(*fields)

    spec = P(*AXES)
    return jax.shard_map(per_device, mesh=mesh, in_specs=(spec, spec), out_specs=(spec, spec), check_vma=False)
```

```python
import itertools

import jax
import jax.numpy as jnp
from jax import lax
from jax.experimental import pallas as pl
from jax.experimental.pallas import tpu as pltpu
from jax.sharding import PartitionSpec as P

LEVELS = 7
COARSE_SWEEPS = 4
SHARED = 4
VMEM_LIMIT = 46
SWEEP_SHARE, REST_SHARE, LAST_SHARE, GRID_SHARE = 0.4, 0.4, 0.3, 0.4
LANES = 128
EDGE = 8
AXES = ("gx", "gy", "gz")
MESH = pl.DeviceIdType.MESH
WAYS = [way for way in itertools.product((-1, 0, 1), repeat=3) if any(way)]
FLAT = [way for way in WAYS if not way[2] or not (way[0] or way[1])]
FINAL = {0: 1, 1: 2, 2: 3, 3: 3}
REACH = {level: FINAL[level] + 3 for level in range(1, SHARED)}
SPARE = {SHARED - 2: 4}


def rows_of(count):
    return max(8, -(-count // 8) * 8)


def lane_iota(rows):
    return lax.broadcasted_iota(jnp.int32, (rows, LANES), 1)


def row_iota(rows):
    return lax.broadcasted_iota(jnp.int32, (rows, LANES), 0)


def loop(count, body):
    if count == 1:
        body(0)
    else:
        def step(i, carry):
            body(i)
            return carry
        lax.fori_loop(0, count, step, 0)


def turn(value, amount):
    amount = amount % LANES
    return pltpu.roll(value, amount, 1) if amount else value


def near_dot(value, matrix):
    first = value.astype(jnp.bfloat16)
    second = (value - first.astype(jnp.float32)).astype(jnp.bfloat16)
    both = jnp.concatenate([first, second], axis=1)
    return jnp.dot(both, jnp.concatenate([matrix, matrix], axis=0), preferred_element_type=jnp.float32)


def write_beside(beside):
    k = lax.broadcasted_iota(jnp.int32, (2 * LANES, LANES), 0)
    f = lax.broadcasted_iota(jnp.int32, (2 * LANES, LANES), 1)
    apart = (k - f + 2 * LANES) % LANES
    beside[...] = jnp.where((apart == 1) | (apart == LANES - 1), 1.0, 0.0).astype(jnp.bfloat16)


def lane_sums(values, beside, share):
    many = int(len(values) * share) if len(values) * values[0].shape[0] >= 60 * 8 else 0
    out = []
    if many:
        height = values[0].shape[0]
        value = jnp.concatenate(values[:many], axis=0)
        first = value.astype(jnp.bfloat16)
        second = (value - first.astype(jnp.float32)).astype(jnp.bfloat16)
        sums = jnp.dot(jnp.concatenate([first, second], axis=1), beside[...], preferred_element_type=jnp.float32)
        out = [sums[i * height:(i + 1) * height] for i in range(many)]
    return out + [pltpu.roll(value, 1, 1) + pltpu.roll(value, LANES - 1, 1) for value in values[many:]]


def widest(count, most, step=1):
    return max(size for size in range(step, count + 1, step) if count % size == 0 and (size <= most or size == step))


def signed(lane):
    return jnp.where(lane < 96, lane, lane - LANES)


def even_cells(height, start=0):
    return (row_iota(height) + lane_iota(height) + start) % 2 == 0


class Grid:
    def __init__(self, number, dims, places, counts, beside, r, b, gr, gb, w, d):
        self.number, self.dims, self.places, self.counts = number, dims, places, counts
        self.r, self.b, self.gr, self.gb, self.w, self.d, self.beside = r, b, gr, gb, w, d, beside
        self.reach = REACH.get(number, 0)
        self.ox, self.start, self.height, _, _ = layout(number, dims)
        self.sx, self.sy = (EDGE // 2, 8) if self.reach else (0, 0)
        self.pairs = dims[0] // 2
        self.spare, self.tall = spare_of(number, dims)

    def prepare(self):
        x, y, z = self.dims
        beyond = EDGE if self.reach else 0

        def base(height, start):
            row, lane = row_iota(height) + (start - 8), signed(lane_iota(height))
            at_y, at_z = self.places[1] * y + row, self.places[2] * z + lane
            last_y, last_z = self.counts[1] * y - 1, self.counts[2] * z - 1
            valid = (lane >= -beyond) & (lane < z + beyond) & (row >= -beyond) & (row < y + beyond)
            valid = valid & (at_y >= 0) & (at_y <= last_y) & (at_z >= 0) & (at_z <= last_z)
            one = lambda at, last: (at == 0).astype(jnp.float32) + (at == last).astype(jnp.float32)
            return valid, 6.0 + one(at_y, last_y) + one(at_z, last_z), even_cells(height, start)
        valid, diagonal, even = base(self.w.shape[1], self.start)
        plain, more = (jnp.where(valid, 1.0 / (diagonal + wall), 0.0) for wall in range(2))
        self.w[0] = plain
        self.w[1] = jnp.where(even, more, plain)
        self.w[2] = jnp.where(even, plain, more)
        self.w[3] = jnp.zeros_like(plain)
        valid, diagonal, even = base(self.tall, 8 - self.spare)
        self.d[0] = jnp.where(valid, diagonal, 0.0)
        self.d[1] = jnp.where(valid, jnp.where(even, diagonal + 1.0, diagonal), 0.0)
        self.d[2] = jnp.where(valid, jnp.where(even, diagonal, diagonal + 1.0), 0.0)
        for ref in (self.r, self.b) + ((self.gr, self.gb) if self.reach else ()):
            ref[...] = jnp.zeros_like(ref)

    def kind(self, pair, beyond):
        at = self.places[0] * self.pairs + pair
        last = self.counts[0] * self.pairs - 1
        if isinstance(at, int):
            return {0: 1, last: 2}.get(at, 0)
        kind = jnp.where(at == 0, 1, jnp.where(at == last, 2, 0))
        return jnp.where((at < 0) | (at > last), 3, kind) if beyond else kind

    def sweep(self, colour, zero=False, beyond=0):
        start, height = self.start, self.height
        if self.reach and not zero:
            start, height = start + 1, inner_height(self.number, self.dims)
        beyond = -(-beyond // 2)
        source, target, given = (self.r, self.b, self.gb) if colour else (self.b, self.r, self.gr)
        even = even_cells(height, start)
        ks = list(range(-beyond, self.pairs + beyond))
        if not zero:
            totals = around(source, [k + self.ox for k in ks], start, height, even, colour, self.beside, GRID_SHARE)
        for i, k in enumerate(ks):
            kind = self.kind(k, beyond > 0)
            weight = self.w[swapped(kind) if colour else kind, pl.ds(start - self.start, height), :]
            value = given[k + self.sx, pl.ds(start - 8 + self.sy, height), :]
            target[k + self.ox, pl.ds(start, height), :] = (value if zero else value + totals[i]) * weight

    def restrict_to(self, target, corner, pairs):
        rows, extra = self.tall, self.spare // 2
        if rows < 16:
            pairs[...] = jnp.zeros_like(pairs)
        ks = list(range(-extra, self.pairs + extra))
        ats = [k + self.ox for k in ks]
        first = 8 - self.spare
        even = even_cells(rows, first)
        reds = around(self.b, ats, first, rows, even, 0, self.beside, GRID_SHARE)
        blacks = around(self.r, ats, first, rows, even, 1, self.beside, GRID_SHARE)
        for i, k in enumerate(ks):
            kind = self.kind(k, False)
            at = (k + self.ox, pl.ds(first, rows), slice(None))
            own = (k + self.sx, pl.ds(self.sy - self.spare, rows), slice(None))
            red = self.gr[own] - (self.d[kind] * self.r[at] - reds[i])
            black = self.gb[own] - (self.d[swapped(kind)] * self.b[at] - blacks[i])
            pairs[i, pl.ds(0, rows), :] = red + black
        narrow(2 * len(ks), rows, self.dims[2], self.spare, target, [at - self.spare // 2 for at in corner], pairs)

    def reflect(self):
        (x, y, z), r, b, ox = self.dims, self.r, self.b, self.ox
        margin = 2 if self.reach else 0
        for_all = pl.ds(ox - margin, self.pairs + 2 * margin)

        def across(to, at):
            r[to] = -b[at]
            b[to] = -r[at]
        sides = (
            (0, 0, lambda: across(ox - 1, ox)),
            (0, 1, lambda: across(ox + self.pairs, ox + self.pairs - 1)),
            (1, 0, lambda: across((for_all, pl.ds(7, 1)), (for_all, pl.ds(8, 1)))),
            (1, 1, lambda: across((for_all, pl.ds(8 + y, 1)), (for_all, pl.ds(7 + y, 1)))),
        )
        for axis, high, step in sides:
            if isinstance(self.places[axis], int):
                step()
            else:
                pl.when(self.places[axis] == (self.counts[axis] - 1 if high else 0))(step)

    def planes(self, step, many, low, tall):
        even = even_cells(tall)
        out = []
        for i in range(many // 2):
            at = (step * (many // 2) + (low // 2 + i + self.ox), pl.ds(0, tall), slice(None))
            r, b = self.r[at], self.b[at]
            out += [jnp.where(even, r, b), jnp.where(even, b, r)]
        return out


def swapped(kind):
    if isinstance(kind, int):
        return {1: 2, 2: 1}.get(kind, kind)
    return jnp.where(kind == 1, 2, jnp.where(kind == 2, 1, kind))


class Block:
    def __init__(self, v, dims, places, counts):
        self.v, self.dims, self.places, self.counts = v, dims, places, counts

    def planes(self, step, many, low, tall):
        return [self.v[step * many + (low + 4 + i), pl.ds(0, tall), :] for i in range(many)]


def narrow(planes, rows, z, spare, target, corner, pairs):
    coarse_rows = rows_of(rows // 2)
    source_lane = signed(lax.broadcasted_iota(jnp.int32, (LANES, LANES), 0))
    target_lane = signed(lax.broadcasted_iota(jnp.int32, (LANES, LANES), 1))
    inside = (source_lane >= -spare) & (source_lane < z + spare)
    halve = jnp.where(((source_lane + LANES) // 2 - LANES // 2 == target_lane) & inside, 0.5, 0.0).astype(jnp.bfloat16)
    planes = planes // 2
    many = widest(planes, max(2, 1024 // coarse_rows), 2)

    def second(step):
        at = pl.ds(step * many, many)
        q = pairs[at, pl.ds(0, coarse_rows, stride=2), :] + pairs[at, pl.ds(1, coarse_rows, stride=2), :]
        q = near_dot(q.reshape(many * coarse_rows, LANES), halve)
        q = q.reshape(many, coarse_rows, LANES)
        if not isinstance(target, tuple):
            target[pl.ds(step * many + corner[0], many), pl.ds(corner[1], coarse_rows), :] = q
            return
        even = even_cells(coarse_rows, corner[1])
        for i in range(many // 2):
            at = (step * (many // 2) + (corner[0] // 2 + i), pl.ds(corner[1], coarse_rows), slice(None))
            target[0][at] = jnp.where(even, q[2 * i], q[2 * i + 1])
            target[1][at] = jnp.where(even, q[2 * i + 1], q[2 * i])
    loop(planes // many, second)


def spare_of(number, dims):
    spare = SPARE.get(number, 0)
    return spare, -(-(dims[1] + 2 * spare) // 16) * 16 if spare else rows_of(dims[1])


def layout(number, dims):
    x, y, z = dims
    if number in REACH:
        reach = REACH[number]
        height = rows_of(y + 2 * reach)
        return EDGE // 2, 8 - reach, height, x // 2 + EDGE, max(40, y + 24)
    if number == SHARED:
        return EDGE // 2, 8, rows_of(y), x // 2 + EDGE, rows_of(y) + 24
    return 1, 8, rows_of(y), x // 2 + 2, rows_of(y) + 16


def inner_height(number, dims):
    return rows_of(dims[1] + 2 * REACH[number] - 2)


def below_zero(number):
    return -((FINAL[number] + 3) // 2) if number in FINAL else 0


def lift_shape(number, coarse):
    low = below_zero(number)
    count = coarse[0] - 2 * low
    height = rows_of(coarse[1] - 2 * low)
    first = (low - 1) // 2 * 2
    return low, count, height, first, -(-(low + count + 1 - first) // 2) * 2, rows_of(8 + low + height + 1)


def widen(below, number, spread, centre):
    dims, places, counts = below.dims, below.places, below.counts
    z = dims[2]
    _, _, _, start, planes, tall = lift_shape(number, dims)
    beyond = EDGE if number in FINAL else 0
    k = signed(lax.broadcasted_iota(jnp.int32, (LANES, LANES), 0))
    f = signed(lax.broadcasted_iota(jnp.int32, (LANES, LANES), 1))
    at = places[2] * (2 * z) + f
    inside = (f >= -beyond) & (f < 2 * z + beyond) & (at >= 0) & (at < counts[2] * 2 * z)
    parent = (f + LANES) // 2 - LANES // 2
    near = parent + jnp.where((f + LANES) % 2 == 1, 1, -1)
    outside = (places[2] * z + near < 0) | (places[2] * z + near >= counts[2] * z)
    own = jnp.where((k == parent) & inside, 0.25, 0.0)
    beside = jnp.where((k == near) & inside, 0.25, 0.0)
    both = own + jnp.where(outside, -own, beside)
    matrix = jnp.concatenate([own, both], axis=1).astype(jnp.bfloat16)
    many = widest(planes, max(2, 2048 // tall), 2)

    def first(step):
        e = jnp.concatenate(below.planes(step, many, start, tall), axis=0)
        product = near_dot(e, matrix)
        at = pl.ds(step * many, many)
        spread[at] = product[:, :LANES].reshape(many, tall, LANES)
        centre[at] = product[:, LANES:].reshape(many, tall, LANES)
    loop(planes // many, first)


def lift(below, fine, spread, centre):
    (x, y, z), places, counts = below.dims, below.places, below.counts
    number = fine.number
    low, count, height, start, _, _ = lift_shape(number, below.dims)
    beyond = number in FINAL
    widen(below, number, spread, centre)
    group = widest(count, max(1, 1536 // height))
    row = places[1] * y + row_iota(height) + low
    valid = (row >= 0) & (row < counts[1] * y)
    even = lane_iota(height) % 2 == 0
    skip = low - start

    def second(step):
        for i in range(group):
            plane = step * group + i
            middle = centre[plane + skip, pl.ds(8 + low, height), :]
            ys = (spread[plane + skip, pl.ds(7 + low, height), :], spread[plane + skip, pl.ds(9 + low, height), :])
            xs = [spread[plane + skip + 2 * up_x - 1, pl.ds(8 + low, height), :] for up_x in range(2)]
            here = valid
            if beyond:
                at = places[0] * x + plane + low
                here = valid & ((at >= 0) & (at < counts[0] * x))
            for up_y in range(2):
                q = (middle + ys[up_y]) + jnp.where(even, xs[1 - up_y], xs[up_y])
                if beyond or y < height:
                    q = jnp.where(here, q, 0.0)
                at = (plane + low + fine.ox, pl.ds(8 + 2 * low + up_y, height, stride=2), slice(None))
                fine.b[at] = fine.b[at] + q
    loop(count // group, second)


def exists(places, counts, way, sign):
    found = None
    for axis in range(3):
        if way[axis]:
            other = places[axis] + sign * way[axis]
            one = (other >= 0) if sign * way[axis] < 0 else (other < counts[axis])
            found = one if found is None else found & one
    return found


def along(places, way):
    return {name: places[axis] + way[axis] for axis, name in enumerate(AXES) if way[axis]}


class Top:
    number, ox, sets = 0, 2, 4

    def __init__(self, dims, places, counts, beside, r, b, gr, gb, w, d, out, got, sems):
        self.beside = beside
        self.dims, self.places, self.counts = dims, places, counts
        self.r, self.b, self.gr, self.gb, self.w, self.d = r, b, gr, gb, w, d
        self.out, self.got, self.sems = out, got, sems
        self.pairs, self.n = dims[0] // 2, dims[1]

    @staticmethod
    def weights(dims, places, counts, height, start, beyond):
        x, y, z = dims
        row, lane = row_iota(height) + (start - 8), signed(lane_iota(height))
        at_y, at_z = places[1] * y + row, places[2] * z + lane
        last_y, last_z = counts[1] * y - 1, counts[2] * z - 1
        valid = (lane >= -beyond) & (lane < z + beyond) & (at_y >= 0) & (at_y <= last_y) & (at_z >= 0) & (at_z <= last_z)
        one = lambda at, last: (at == 0).astype(jnp.float32) + (at == last).astype(jnp.float32)
        return valid, 6.0 + one(at_y, last_y) + one(at_z, last_z), (row + lane + LANES) % 2 == 0

    def clear(self):
        for ref in (self.r, self.b, self.gr, self.gb):
            ref[...] = jnp.zeros_like(ref)

    def prepare(self):
        valid, diagonal, even = self.weights(self.dims, self.places, self.counts, self.n + 8, 6, 4)
        plain, more = (jnp.where(valid, 1.0 / (diagonal + wall), 0.0) for wall in range(2))
        self.w[0] = plain
        self.w[1] = jnp.where(even, more, plain)
        self.w[2] = jnp.where(even, plain, more)
        self.w[3] = jnp.zeros_like(plain)
        write_diagonals(self.d, self.dims, self.places, self.counts)

    def missing(self):
        for way in WAYS:
            @pl.when(jnp.logical_not(exists(self.places, self.counts, way, -1)))
            def _(way=way):
                self.got[way][...] = jnp.zeros_like(self.got[way])

    def kind(self, pair):
        at = self.places[0] * self.pairs + pair
        last = self.counts[0] * self.pairs - 1
        return jnp.where((at < 0) | (at > last), 3, jnp.where(at == 0, 1, jnp.where(at == last, 2, 0)))

    def sweep(self, colour):
        start, height = 6, self.n + 8
        source, target, given = (self.r, self.b, self.gb) if colour else (self.b, self.r, self.gr)
        count = self.pairs + 2
        chunk = widest(count, 34)
        even = (row_iota(height) + lane_iota(height)) % 2 == 0

        def body(step):
            ats = [step * chunk + i + 1 for i in range(chunk)]
            for at, total in zip(ats, around(source, ats, start, height, even, colour, self.beside, SWEEP_SHARE)):
                k = at - 2
                kind = self.kind(k)
                if colour:
                    kind = jnp.where(kind == 1, 2, jnp.where(kind == 2, 1, kind))
                target[at, pl.ds(start, height), :] = (given[at, pl.ds(start, height), :] + total) * self.w[kind]
        loop(count // chunk, body)

    def restrict_to(self, target, corner, pairs):
        n = self.n
        even = (row_iota(n) + lane_iota(n)) % 2 == 0
        chunk = 16

        def body(step):
            ks = [step * chunk + i for i in range(chunk)]
            kinds = [self.kind(k) for k in ks]
            ats = [k + 2 for k in ks]
            for k, (red, black) in zip(ks, remainders(self.r, self.b, self.gr, self.gb, self.d, ats, kinds, even, n, self.beside, REST_SHARE)):
                pairs[k] = red + black
        loop(self.pairs // chunk, body)
        narrow(self.dims[0], n, self.dims[2], 0, target, corner, pairs)

    @staticmethod
    def shapes(n):
        face = {0: (2, n, LANES), 1: (n // 4, 8, LANES), 2: (3, n, LANES)}
        sent = [face[0], face[0], face[1], face[1], face[2], face[2], (4, 8, LANES)]
        got = {}
        for way in WAYS:
            if sum(map(abs, way)) == 1:
                got[way] = face[[abs(part) for part in way].index(1)]
            elif not way[2]:
                got[way] = (2, 8, LANES)
            elif not way[0]:
                got[way] = (2, 8, LANES)
            else:
                got[way] = (8, LANES)
        return sent, got

    def copies(self, way, again):
        n, out, got = self.n, self.out, self.got[way]
        high = [part > 0 for part in way]
        if sum(map(abs, way)) == 1:
            axis = [abs(part) for part in way].index(1)
            source = out[2 * axis + high[axis]]
            if again and axis != 1:
                source, got = source.at[pl.ds(0, 1)], got.at[pl.ds(0, 1)]
        elif not way[2]:
            source = out[2 + high[1]].at[pl.ds(n // 4 - 2 if high[0] else 0, 2)]
        elif not way[0]:
            row = pl.ds(n - 8 if high[1] else 0, 8)
            source = out[4 + high[2]].at[pl.ds(0, 2), row]
        else:
            source = out[6].at[2 * high[0] + high[2]]
        k = WAYS.index(way)
        return pltpu.make_async_remote_copy(
            src_ref=source, dst_ref=got, send_sem=self.sems[0].at[k], recv_sem=self.sems[1].at[k],
            device_id=along(self.places, way), device_id_type=MESH)

    def pack_ends(self, part, again):
        tile = lane_iota(8)
        many = self.pairs // self.sets
        ahead = (tile + (LANES - 60)) % LANES
        wide = 4 * many
        for t in range(self.n // 8):
            at = pl.ds(8 * t, 8)
            for index, ref in enumerate([self.b] if again else [self.b, self.gr, self.gb]):
                first = last = None
                for k in range(part * many, part * many + many):
                    moved = turn(ref[k + 2, pl.ds(8 * t + 8, 8), :], 4 * k)
                    first = moved if first is None else jnp.where(tile // 4 == k, moved, first)
                    last = moved if last is None else jnp.where(ahead // 4 == k, moved, last)
                if part:
                    first = jnp.where(tile // wide == part, first, self.out[4][index, at])
                    last = jnp.where(ahead // wide == part, last, self.out[5][index, at])
                self.out[4][index, at] = first
                self.out[5][index, at] = last

    def pack(self, again):
        n, pairs = self.n, self.pairs
        low, tile = lane_iota(n) < 64, lane_iota(8)
        row = row_iota(8)
        half = pairs // 2
        own = lambda ref, k: ref[k + 2, pl.ds(8, n), :]
        for high in range(2):
            near, far = (pairs - 1, pairs - 2) if high else (0, 1)
            self.out[high][0] = jnp.where(low, own(self.b, near), pltpu.roll(own(self.b, far), 64, 1))
            if not again:
                self.out[high][1] = jnp.where(low, own(self.gr, near), pltpu.roll(own(self.gb, near), 64, 1))

            def edge(k, high=high):
                first = 8 + n - 8 if high else 8
                b = self.b[k + 2, pl.ds(first, 8), :]
                if again:
                    return b
                red, black = (pltpu.roll(ref[k + 2, pl.ds(first, 8), :], by, 0) for ref, by in ((self.gr, 4), (self.gb, 2 if high else 6)))
                if high:
                    return jnp.where(row >= 4, b, jnp.where(row >= 2, red, black))
                return jnp.where(row < 4, b, jnp.where(row < 6, red, black))
            for k in range(half):
                self.out[2 + high][k] = jnp.where(tile < 64, edge(k), pltpu.roll(edge(k + half), 64, 1))
        for high_x in range(2):
            for high_z in range(2):
                offset = 60 if high_z else 0
                pair, near = (pairs - 2, pairs - 1) if high_x else (0, 0)
                value = jnp.zeros((8, LANES), jnp.float32)
                for t in range(n // 8):
                    rows = pl.ds(8 * t, 8)
                    moved = turn(self.out[4 + high_z][0, rows], 16 * t - 4 * pair - offset)
                    value = jnp.where((tile >= 16 * t) & (tile < 16 * t + 8), moved, value)
                    if not again:
                        moved = turn(self.out[4 + high_z][1, rows], 16 * t + 8 - 4 * near - offset)
                        value = jnp.where((tile >= 16 * t + 8) & (tile < 16 * t + 16), moved, value)
                self.out[6][2 * high_x + high_z] = value

    def post(self, again=False):
        for part in range(self.sets):
            self.pack_ends(part, again)
        self.pack(again)
        self.send(again)

    def send(self, again=False):
        for way in WAYS:
            pl.when(exists(self.places, self.counts, way, 1))(self.copies(way, again).start)

    def sent(self, again=False):
        for way in WAYS:
            pl.when(exists(self.places, self.counts, way, 1))(self.copies(way, again).wait_send)

    def wait(self, ways, again):
        for way in ways:
            pl.when(exists(self.places, self.counts, way, -1))(self.copies(way, again).wait_recv)

    def land(self, again=False):
        n, pairs, got = self.n, self.pairs, self.got
        half = pairs // 2
        arrays = [self.b] if again else [self.b, self.gr, self.gb]
        lane, tile = lane_iota(n), lane_iota(8)

        def ends(high, low, to, k):
            pick = to % 8 < 4
            return turn(jnp.where(pick, high, low) if k % 2 == 0 else jnp.where(pick, low, high), 64 - 4 * k)
        self.wait([way for way in WAYS if not (way[0] or way[1])], again)
        high, low = got[(0, 0, -1)], got[(0, 0, 1)]

        def body(t):
            at = pl.ds(t * 8, 8)
            packs = [(high[index, at], low[index, at]) for index in range(len(arrays))]
            for k in range(pairs):
                own = (k + 2, pl.ds(t * 8 + 8, 8), slice(None))
                for (h, l), ref in zip(packs, arrays):
                    ref[own] = jnp.where(tile < 64, ref[own], ends(h, l, tile, k))
        for t in range(n // 8):
            body(t)
        self.wait([way for way in WAYS if way[1] and not way[0]], again)
        for side in (-1, 1):
            face = got[(0, -side, 0)]
            base = 8 + n if side > 0 else 0
            shifts = (0, 4, 2 if side > 0 else 6)
            for index, ref in enumerate(arrays):
                if index < 2:
                    h, l = got[(0, -side, -1)][index], got[(0, -side, 1)][index]
                for k in range(pairs):
                    value = face[k % half]
                    if k >= half:
                        value = pltpu.roll(value, 64, 1)
                    if shifts[index]:
                        value = pltpu.roll(value, shifts[index], 0)
                    if index < 2:
                        value = jnp.where(tile < 64, value, ends(h, l, tile, k))
                    ref[k + 2, pl.ds(base, 8), :] = value
        self.wait([way for way in WAYS if way[0]], again)
        for side in (-1, 1):
            face = got[(-side, 0, 0)]
            near, far = (pairs + 2, pairs + 3) if side > 0 else (1, 0)
            high, low = got[(-side, 0, -1)], got[(-side, 0, 1)]
            near_lane, far_lane = (0, 4) if side > 0 else (4, 0)

            def beside(first, at, high=high, low=low):
                out = []
                for t in at:
                    up = turn(high[...], 64 - 16 * t - first)
                    out.append(jnp.where(tile < 96, up, turn(low[...], 124 - 16 * t - first)))
                return jnp.concatenate(out, axis=0) if len(out) > 1 else out[0]
            every = range(n // 8)
            both = face[0]
            self.b[near, pl.ds(8, n), :] = jnp.where(lane < 64, both, beside(near_lane, every))
            self.b[far, pl.ds(8, n), :] = jnp.where(lane < 64, pltpu.roll(both, 64, 1), beside(far_lane, every))
            if not again:
                both = face[1]
                self.gr[near, pl.ds(8, n), :] = jnp.where(lane < 64, both, beside(8, every))
                self.gb[near, pl.ds(8, n), :] = pltpu.roll(both, 64, 1)
            for up in (-1, 1):
                edge = got[(-side, -up, 0)]
                base = 8 + n if up > 0 else 0
                corner = (got[(-side, -up, -1)], got[(-side, -up, 1)])
                t = [0 if up > 0 else n // 8 - 1]
                if side > 0:
                    pieces = {near: (0, False), far: (1, False)}
                else:
                    pieces = {near: (1, True), far: (0, True)}
                for place, (group, upper) in pieces.items():
                    value = edge[group]
                    if upper:
                        value = pltpu.roll(value, 64, 1)
                    first = near_lane if place == near else far_lane
                    self.b[place, pl.ds(base, 8), :] = jnp.where(tile < 64, value, beside(first, t, *corner))
                    if place == near and not again:
                        self.gr[place, pl.ds(base, 8), :] = pltpu.roll(value, 4, 0)


def around(source, ats, start, height, even, colour, beside, share):
    rows = pl.ds(start, height)
    centres = [source[at, rows, :] for at in ats]
    out = []
    for at, s, z_sum in zip(ats, centres, lane_sums(centres, beside, share)):
        left, right = source[at - 1, rows, :], source[at + 1, rows, :]
        across = jnp.where(even, right, left) if colour else jnp.where(even, left, right)
        total = (s + across) + (source[at, pl.ds(start + 1, height), :] + source[at, pl.ds(start - 1, height), :])
        out.append(total + z_sum)
    return out


def remainders(r, b, gr, gb, d, ats, kinds, even, n, beside, share):
    rows = pl.ds(8, n)
    out = []
    for at, kind, reds, blacks in zip(ats, kinds, around(b, ats, 8, n, even, 0, beside, share), around(r, ats, 8, n, even, 1, beside, share)):
        other = swapped(kind)
        out.append((gr[at, rows, :] - (d[kind] * r[at, rows, :] - reds), gb[at, rows, :] - (d[other] * b[at, rows, :] - blacks)))
    return out


def write_diagonals(d, dims, places, counts):
    _, diagonal, even = Top.weights(dims, places, counts, dims[1], 8, 0)
    d[0] = diagonal
    d[1] = jnp.where(even, diagonal + 1.0, diagonal)
    d[2] = jnp.where(even, diagonal, diagonal + 1.0)


class Ring:
    def __init__(self, level, refs, sems):
        self.level, self.sems = level, sems
        self.body, self.parts = refs[0], refs[1:-len(WAYS)]
        self.got = dict(zip(WAYS, refs[-len(WAYS):]))
        self.places, self.counts = level.places, level.counts

    @staticmethod
    def sizes(n):
        each = LANES // n
        cut = n if n <= 16 else 8
        return each, max(1, n // each), cut, LANES // cut, max(1, n * cut // LANES)

    @staticmethod
    def thick(n, reach, way):
        each, groups, _, _, cuts = Ring.sizes(n)
        if not way[0]:
            return cuts if way[2] else groups
        return 1 if way[2] else -(-reach // each)

    @staticmethod
    def shape(n, reach, way):
        return (Ring.thick(n, reach, way), 8 if way[1] else n, LANES)

    def clear(self):
        for way in WAYS:
            @pl.when(jnp.logical_not(exists(self.places, self.counts, way, -1)))
            def _(way=way):
                self.got[way][...] = jnp.zeros_like(self.got[way])

    def copy(self, way):
        n = self.level.dims[0]
        shape = Ring.shape(n, self.level.reach, way)
        source = self.body
        if way[2] and self.parts:
            source = self.parts[0] if way[2] < 0 else self.parts[1]
        groups = source.shape[0]
        group = 0 if way[0] <= 0 else groups - shape[0]
        row = 0 if way[1] <= 0 else n - 8
        k = WAYS.index(way)
        return pltpu.make_async_remote_copy(
            src_ref=source.at[pl.ds(group, shape[0]), pl.ds(row, shape[1])], dst_ref=self.got[way],
            send_sem=self.sems[0].at[k], recv_sem=self.sems[1].at[k],
            device_id={name: self.places[axis] + way[axis] for axis, name in enumerate(AXES) if way[axis]}, device_id_type=MESH)

    def post(self):
        n, gr, gb = self.level.dims[0], self.level.gr, self.level.gb
        each, groups, cut, cuts_each, cuts = Ring.sizes(n)
        even = even_cells(n)

        def plane(x):
            at = (x // 2 + EDGE // 2, pl.ds(8, n), slice(None))
            value = jnp.where(even, gb[at], gr[at]) if x % 2 else jnp.where(even, gr[at], gb[at])
            return jnp.where(lane_iota(n) < n, value, 0.0) if SPARE.get(self.level.number - 1) else value
        for g in range(groups):
            value = plane(g * each)
            for i in range(1, min(each, n)):
                value = value + turn(plane(g * each + i), i * n)
            self.body[g] = value
        if self.parts:
            lane = lane_iota(n)
            for g in range(cuts):
                low = high = jnp.zeros((n, LANES), jnp.float32)
                for i in range(cuts_each):
                    moved = turn(plane(g * cuts_each + i), cut * i)
                    low = jnp.where(lane // cut == i, moved, low)
                    high = jnp.where((lane + (LANES - n + cut)) % LANES // cut == i, moved, high)
                self.parts[0][g] = low
                self.parts[1][g] = high
        for way in sorted(WAYS, key=all):
            pl.when(exists(self.places, self.counts, way, 1))(self.copy(way).start)

    def land(self, near=False, rest=False):
        n, gr, gb, reach = self.level.dims[0], self.level.gr, self.level.gb, self.level.reach
        reach = 2 if near else reach + reach % 2
        each, groups, cut, cuts_each, cuts = Ring.sizes(n)
        for to_x, to_y in sorted(itertools.product((-1, 0, 1), repeat=2), key=lambda at: abs(at[0]) * 3 + abs(at[1])):
            for way in WAYS:
                if way[:2] == (-to_x, -to_y) and not (near and all(way)) and (all(way) or not rest):
                    pl.when(exists(self.places, self.counts, way, -1))(self.copy(way).wait_recv)
            height = 8 if to_y else n
            row = {-1: 0, 0: 8, 1: 8 + n}[to_y]
            lane = lane_iota(height)
            body = self.got[(-to_x, -to_y, 0)] if to_x or to_y else None
            high = self.got[(-to_x, -to_y, -1)]
            low = self.got[(-to_x, -to_y, 1)]

            made = {}

            def merged(h, flip, made=made, high=high, low=low, lane=lane):
                if (h, flip) not in made:
                    both = (high[h], turn(low[h], -2 * n))
                    made[h, flip] = jnp.where(lane % 16 < 8, both[flip], both[1 - flip])
                return made[h, flip]
            even = even_cells(height, row)

            def value(x, body=body, high=high, low=low, lane=lane, merged=merged, to_x=to_x):
                g, h = x // each, x // cuts_each
                if to_x < 0:
                    g, h = g - (groups - body.shape[0]), h - (cuts - high.shape[0])
                if near and to_x and to_y:
                    return jnp.where(lane < n, turn(body[g], -(x % each) * n), 0.0)
                if n == 8:
                    ends = jnp.where(lane < 64, turn(high[h], n - cut * (x % cuts_each)), turn(low[h], -n - cut * (x % cuts_each)))
                else:
                    ends = turn(merged(h, x % 2 if n == 32 else 0), n - cut * (x % cuts_each))
                return ends if body is None else jnp.where(lane < n, turn(body[g], -(x % each) * n), ends)
            for x in {-1: range(n - reach, n, 2), 0: range(0, n, 2), 1: range(0, reach, 2)}[to_x]:
                at = (EDGE // 2 + (to_x * n + x) // 2, pl.ds(row, height), slice(None))
                first, second = value(x), value(x + 1)
                red, black = jnp.where(even, first, second), jnp.where(even, second, first)
                if body is None:
                    red, black = jnp.where(lane < n, gr[at], red), jnp.where(lane < n, gb[at], black)
                gr[at] = red
                gb[at] = black

    def finish(self):
        for way in WAYS:
            pl.when(exists(self.places, self.counts, way, 1))(self.copy(way).wait_send)


def solve_kernel(counts, blocks, coarse, refs):
    right_side, guess, r, b, gr, gb = refs[:6]
    refs = list(refs[6:])
    take = lambda count=1: [refs.pop(0) for _ in range(count)] if count > 1 else refs.pop(0)
    places = tuple(lax.axis_index(axis) for axis in AXES)
    n0 = blocks[0][0]
    raw_g, raw_v, raw_sems = take(3)
    sent_shapes, got_shapes = Top.shapes(n0)
    w0, d0, beside = take(3)
    top = Top(blocks[0], places, counts, beside, r, b, gr, gb, w0, d0, take(len(sent_shapes)), dict(zip(WAYS, take(len(WAYS)))), take(2))
    levels = [top]
    for number in range(1, LEVELS):
        if number < SHARED:
            levels.append(Grid(number, blocks[number], places, counts, beside, *take(6)))
        else:
            levels.append(Grid(number, coarse[number - SHARED], (0, 0, 0), (1, 1, 1), beside, *take(6)))
    rings = {}
    for number in REACH:
        n = blocks[number][0]
        members = take(1 + (2 if Ring.sizes(n)[2] != n else 0) + len(WAYS))
        rings[number] = Ring(levels[number], members, take(2))
    pairs = take(LEVELS - 1)
    spreads = take(LEVELS - 1)
    centres = take(LEVELS - 1)
    block_s, block_v, packet, line, joined, packets, line_send, line_recv, gather_send, gather_recv, spread_sem = refs

    cut = n0 // top.sets
    loads = [[pltpu.make_async_copy(source.at[pl.ds(part * cut, cut)], target.at[pl.ds(part * cut, cut)], raw_sems.at[i, part])
              for i, (source, target) in enumerate(((right_side, raw_g), (guess, raw_v)))] for part in range(top.sets)]
    for load in sum(loads, []):
        load.start()
    barrier = pltpu.get_barrier_semaphore()
    nx, ny, nz = counts

    def greet(device):
        pl.semaphore_signal(barrier, inc=1, device_id=device, device_id_type=MESH)

    def around_torus(way, far):
        return {name: lax.rem(places[axis] + way[axis] * far + counts[axis], counts[axis]) for axis, name in enumerate(AXES) if way[axis]}

    for way in WAYS:
        greet(around_torus(way, 1))

    def tell(turn):
        for way in FLAT:
            pl.semaphore_signal(spread_sem.at[turn], inc=1, device_id=around_torus(way, turn + 1), device_id_type=MESH)

    def hear(turn):
        pl.semaphore_wait(spread_sem.at[turn], len(FLAT))

    top.clear()
    top.prepare()
    write_beside(beside)
    top.missing()
    even = (lax.broadcasted_iota(jnp.int32, (n0, n0), 0) + lax.broadcasted_iota(jnp.int32, (n0, n0), 1)) % 2 == 0
    for part in range(top.sets):
        for load in loads[part]:
            load.wait()
        for k in range(part * cut // 2, (part + 1) * cut // 2):
            at = (k + 2, pl.ds(8, n0), pl.ds(0, n0))
            first, second = raw_g[2 * k], raw_g[2 * k + 1]
            gr[at] = jnp.where(even, first, second)
            gb[at] = jnp.where(even, second, first)
            b[at] = jnp.where(even, raw_v[2 * k + 1], raw_v[2 * k])
        top.pack_ends(part, False)
    top.pack(False)
    pl.semaphore_wait(barrier, len(WAYS))
    top.send()
    tell(0)
    for level in levels[1:]:
        level.prepare()
    for ring in rings.values():
        ring.clear()
    block_v[...] = jnp.zeros_like(block_v)
    top.land()
    hear(0)
    tell(1)
    top.sweep(0)
    top.sweep(1)
    top.restrict_to((levels[1].gr, levels[1].gb), (EDGE, 8), pairs[0])
    for number in range(1, SHARED - 1):
        level = levels[number]
        rings[number].post()
        if number == 1:
            rings[1].land(near=True)
            level.sweep(0, zero=True, beyond=2)
            level.sweep(1, beyond=1)
        else:
            rings[1].land(rest=True)
            levels[1].sweep(0, zero=True, beyond=levels[1].reach)
            levels[1].sweep(1, beyond=levels[1].reach - 1)
            rings[number].land()
            level.sweep(0, zero=True, beyond=level.reach)
            level.sweep(1, beyond=level.reach - 1)
        level.restrict_to((levels[number + 1].gr, levels[number + 1].gb), (EDGE, 8), pairs[number])
    last = levels[SHARED - 1]
    last.sweep(0, zero=True, beyond=2)
    last.sweep(1, beyond=1)
    last.restrict_to(block_s, (0, 0), pairs[SHARED - 1])
    hear(1)

    bx, by, bz = blocks[SHARED]
    wide = LANES // bx
    packed = jnp.zeros((rows_of(by), LANES), jnp.float32)
    for x in range(bx):
        packed = packed + pltpu.roll(block_s[x], x * wide + places[2] * bz, 1)
    packet[...] = packed[:by]

    def line_copy(source, target):
        return pltpu.make_async_remote_copy(
            src_ref=packet, dst_ref=line.at[source], send_sem=line_send.at[target], recv_sem=line_recv.at[source],
            device_id={AXES[2]: target}, device_id_type=MESH)

    for offset in range(1, nz):
        line_copy(places[2], lax.rem(places[2] + offset, nz)).start()
    rings[1].finish()
    rings[SHARED - 1].post()
    top.sent()
    top.post(True)
    merged = packed[:by]
    for offset in range(1, nz):
        source = lax.rem(places[2] + nz - offset, nz)
        line_copy(source, lax.rem(places[2] + offset, nz)).wait_recv()
        merged = merged + line[source]
    joined[...] = merged
    total = nx * ny
    me = places[0] * ny + places[1]

    def plane_copy(to_x, to_y):
        return pltpu.make_async_remote_copy(
            src_ref=joined, dst_ref=packets.at[me], send_sem=gather_send, recv_sem=gather_recv,
            device_id={AXES[0]: to_x, AXES[1]: to_y}, device_id_type=MESH)

    xs = [lax.rem(places[0] + step, nx) for step in range(nx)]
    ys = [lax.rem(places[1] + step, ny) for step in range(ny)]
    far = lambda at: min(at[0], nx - at[0]) + min(at[1], ny - at[1])
    for to_x, to_y in sorted(itertools.product(range(nx), range(ny)), key=far, reverse=True)[:-1]:
        plane_copy(xs[to_x], ys[to_y]).start()
    packets[me] = merged
    rings[SHARED - 1].land()
    last.sweep(0, zero=True, beyond=last.reach)
    last.sweep(1, beyond=last.reach - 1)
    top.land(True)
    top.sent(True)
    for number in (SHARED - 2, SHARED - 1):
        rings[number].finish()
    for offset in range(1, nz):
        line_copy(places[2], lax.rem(places[2] + offset, nz)).wait_send()
    everyone = pltpu.make_async_remote_copy(
        src_ref=packets.at[pl.ds(0, total - 1)], dst_ref=packets.at[pl.ds(0, total - 1)], send_sem=gather_send, recv_sem=gather_recv,
        device_id={AXES[0]: places[0]}, device_id_type=MESH)
    everyone.wait_recv()
    whole = levels[SHARED]

    def unpack(px):
        for py in range(0, ny, 2):
            pair = jnp.concatenate([packets[px * ny + py], packets[px * ny + py + 1]], axis=0)
            cells = even_cells(2 * by)
            for x in range(0, bx, 2):
                first, second = turn(pair, -x * wide), turn(pair, -(x + 1) * wide)
                at = (px * (bx // 2) + x // 2, pl.ds(py * by, 2 * by), slice(None))
                whole.gr[at] = jnp.where(cells, first, second)
                whole.gb[at] = jnp.where(cells, second, first)
    loop(nx, unpack)

    for number in range(SHARED, LEVELS - 1):
        level = levels[number]
        level.sweep(0, zero=True)
        level.sweep(1)
        level.restrict_to((levels[number + 1].gr, levels[number + 1].gb), (0, 0), pairs[number])
    level = levels[LEVELS - 1]
    level.sweep(0, zero=True)
    level.sweep(1)
    for _ in range(COARSE_SWEEPS - 1):
        level.sweep(0)
        level.sweep(1)
    for number in reversed(range(SHARED, LEVELS - 1)):
        level, below = levels[number], levels[number + 1]
        below.reflect()
        lift(below, level, spreads[number], centres[number])
        level.sweep(0)
        level.sweep(1)

    whole.reflect()
    shift = lax.rem(LANES - places[2] * bz, LANES)
    odd = lax.rem(places[1] + 1, 2) == 1
    cells = even_cells(24)
    for x in range(0, bx + 8, 2):
        at = (places[0] * (bx // 2) + (x // 2 - 2 + whole.ox), pl.ds(pl.multiple_of((places[1] + 1) // 2 * 8, 8), 24), slice(None))
        r_part, b_part = whole.r[at], whole.b[at]
        for i, part in enumerate((jnp.where(cells, r_part, b_part), jnp.where(cells, b_part, r_part))):
            block_v[x + i, pl.ds(4, 16)] = pltpu.roll(jnp.where(odd, part[4:20], part[:16]), shift, 1)
    around_block = Block(block_v, blocks[SHARED], places, counts)
    lift(around_block, levels[SHARED - 1], spreads[SHARED - 1], centres[SHARED - 1])
    for number in reversed(range(1, SHARED)):
        level = levels[number]
        level.sweep(0, beyond=level.reach - 2)
        level.sweep(1, beyond=level.reach - 3)
        level.reflect()
        lift(level, levels[number - 1], spreads[number - 1], centres[number - 1])
    top.sweep(0)
    top.sweep(1)

    everyone.wait_send()


def finish_kernel(counts, dims, r, b, gr, gb, solution, residual, out_v, out_r, d, beside, sems):
    places = tuple(lax.axis_index(axis) for axis in AXES)
    n, half = dims[1], dims[0] // 2
    write_diagonals(d, dims, places, counts)
    write_beside(beside)
    even = even_cells(n)
    last = counts[0] * half - 1
    group = 8

    def copies(step):
        part = pl.ds(step * 2 * group, 2 * group)
        return [pltpu.make_async_copy(source.at[part], target.at[part], sems.at[i, step])
                for i, (source, target) in enumerate(((out_v, solution), (out_r, residual)))]

    def compute(step):
        ks = [step * group + i for i in range(group)]
        globally = [places[0] * half + k for k in ks]
        kinds = [jnp.where(at == 0, 1, jnp.where(at == last, 2, 0)) for at in globally]
        results = remainders(r, b, gr, gb, d, [k + 2 for k in ks], kinds, even, n, beside, LAST_SHARE)
        for k, (red, black) in zip(ks, results):
            own = (k + 2, pl.ds(8, n), slice(None))
            for out, x, y in ((out_v, r[own], b[own]), (out_r, red, black)):
                out[2 * k] = jnp.where(even, x, y)[:, :n]
                out[2 * k + 1] = jnp.where(even, y, x)[:, :n]
        for copy in copies(step):
            copy.start()
    for step in range(half // group):
        compute(step)
    for step in range(half // group):
        for copy in copies(step):
            copy.wait()


def solution(mesh):
    counts = tuple(mesh.shape[axis] for axis in AXES)

    def per_device(right_side, guess):
        shape = right_side.shape
        blocks = [tuple(side >> level for side in shape) for level in range(SHARED + 1)]
        whole = tuple(side * count for side, count in zip(blocks[SHARED], counts))
        coarse = [tuple(side >> level for side in whole) for level in range(LEVELS - SHARED)]
        grids = blocks[:SHARED] + coarse
        n0 = blocks[0][0]
        scratch = []
        vmem = lambda *dims: scratch.append(pltpu.VMEM(dims, jnp.float32))
        sems = lambda *dims: scratch.append(pltpu.SemaphoreType.DMA(dims))
        vmem(*shape)
        vmem(*shape)
        sems(2, Top.sets)
        vmem(4, n0 + 8, LANES)
        vmem(3, n0, LANES)
        scratch.append(pltpu.VMEM((2 * LANES, LANES), jnp.bfloat16))
        sent, got = Top.shapes(n0)
        for dims in sent:
            vmem(*dims)
        for way in WAYS:
            vmem(*got[way])
        sems(len(WAYS))
        sems(len(WAYS))
        for number, (x, y, z) in enumerate(grids):
            if number == 0:
                continue
            _, _, height, extent, tall = layout(number, (x, y, z))
            vmem(extent, tall, LANES)
            vmem(extent, tall, LANES)
            for _ in range(2):
                vmem(*((extent, tall) if number in REACH else (x // 2, rows_of(y))), LANES)
            vmem(4, max(height, rows_of(inner_height(number, (x, y, z)) + 1)) if number in REACH else height, LANES)
            vmem(3, spare_of(number, (x, y, z))[1], LANES)
        for number in REACH:
            n = blocks[number][0]
            _, groups, cut, _, cuts = Ring.sizes(n)
            vmem(groups, n, LANES)
            if cut != n:
                vmem(cuts, n, LANES)
                vmem(cuts, n, LANES)
            for way in WAYS:
                vmem(*Ring.shape(n, REACH[number], way))
            sems(len(WAYS))
            sems(len(WAYS))
        for number, (x, y, z) in enumerate(grids[:-1]):
            spare, tall = spare_of(number, (x, y, z))
            vmem(x // 2 + spare, max(16, tall), LANES)
        for _ in range(2):
            for number in range(LEVELS - 1):
                _, _, _, _, planes, tall = lift_shape(number, blocks[number + 1] if number < SHARED else grids[number + 1])
                vmem(planes, tall, LANES)
        bx, by, bz = blocks[SHARED]
        vmem(bx, rows_of(by), LANES)
        vmem(bx + 8, 24, LANES)
        vmem(by, LANES)
        vmem(counts[2], by, LANES)
        vmem(by, LANES)
        total = counts[0] * counts[1]
        vmem(total, by, LANES)
        sems(counts[2])
        sems(counts[2])
        scratch.append(pltpu.SemaphoreType.DMA)
        scratch.append(pltpu.SemaphoreType.DMA)
        scratch.append(pltpu.SemaphoreType.REGULAR((2,)))

        def kernel(*refs):
            solve_kernel(counts, blocks, coarse, refs)

        whole_block = pl.BlockSpec(memory_space=pltpu.VMEM)
        field = jax.ShapeDtypeStruct((n0 // 2 + 4, n0 + 24, LANES), jnp.float32)
        fields = pl.pallas_call(
            kernel,
            out_shape=(field,) * 4,
            in_specs=[pl.BlockSpec(memory_space=pltpu.HBM)] * 2,
            out_specs=(whole_block,) * 4,
            scratch_shapes=scratch,
            compiler_params=pltpu.CompilerParams(collective_id=0, has_side_effects=True, vmem_limit_bytes=VMEM_LIMIT * 2**20),
            name="vcycle",
        )(right_side, guess)

        def last(*refs):
            finish_kernel(counts, shape, *refs)
        in_hbm = pl.BlockSpec(memory_space=pltpu.HBM)
        return pl.pallas_call(
            last,
            out_shape=(jax.ShapeDtypeStruct(shape, jnp.float32),) * 2,
            in_specs=[whole_block] * 4,
            out_specs=(in_hbm,) * 2,
            scratch_shapes=[
                pltpu.VMEM(shape, jnp.float32), pltpu.VMEM(shape, jnp.float32), pltpu.VMEM((3, n0, LANES), jnp.float32),
                pltpu.VMEM((2 * LANES, LANES), jnp.bfloat16), pltpu.SemaphoreType.DMA((2, n0 // 16))],
            compiler_params=pltpu.CompilerParams(vmem_limit_bytes=8 * 2**20),
            name="finish",
        )(*fields)

    spec = P(*AXES)
    return jax.shard_map(per_device, mesh=mesh, in_specs=(spec, spec), out_specs=(spec, spec), check_vma=False)
```
